8 devices in a mesh: dp: 1 (over z), tp: 8 (over y, x, core).
Axes of the slice: x: 2, y: 2, z: 1, core: 2. Of those that a mesh axis runs over, the one named last changes fastest.
Arguments:
- tokens: int32 [1, 1024], P('dp')
- embed_table: bfloat16 [73448, 2560], P('tp')
- w_q: bfloat16 [2560, 40, 96], P(None, 'tp')
- w_dkv: bfloat16 [2560, 288], replicated
- g_kv: float32 [256], replicated
- w_uk: bfloat16 [256, 40, 64], P(None, 'tp')
- w_uv: bfloat16 [256, 40, 64], P(None, 'tp')
- w_o: bfloat16 [40, 64, 2560], P('tp')
- g_attn: float32 [2560], replicated
- g_mlp: float32 [2560], replicated
- w_gate: bfloat16 [2560, 6400], P(None, 'tp')
- w_up: bfloat16 [2560, 6400], P(None, 'tp')
- w_down: bfloat16 [6400, 2560], P('tp')
- d_out: bfloat16 [1, 1024, 2560], P('dp', 'tp')
Outputs:
- output 1: bfloat16 [1, 1024, 2560], P('dp', 'tp')
- output 2: bfloat16 [73448, 2560], P(('dp', 'tp'))
- output 3: float32 [2560, 40, 96], P('dp', 'tp')
- output 4: float32 [2560, 288], P('dp')
- output 5: float32 [256], P('dp')
- output 6: float32 [256, 40, 64], P('dp', 'tp')
- output 7: float32 [256, 40, 64], P('dp', 'tp')
- output 8: float32 [40, 64, 2560], P(('dp', 'tp'))
- output 9: float32 [2560], P('dp')
- output 10: float32 [2560], P('dp')
- output 11: float32 [2560, 6400], P('dp', 'tp')
- output 12: float32 [2560, 6400], P('dp', 'tp')
- output 13: float32 [6400, 2560], P(('dp', 'tp'))
All inputs are finite; a program needn't handle non-finite values.
Results may differ from the reference program's by a relative error of at most 0.02.
Values are sent between devices in bfloat16 or wider.
A program may use at most 1 GiB of HBM per device.

```python
import jax
import jax.numpy as jnp
import numpy as np
from jax import lax

VOCAB_SIZE = 73448
MODEL_DIM = 2560
NUM_HEADS = 40
NOPE_DIM = 64
ROPE_DIM = 32
VALUE_DIM = 64
KV_LORA = 256
FFN_DIM = 6400
BATCH_SIZE = 1
SEQ_LEN = 1024


def draw_tokens(tok_key):
    num_tokens = BATCH_SIZE * SEQ_LEN
    pool_size = num_tokens // 4
    bounds = jnp.asarray(np.arange(pool_size + 1, dtype=np.int64) * VOCAB_SIZE // pool_size, dtype=jnp.int32)
    key_list = jax.random.split(tok_key, 3)
    pool_ids = bounds[:-1] + jax.random.randint(key_list[0], (pool_size,), 0, bounds[1:] - bounds[:-1], dtype=jnp.int32)
    extra_picks = jax.random.randint(key_list[1], (num_tokens - pool_size,), 0, pool_size, dtype=jnp.int32)
    pick_idx = jax.random.permutation(key_list[2], jnp.concatenate([jnp.arange(pool_size, dtype=jnp.int32), extra_picks]))
    return pool_ids[pick_idx].reshape(BATCH_SIZE, SEQ_LEN)


def setup_inputs(seed: int = 0, part: int = 0) -> dict:
    base_key = jax.random.key(seed)
    part_key = jax.random.fold_in(base_key, part)
    key_list = jax.random.split(base_key, 12)
    part_list = jax.random.split(part_key, 2)
    qk_dim = NOPE_DIM + ROPE_DIM

    def normal_bf(idx, shape, scale):
        return (jax.random.normal(key_list[idx], shape, jnp.float32) * scale).astype(jnp.bfloat16)

    def gain_vec(idx, size):
        return 1.0 + 0.3 * jax.random.normal(key_list[idx], (size,), jnp.float32)

    return {
        'tokens': draw_tokens(part_list[0]),
        'embed_table': normal_bf(0, (VOCAB_SIZE, MODEL_DIM), 0.5),
        'w_q': normal_bf(1, (MODEL_DIM, NUM_HEADS, qk_dim), MODEL_DIM ** -0.5),
        'w_dkv': normal_bf(2, (MODEL_DIM, KV_LORA + ROPE_DIM), MODEL_DIM ** -0.5),
        'g_kv': gain_vec(3, KV_LORA),
        'w_uk': normal_bf(4, (KV_LORA, NUM_HEADS, NOPE_DIM), KV_LORA ** -0.5),
        'w_uv': normal_bf(5, (KV_LORA, NUM_HEADS, VALUE_DIM), KV_LORA ** -0.5),
        'w_o': normal_bf(6, (NUM_HEADS, VALUE_DIM, MODEL_DIM), (NUM_HEADS * VALUE_DIM) ** -0.5),
        'g_attn': gain_vec(7, MODEL_DIM),
        'g_mlp': gain_vec(8, MODEL_DIM),
        'w_gate': normal_bf(9, (MODEL_DIM, FFN_DIM), MODEL_DIM ** -0.5),
        'w_up': normal_bf(10, (MODEL_DIM, FFN_DIM), MODEL_DIM ** -0.5),
        'w_down': normal_bf(11, (FFN_DIM, MODEL_DIM), FFN_DIM ** -0.5),
        'd_out': jax.random.normal(part_list[1], (BATCH_SIZE, SEQ_LEN, MODEL_DIM), jnp.float32).astype(jnp.bfloat16),
    }


def to_bf(x_in):
    return x_in.astype(jnp.bfloat16).astype(jnp.float32)


def rms_scale(x_in, gain):
    return x_in * lax.rsqrt(jnp.mean(x_in * x_in, axis=-1, keepdims=True) + 1e-6) * gain


def rope_tables(seq_len, rope_dim):
    inv_freq = 10000.0 ** (-jnp.arange(0, rope_dim, 2, dtype=jnp.float32) / rope_dim)
    angles = jnp.arange(seq_len, dtype=jnp.float32)[:, None] * inv_freq[None, :]
    return jnp.cos(angles), jnp.sin(angles)


def apply_rope(x_in, cos_t, sin_t):
    half_dim = x_in.shape[-1] // 2
    x_lo = x_in[..., :half_dim]
    x_hi = x_in[..., half_dim:]
    return jnp.concatenate([x_lo * cos_t - x_hi * sin_t, x_hi * cos_t + x_lo * sin_t], axis=-1)


def attention(q_nope, q_pe, k_nope, k_pe, value):
    seq_len = q_nope.shape[1]
    scale = (NOPE_DIM + ROPE_DIM) ** -0.5
    causal = jnp.arange(seq_len)[:, None] >= jnp.arange(seq_len)[None, :]

    def one_head(head_in):
        head_qn, head_qp, head_kn, head_val = head_in
        scores = (jnp.einsum('bqn,bkn->bqk', head_qn, head_kn) + jnp.einsum('bqr,bkr->bqk', head_qp, k_pe)) * scale
        scores = jnp.where(causal[None], scores, -1e30)
        attn_prob = to_bf(jax.nn.softmax(scores, axis=-1))
        return to_bf(jnp.einsum('bqk,bkv->bqv', attn_prob, head_val))

    per_head = lax.map(one_head, (jnp.moveaxis(q_nope, 2, 0), jnp.moveaxis(q_pe, 2, 0), jnp.moveaxis(k_nope, 2, 0), jnp.moveaxis(value, 2, 0)))
    return jnp.moveaxis(per_head, 0, 2)


def layer_fwd(embedded, w_q, w_dkv, g_kv, w_uk, w_uv, w_o, g_attn, g_mlp, w_gate, w_up, w_down):
    cos_t, sin_t = rope_tables(embedded.shape[1], ROPE_DIM)
    x_attn = to_bf(rms_scale(embedded, g_attn))
    query = to_bf(jnp.einsum('bsd,dhe->bshe', x_attn, w_q))
    latent = jnp.einsum('bsd,dc->bsc', x_attn, w_dkv)
    c_kv = to_bf(rms_scale(latent[..., :KV_LORA], g_kv))
    k_pe = to_bf(apply_rope(latent[..., KV_LORA:], cos_t, sin_t))
    q_pe = to_bf(apply_rope(query[..., NOPE_DIM:], cos_t[:, None, :], sin_t[:, None, :]))
    k_nope = to_bf(jnp.einsum('bsc,che->bshe', c_kv, w_uk))
    value = to_bf(jnp.einsum('bsc,chv->bshv', c_kv, w_uv))
    attn_out = attention(query[..., :NOPE_DIM], q_pe, k_nope, k_pe, value)
    residual = to_bf(embedded + to_bf(jnp.einsum('bshv,hvd->bsd', attn_out, w_o)))
    x_mlp = to_bf(rms_scale(residual, g_mlp))
    gate = jnp.einsum('bsd,df->bsf', x_mlp, w_gate)
    up_proj = jnp.einsum('bsd,df->bsf', x_mlp, w_up)
    hidden = to_bf(jax.nn.silu(gate) * up_proj)
    mlp_out = to_bf(jnp.einsum('bsf,fd->bsd', hidden, w_down))
    return to_bf(residual + mlp_out)


def reference(tokens, embed_table, w_q, w_dkv, g_kv, w_uk, w_uv, w_o, g_attn, g_mlp, w_gate, w_up, w_down, d_out):
    embedded = jnp.take(embed_table, tokens, axis=0).astype(jnp.float32)
    layer_out, pullback = jax.vjp(layer_fwd, embedded, w_q.astype(jnp.float32), w_dkv.astype(jnp.float32), g_kv, w_uk.astype(jnp.float32), w_uv.astype(jnp.float32), w_o.astype(jnp.float32), g_attn, g_mlp, w_gate.astype(jnp.float32), w_up.astype(jnp.float32), w_down.astype(jnp.float32))
    grad_list = pullback(d_out.astype(jnp.float32))
    d_embed = to_bf(grad_list[0]).reshape(-1, MODEL_DIM)
    d_table = jax.ops.segment_sum(d_embed, tokens.reshape(-1), num_segments=VOCAB_SIZE).astype(jnp.bfloat16)
    return (layer_out.astype(jnp.bfloat16), d_table, grad_list[1], grad_list[2], grad_list[3], grad_list[4], grad_list[5], grad_list[6], grad_list[7], grad_list[8], grad_list[9], grad_list[10], grad_list[11])
```

```python
import functools

import jax
import jax.numpy as jnp
from jax import lax
from jax.experimental import pallas as pl
from jax.experimental.pallas import tpu as pltpu
from jax.sharding import PartitionSpec as P

EPSILON = 1e-6
ROPE_BASE = 10000.0
F32, BF16 = jnp.float32, jnp.bfloat16
LOG2E = 1.4426950408889634
VM = pltpu.VMEM
GB = 64
QB = 256


def mm(lhs, rhs, lc, rc):
    return lax.dot_general(lhs, rhs, (((lc,), (rc,)), ((), ())), preferred_element_type=F32)


def rope_tables(seq_len, rope_dim):
    inv_freq = ROPE_BASE ** (-jnp.arange(0, rope_dim, 2, dtype=F32) / rope_dim)
    angles = jnp.arange(seq_len, dtype=F32)[:, None] * inv_freq[None, :]
    return jnp.cos(angles), jnp.sin(angles)


def apply_rope(x_in, cos_t, sin_t):
    half_dim = x_in.shape[-1] // 2
    x_lo, x_hi = x_in[..., :half_dim], x_in[..., half_dim:]
    return jnp.concatenate([x_lo * cos_t - x_hi * sin_t, x_hi * cos_t + x_lo * sin_t], axis=-1)


def rms_norm(x_in, gain):
    inv_rms = lax.rsqrt(jnp.mean(x_in * x_in, axis=-1, keepdims=True) + EPSILON)
    return (x_in * inv_rms * gain).astype(BF16)


def kv_prep(latent, g_kv):
    lora = g_kv.shape[0]
    cos_t, sin_t = rope_tables(latent.shape[0], latent.shape[-1] - lora)
    k_pe = apply_rope(latent[:, lora:], cos_t, sin_t).astype(BF16)
    return rms_norm(latent[:, :lora], g_kv), k_pe


def block_index(tokens, vocab_local):
    ids = tokens.reshape(-1) - lax.axis_index('tp') * vocab_local
    n = ids.shape[0]
    owned = (ids >= 0) & (ids < vocab_local)
    blk = jnp.where(owned, ids >> 3, -1)
    pos = jnp.arange(n, dtype=jnp.int32)
    eq = (blk[:, None] == blk[None, :])
    first = jnp.min(jnp.where(eq, pos[None, :], n), axis=1)
    isf = owned & (first == pos)
    slot = jnp.sum((isf[None, :] & (pos[None, :] < first[:, None])).astype(jnp.int32), axis=1)
    key = jnp.where(owned, slot * 8 + (ids & 7), -1)
    blocks = jnp.sum(jnp.where(isf[None, :] & (slot[None, :] == pos[:, None]), blk[None, :], 0), axis=1)
    count = jnp.sum(isf.astype(jnp.int32)).reshape(1)
    return key, blocks, count


def gather_body(count_ref, blocks_ref, key_ref, tail_ref, table_ref, out_ref, stage, sem):
    rows, width = out_ref.shape
    full = table_ref.shape[0] // 8
    stage[...] = jnp.zeros_like(stage)
    out_ref[...] = jnp.zeros_like(out_ref)
    count = count_ref[0]

    def fetch(b, i):
        return pltpu.make_async_copy(table_ref.at[pl.ds(pl.multiple_of(b * 8, 8), 8), :], stage.at[i], sem)

    def chunk(ci, carry):
        base = ci * GB
        n = jnp.minimum(GB, count - base)

        def start(i, c):
            b = blocks_ref[base + i]

            @pl.when(b < full)
            def _():
                fetch(b, i).start()

            @pl.when(b >= full)
            def _():
                stage[i] = tail_ref[...]
            return c

        def wait(i, c):
            b = blocks_ref[base + i]

            @pl.when(b < full)
            def _():
                fetch(b, i).wait()
            return c

        lax.fori_loop(0, n, start, 0)
        lax.fori_loop(0, n, wait, 0)
        cols = lax.broadcasted_iota(jnp.int32, (rows, GB * 8), 1) + base * 8
        hot = jnp.where(cols == key_ref[...], 1.0, 0.0).astype(BF16)
        for c in range(0, width, 512):
            got = mm(hot, stage[:, :, c:c + 512].reshape(GB * 8, 512), 1, 0)
            out_ref[:, c:c + 512] += got.astype(BF16)
        return carry

    lax.fori_loop(0, (count + GB - 1) // GB, chunk, 0)


def gather_rows(key, blocks, count, table):
    rows, (vocab, width) = key.shape[0], table.shape
    full = vocab // 8 * 8
    tail = jnp.pad(table[full:], ((0, 8 - (vocab - full)), (0, 0)))
    smem = pl.BlockSpec(memory_space=pltpu.SMEM)
    return pl.pallas_call(
        gather_body, out_shape=jax.ShapeDtypeStruct((rows, width), BF16),
        in_specs=[smem, smem, pl.BlockSpec(memory_space=VM), pl.BlockSpec(memory_space=VM), pl.BlockSpec(memory_space=pl.ANY)],
        out_specs=pl.BlockSpec(memory_space=VM),
        scratch_shapes=[VM((GB, 8, width), BF16), pltpu.SemaphoreType.DMA],
        compiler_params=pltpu.CompilerParams(vmem_limit_bytes=40 << 20), name='gather_rows',
    )(count, blocks, key[:, None], tail, table)


ZR = 248


def table_grad_body(count_ref, blocks_ref, key_ref, de_ref, out_ref, tail_ref, zero, stage, zsem, sem):
    rows, width = de_ref.shape
    vocab = out_ref.shape[0]
    full = vocab // 8
    zero[...] = jnp.zeros_like(zero)
    tail_ref[...] = jnp.zeros_like(tail_ref)
    fills = [(r, min(ZR, full * 8 - r)) for r in range(0, full * 8, ZR)]
    copies = [pltpu.make_async_copy(zero.at[pl.ds(0, n), :], out_ref.at[pl.ds(r, n), :], zsem) for r, n in fills]
    for cp in copies:
        cp.start()
    count = count_ref[0]

    def put(b, i):
        return pltpu.make_async_copy(stage.at[i], out_ref.at[pl.ds(pl.multiple_of(b * 8, 8), 8), :], sem)

    def sums(ci):
        ids = lax.broadcasted_iota(jnp.int32, (GB * 8, rows), 0) + ci * (GB * 8)
        hot = jnp.where(ids == key_ref[...], 1.0, 0.0).astype(BF16)
        for c in range(0, width, 512):
            got = mm(hot, de_ref[:, c:c + 512], 1, 0)
            stage[:, :, c:c + 512] = got.astype(BF16).reshape(GB, 8, 512)

    def move(ci, go):
        base = ci * GB

        def one(i, c):
            b = blocks_ref[base + i]

            @pl.when(b < full)
            def _():
                go(put(b, i))
            @pl.when(b >= full)
            def _():
                tail_ref[...] = stage[i]
            return c

        lax.fori_loop(0, jnp.minimum(GB, count - base), one, 0)

    sums(0)
    for cp in copies:
        cp.wait()

    def chunk(ci, carry):
        @pl.when(ci > 0)
        def _():
            sums(ci)
        move(ci, lambda cp: cp.start())
        move(ci, lambda cp: cp.wait())
        return carry

    lax.fori_loop(0, (count + GB - 1) // GB, chunk, 0)


def table_grad(key, blocks, count, de_full, vocab):
    width = de_full.shape[1]
    smem = pl.BlockSpec(memory_space=pltpu.SMEM)
    full = vocab // 8 * 8
    out, tail = pl.pallas_call(
        table_grad_body, out_shape=[jax.ShapeDtypeStruct((vocab, width), BF16), jax.ShapeDtypeStruct((8, width), BF16)],
        in_specs=[smem, smem, pl.BlockSpec(memory_space=VM), pl.BlockSpec(memory_space=VM)],
        out_specs=[pl.BlockSpec(memory_space=pl.ANY), pl.BlockSpec(memory_space=VM)],
        scratch_shapes=[VM((ZR, width), BF16), VM((GB, 8, width), BF16), pltpu.SemaphoreType.DMA, pltpu.SemaphoreType.DMA],
        compiler_params=pltpu.CompilerParams(vmem_limit_bytes=40 << 20), name='table_grad',
    )(count, blocks, key[None, :], de_full)
    return lax.dynamic_update_slice(out, tail[:vocab - full], (full, 0))


def heads_of(q_ref, kn_ref, kp_ref, cos_ref, sin_ref, nope, half):
    q_pe = q_ref[nope:, :].astype(F32)
    lo, hi, cos_t, sin_t = q_pe[:half], q_pe[half:], cos_ref[...], sin_ref[...]
    q_all = jnp.concatenate([q_ref[:nope, :], (lo * cos_t - hi * sin_t).astype(BF16), (hi * cos_t + lo * sin_t).astype(BF16)], axis=0)
    return q_all, jnp.concatenate([kn_ref[...], kp_ref[...]], axis=0)


def scores_of(k_all, q_all, ki, qi, scale):
    s = mm(k_all[:, ki * QB:(ki + 1) * QB], q_all[:, qi * QB:(qi + 1) * QB], 0, 0) * scale
    if ki == qi:
        keys = lax.broadcasted_iota(jnp.int32, (QB, QB), 0)
        s = jnp.where(keys <= lax.broadcasted_iota(jnp.int32, (QB, QB), 1), s, -1e30)
    return s


def attn_fwd_body(q_ref, kn_ref, kp_ref, v_ref, cos_ref, sin_ref, o_ref, lse_ref):
    nope, half = kn_ref.shape[0], cos_ref.shape[0]
    scale = q_ref.shape[0] ** -0.5 * LOG2E
    q_all, k_all = heads_of(q_ref, kn_ref, kp_ref, cos_ref, sin_ref, nope, half)
    for qi in range(q_ref.shape[1] // QB):
        lanes = slice(qi * QB, (qi + 1) * QB)
        s = [scores_of(k_all, q_all, ki, qi, scale) for ki in range(qi + 1)]
        top = functools.reduce(jnp.maximum, [jnp.max(x, axis=0, keepdims=True) for x in s])
        p = [jnp.exp2(x - top) for x in s]
        total = sum(jnp.sum(x, axis=0, keepdims=True) for x in p)
        inv = 1.0 / total
        o = sum(mm(v_ref[:, ki * QB:(ki + 1) * QB], (x * inv).astype(BF16), 1, 0) for ki, x in enumerate(p))
        o_ref[:, lanes] = o.astype(BF16)
        lse_ref[0, :, lanes] = top + jnp.log2(total)


def attn_bwd_body(q_ref, kn_ref, kp_ref, v_ref, cos_ref, sin_ref, lse_ref, do_ref, dq_ref, dkn_ref, dv_ref, dkp_ref, dk_acc, dv_acc):
    nope, half = kn_ref.shape[0], cos_ref.shape[0]
    raw = q_ref.shape[0] ** -0.5
    q_all, k_all = heads_of(q_ref, kn_ref, kp_ref, cos_ref, sin_ref, nope, half)
    dk_acc[...] = jnp.zeros_like(dk_acc)
    dv_acc[...] = jnp.zeros_like(dv_acc)
    for qi in range(q_ref.shape[1] // QB):
        lanes = slice(qi * QB, (qi + 1) * QB)
        q_b, do_b, lse = q_all[:, lanes], do_ref[:, lanes], lse_ref[0, :, lanes]
        p = [jnp.exp2(scores_of(k_all, q_all, ki, qi, raw * LOG2E) - lse) for ki in range(qi + 1)]
        dp = [mm(v_ref[:, ki * QB:(ki + 1) * QB], do_b, 0, 0) for ki in range(qi + 1)]
        delta = sum(jnp.sum(a * b, axis=0, keepdims=True) for a, b in zip(p, dp))
        dq = None
        for ki in range(qi + 1):
            keys = slice(ki * QB, (ki + 1) * QB)
            ds = (p[ki] * (dp[ki] - delta) * raw).astype(BF16)
            part = mm(k_all[:, keys], ds, 1, 0)
            dq = part if dq is None else dq + part
            dk_acc[:, keys] += mm(q_b, ds, 1, 1)
            dv_acc[:, keys] += mm(do_b, p[ki].astype(BF16), 1, 1)
        cos_t, sin_t = cos_ref[:, lanes], sin_ref[:, lanes]
        lo, hi = dq[nope:nope + half], dq[nope + half:]
        dq_ref[:nope, lanes] = dq[:nope].astype(BF16)
        dq_ref[nope:nope + half, lanes] = (lo * cos_t + hi * sin_t).astype(BF16)
        dq_ref[nope + half:, lanes] = (hi * cos_t - lo * sin_t).astype(BF16)
    dkn_ref[...] = dk_acc[:nope, :].astype(BF16)
    dv_ref[...] = dv_acc[...].astype(BF16)

    @pl.when(pl.program_id(0) == 0)
    def _():
        dkp_ref[...] = jnp.zeros_like(dkp_ref)
    dkp_ref[...] += dk_acc[nope:, :]


def attn_specs(heads, qd, nope, rope, vd, seq):
    per = lambda r: pl.BlockSpec((r, seq), lambda h: (h, 0))
    one = lambda r: pl.BlockSpec((r, seq), lambda h: (0, 0))
    return [per(qd), per(nope), one(rope), per(vd), one(rope // 2), one(rope // 2)], per, one, pl.BlockSpec((1, 1, seq), lambda h: (h, 0, 0))


def attend_fwd(q, kn, kp, v, cos_t, sin_t, heads):
    seq, qd, nope, vd, rope = q.shape[1], q.shape[0] // heads, kn.shape[0] // heads, v.shape[0] // heads, kp.shape[0]
    ins, per, one, lse = attn_specs(heads, qd, nope, rope, vd, seq)
    return pl.pallas_call(
        attn_fwd_body, grid=(heads,), in_specs=ins, out_specs=[per(vd), lse],
        out_shape=[jax.ShapeDtypeStruct((heads * vd, seq), BF16), jax.ShapeDtypeStruct((heads, 1, seq), F32)],
        compiler_params=pltpu.CompilerParams(vmem_limit_bytes=40 << 20), name='attend_fwd',
    )(q, kn, kp, v, cos_t, sin_t)


def attend_bwd(q, kn, kp, v, cos_t, sin_t, lse, do, heads):
    seq, qd, nope, vd, rope = q.shape[1], q.shape[0] // heads, kn.shape[0] // heads, v.shape[0] // heads, kp.shape[0]
    ins, per, one, lse_spec = attn_specs(heads, qd, nope, rope, vd, seq)
    return pl.pallas_call(
        attn_bwd_body, grid=(heads,), in_specs=ins + [lse_spec, per(vd)], out_specs=[per(qd), per(nope), per(vd), one(rope)],
        out_shape=[jax.ShapeDtypeStruct(q.shape, BF16), jax.ShapeDtypeStruct(kn.shape, BF16), jax.ShapeDtypeStruct(v.shape, BF16), jax.ShapeDtypeStruct(kp.shape, F32)],
        scratch_shapes=[VM((qd, seq), F32), VM((vd, seq), F32)],
        compiler_params=pltpu.CompilerParams(vmem_limit_bytes=40 << 20), name='attend_bwd',
    )(q, kn, kp, v, cos_t, sin_t, lse, do)


def gather(x):
    return lax.all_gather(x, 'tp', axis=0, tiled=True)


def scatter(x):
    return lax.psum_scatter(x, 'tp', scatter_dimension=0, tiled=True)


def layer_pass(embedded, d_out, w_q, w_dkv, g_kv, w_uk, w_uv, w_o, g_attn, g_mlp, w_gate, w_up, w_down):
    w_q, heads = w_q
    x_attn_loc, attn_norm_pull = jax.vjp(rms_norm, embedded.astype(F32), g_attn)
    x_attn = gather(x_attn_loc)
    seq = x_attn.shape[0]
    rope = w_dkv.shape[0] - g_kv.shape[0]
    cos_t, sin_t = (t.T for t in rope_tables(seq, rope))
    query = mm(w_q, x_attn, 1, 1).astype(BF16)
    latent = mm(x_attn, w_dkv, 1, 1)
    (c_kv, k_pe), kv_pull = jax.vjp(kv_prep, latent, g_kv)
    k_nope = mm(w_uk, c_kv, 1, 1).astype(BF16)
    value = mm(w_uv, c_kv, 1, 1).astype(BF16)
    k_pe_t = k_pe.T
    attn_out, lse = attend_fwd(query, k_nope, k_pe_t, value, cos_t, sin_t, heads)
    attn_part = mm(attn_out, w_o, 0, 0).astype(BF16)
    attn_loc = scatter(attn_part)
    residual = (embedded.astype(F32) + attn_loc.astype(F32)).astype(BF16)
    x_mlp_loc, mlp_norm_pull = jax.vjp(rms_norm, residual.astype(F32), g_mlp)
    x_mlp = gather(x_mlp_loc)
    gate = mm(x_mlp, w_gate, 1, 1)
    up_proj = mm(x_mlp, w_up, 1, 1)
    gate_sig = jax.nn.sigmoid(gate)
    hidden = (gate * gate_sig * up_proj).astype(BF16)
    mlp_loc = scatter(mm(hidden, w_down, 1, 0).astype(BF16))
    layer_out = (residual.astype(F32) + mlp_loc.astype(F32)).astype(BF16)

    dy_full = gather(d_out)
    d_hidden = mm(dy_full, w_down, 1, 1)
    dw_down = mm(hidden, dy_full, 0, 0)
    d_up = (d_hidden * gate * gate_sig).astype(BF16)
    d_gate = (d_hidden * up_proj * gate_sig * (1.0 + gate * (1.0 - gate_sig))).astype(BF16)
    dw_gate = mm(d_gate, x_mlp, 0, 0)
    dw_up = mm(d_up, x_mlp, 0, 0)
    dx_mlp = scatter((mm(d_gate, w_gate, 1, 0) + mm(d_up, w_up, 1, 0)).astype(BF16))
    d_res_norm, dg_mlp_part = mlp_norm_pull(dx_mlp)
    d_residual = d_out.astype(F32) + d_res_norm
    d_attn_full = gather(d_residual.astype(BF16))
    dw_o = mm(attn_out, d_attn_full, 1, 0)
    d_attn_out = mm(w_o, d_attn_full, 1, 1).astype(BF16)
    d_query, d_knope, d_value, d_kpe = attend_bwd(query, k_nope, k_pe_t, value, cos_t, sin_t, lse, d_attn_out, heads)
    dw_uk = mm(d_knope, c_kv, 1, 0)
    dw_uv = mm(d_value, c_kv, 1, 0)
    d_ckv = (mm(d_knope, w_uk, 0, 0) + mm(d_value, w_uv, 0, 0)).astype(BF16)
    d_latent, dg_kv_part = kv_pull((d_ckv, d_kpe.T.astype(BF16)))
    d_latent = d_latent.astype(BF16)
    dw_q = mm(d_query, x_attn, 1, 0)
    dw_dkv_part = mm(d_latent, x_attn, 0, 0)
    dx_attn = scatter((mm(d_query, w_q, 0, 0) + mm(d_latent, w_dkv, 1, 0)).astype(BF16))
    d_emb_norm, dg_attn_part = attn_norm_pull(dx_attn)
    d_embed = (d_residual + d_emb_norm).astype(BF16)
    dw_dkv, dg_kv, dg_attn, dg_mlp = lax.psum((dw_dkv_part, dg_kv_part, dg_attn_part, dg_mlp_part), 'tp')
    return layer_out, d_embed, (dw_q, dw_dkv, dg_kv, dw_uk, dw_uv, dw_o, dg_attn, dg_mlp, dw_gate, dw_up, dw_down)


def rows_of(w):
    return jnp.transpose(w, (1, 2, 0)).reshape(-1, w.shape[0])


def unrows(g, heads):
    return jnp.transpose(g.reshape(heads, -1, g.shape[1]), (2, 0, 1))


def solution(mesh):
    def device_step(tokens, embed_table, w_q, w_dkv, g_kv, w_uk, w_uv, w_o, g_attn, g_mlp, w_gate, w_up, w_down, d_out):
        vocab_local, model_dim = embed_table.shape
        heads = w_q.shape[1]
        key, blocks, count = block_index(tokens, vocab_local)
        rows = gather_rows(key, blocks, count, embed_table)
        embedded = scatter(rows)
        layer_out, d_embed, grads = layer_pass(
            embedded, d_out[0], (rows_of(w_q), heads), w_dkv.T, g_kv, rows_of(w_uk), rows_of(w_uv), w_o.reshape(-1, model_dim),
            g_attn, g_mlp, w_gate.T, w_up.T, w_down)
        de_full = gather(d_embed)
        d_table = table_grad(key, blocks, count, de_full, vocab_local)
        dw_q, dw_dkv, dg_kv, dw_uk, dw_uv, dw_o, dg_attn, dg_mlp, dw_gate, dw_up, dw_down = grads
        return (layer_out[None], d_table, unrows(dw_q, heads), dw_dkv.T, dg_kv, unrows(dw_uk, heads), unrows(dw_uv, heads),
                dw_o.reshape(w_o.shape), dg_attn, dg_mlp, dw_gate.T, dw_up.T, dw_down)

    row_spec = P('dp', 'tp', None)
    head_spec = P(None, 'tp', None)
    in_specs = (P('dp', None), P('tp', None), head_spec, P(None, None), P(None), head_spec, head_spec, P('tp', None, None), P(None), P(None), P(None, 'tp'), P(None, 'tp'), P('tp', None), row_spec)
    out_specs = (row_spec, P(('dp', 'tp'), None), P('dp', 'tp', None), P('dp', None), P('dp'), P('dp', 'tp', None), P('dp', 'tp', None), P(('dp', 'tp'), None, None), P('dp'), P('dp'), P('dp', 'tp'), P('dp', 'tp'), P(('dp', 'tp'), None))
    return jax.shard_map(device_step, mesh=mesh, in_specs=in_specs, out_specs=out_specs, check_vma=False)
```

```python
import functools

import jax
import jax.numpy as jnp
from jax import lax
from jax.experimental import pallas as pl
from jax.experimental.pallas import tpu as pltpu
from jax.sharding import PartitionSpec as P

EPSILON = 1e-6
ROPE_BASE = 10000.0
F32, BF16 = jnp.float32, jnp.bfloat16
LOG2E = 1.4426950408889634
VM = pltpu.VMEM
GB = 64
QB = 256


def mm(lhs, rhs, lc, rc):
    return lax.dot_general(lhs, rhs, (((lc,), (rc,)), ((), ())), preferred_element_type=F32)


def rope_tables(seq_len, rope_dim):
    inv_freq = ROPE_BASE ** (-jnp.arange(0, rope_dim, 2, dtype=F32) / rope_dim)
    angles = jnp.arange(seq_len, dtype=F32)[:, None] * inv_freq[None, :]
    return jnp.cos(angles), jnp.sin(angles)


def apply_rope(x_in, cos_t, sin_t):
    half_dim = x_in.shape[-1] // 2
    x_lo, x_hi = x_in[..., :half_dim], x_in[..., half_dim:]
    return jnp.concatenate([x_lo * cos_t - x_hi * sin_t, x_hi * cos_t + x_lo * sin_t], axis=-1)


def rms_norm(x_in, gain):
    inv_rms = lax.rsqrt(jnp.mean(x_in * x_in, axis=-1, keepdims=True) + EPSILON)
    return (x_in * inv_rms * gain).astype(BF16)


def kv_prep(latent, g_kv):
    lora = g_kv.shape[0]
    cos_t, sin_t = rope_tables(latent.shape[0], latent.shape[-1] - lora)
    k_pe = apply_rope(latent[:, lora:], cos_t, sin_t).astype(BF16)
    return rms_norm(latent[:, :lora], g_kv), k_pe


def block_index(tokens, vocab_local):
    ids = tokens.reshape(-1) - lax.axis_index('tp') * vocab_local
    n = ids.shape[0]
    owned = (ids >= 0) & (ids < vocab_local)
    blk = jnp.where(owned, ids >> 3, -1)
    pos = jnp.arange(n, dtype=jnp.int32)
    eq = (blk[:, None] == blk[None, :])
    first = jnp.min(jnp.where(eq, pos[None, :], n), axis=1)
    isf = owned & (first == pos)
    slot = jnp.sum((isf[None, :] & (pos[None, :] < first[:, None])).astype(jnp.int32), axis=1)
    key = jnp.where(owned, slot * 8 + (ids & 7), -1)
    blocks = jnp.sum(jnp.where(isf[None, :] & (slot[None, :] == pos[:, None]), blk[None, :], 0), axis=1)
    count = jnp.sum(isf.astype(jnp.int32)).reshape(1)
    return key, blocks, count


def gather_body(count_ref, blocks_ref, key_ref, tail_ref, table_ref, out_ref, stage, sem):
    rows, width = out_ref.shape
    full = table_ref.shape[0] // 8
    stage[...] = jnp.zeros_like(stage)
    out_ref[...] = jnp.zeros_like(out_ref)
    count = count_ref[0]

    def fetch(b, i):
        return pltpu.make_async_copy(table_ref.at[pl.ds(pl.multiple_of(b * 8, 8), 8), :], stage.at[i], sem)

    def chunk(ci, carry):
        base = ci * GB
        n = jnp.minimum(GB, count - base)

        def start(i, c):
            b = blocks_ref[base + i]

            @pl.when(b < full)
            def _():
                fetch(b, i).start()

            @pl.when(b >= full)
            def _():
                stage[i] = tail_ref[...]
            return c

        def wait(i, c):
            b = blocks_ref[base + i]

            @pl.when(b < full)
            def _():
                fetch(b, i).wait()
            return c

        lax.fori_loop(0, n, start, 0)
        lax.fori_loop(0, n, wait, 0)
        cols = lax.broadcasted_iota(jnp.int32, (rows, GB * 8), 1) + base * 8
        hot = jnp.where(cols == key_ref[...], 1.0, 0.0).astype(BF16)
        for c in range(0, width, 512):
            got = mm(hot, stage[:, :, c:c + 512].reshape(GB * 8, 512), 1, 0)
            out_ref[:, c:c + 512] += got.astype(BF16)
        return carry

    lax.fori_loop(0, (count + GB - 1) // GB, chunk, 0)


def gather_rows(key, blocks, count, table):
    rows, (vocab, width) = key.shape[0], table.shape
    full = vocab // 8 * 8
    tail = jnp.pad(table[full:], ((0, 8 - (vocab - full)), (0, 0)))
    smem = pl.BlockSpec(memory_space=pltpu.SMEM)
    return pl.pallas_call(
        gather_body, out_shape=jax.ShapeDtypeStruct((rows, width), BF16),
        in_specs=[smem, smem, pl.BlockSpec(memory_space=VM), pl.BlockSpec(memory_space=VM), pl.BlockSpec(memory_space=pl.ANY)],
        out_specs=pl.BlockSpec(memory_space=VM),
        scratch_shapes=[VM((GB, 8, width), BF16), pltpu.SemaphoreType.DMA],
        compiler_params=pltpu.CompilerParams(vmem_limit_bytes=40 << 20), name='gather_rows',
    )(count, blocks, key[:, None], tail, table)


ZR = 248


def table_grad_body(count_ref, blocks_ref, key_ref, de_ref, out_ref, tail_ref, zero, stage, zsem, sem):
    rows, width = de_ref.shape
    vocab = out_ref.shape[0]
    full = vocab // 8
    zero[...] = jnp.zeros_like(zero)
    tail_ref[...] = jnp.zeros_like(tail_ref)
    fills = [(r, min(ZR, full * 8 - r)) for r in range(0, full * 8, ZR)]
    copies = [pltpu.make_async_copy(zero.at[pl.ds(0, n), :], out_ref.at[pl.ds(r, n), :], zsem) for r, n in fills]
    for cp in copies:
        cp.start()
    count = count_ref[0]

    def put(b, i):
        return pltpu.make_async_copy(stage.at[i], out_ref.at[pl.ds(pl.multiple_of(b * 8, 8), 8), :], sem)

    def sums(ci):
        ids = lax.broadcasted_iota(jnp.int32, (GB * 8, rows), 0) + ci * (GB * 8)
        hot = jnp.where(ids == key_ref[...], 1.0, 0.0).astype(BF16)
        for c in range(0, width, 512):
            got = mm(hot, de_ref[:, c:c + 512], 1, 0)
            stage[:, :, c:c + 512] = got.astype(BF16).reshape(GB, 8, 512)

    def move(ci, go):
        base = ci * GB

        def one(i, c):
            b = blocks_ref[base + i]

            @pl.when(b < full)
            def _():
                go(put(b, i))
            @pl.when(b >= full)
            def _():
                tail_ref[...] = stage[i]
            return c

        lax.fori_loop(0, jnp.minimum(GB, count - base), one, 0)

    sums(0)
    for cp in copies:
        cp.wait()

    def chunk(ci, carry):
        @pl.when(ci > 0)
        def _():
            sums(ci)
        move(ci, lambda cp: cp.start())
        move(ci, lambda cp: cp.wait())
        return carry

    lax.fori_loop(0, (count + GB - 1) // GB, chunk, 0)


def table_grad(key, blocks, count, de_full, vocab):
    width = de_full.shape[1]
    smem = pl.BlockSpec(memory_space=pltpu.SMEM)
    full = vocab // 8 * 8
    out, tail = pl.pallas_call(
        table_grad_body, out_shape=[jax.ShapeDtypeStruct((vocab, width), BF16), jax.ShapeDtypeStruct((8, width), BF16)],
        in_specs=[smem, smem, pl.BlockSpec(memory_space=VM), pl.BlockSpec(memory_space=VM)],
        out_specs=[pl.BlockSpec(memory_space=pl.ANY), pl.BlockSpec(memory_space=VM)],
        scratch_shapes=[VM((ZR, width), BF16), VM((GB, 8, width), BF16), pltpu.SemaphoreType.DMA, pltpu.SemaphoreType.DMA],
        compiler_params=pltpu.CompilerParams(vmem_limit_bytes=40 << 20), name='table_grad',
    )(count, blocks, key[None, :], de_full)
    return lax.dynamic_update_slice(out, tail[:vocab - full], (full, 0))


def heads_of(q_ref, kn_ref, kp_ref, cos_ref, sin_ref, nope, half):
    q_pe = q_ref[nope:, :].astype(F32)
    lo, hi, cos_t, sin_t = q_pe[:half], q_pe[half:], cos_ref[...], sin_ref[...]
    q_all = jnp.concatenate([q_ref[:nope, :], (lo * cos_t - hi * sin_t).astype(BF16), (hi * cos_t + lo * sin_t).astype(BF16)], axis=0)
    return q_all, jnp.concatenate([kn_ref[...], kp_ref[...]], axis=0)


def scores_of(k_all, q_all, ki, qi, scale):
    s = mm(k_all[:, ki * QB:(ki + 1) * QB], q_all[:, qi * QB:(qi + 1) * QB], 0, 0) * scale
    if ki == qi:
        keys = lax.broadcasted_iota(jnp.int32, (QB, QB), 0)
        s = jnp.where(keys <= lax.broadcasted_iota(jnp.int32, (QB, QB), 1), s, -1e30)
    return s


def attn_fwd_body(q_ref, kn_ref, kp_ref, v_ref, cos_ref, sin_ref, o_ref, lse_ref):
    nope, half = kn_ref.shape[0], cos_ref.shape[0]
    scale = q_ref.shape[0] ** -0.5 * LOG2E
    q_all, k_all = heads_of(q_ref, kn_ref, kp_ref, cos_ref, sin_ref, nope, half)
    for qi in range(q_ref.shape[1] // QB):
        lanes = slice(qi * QB, (qi + 1) * QB)
        s = [scores_of(k_all, q_all, ki, qi, scale) for ki in range(qi + 1)]
        top = functools.reduce(jnp.maximum, [jnp.max(x, axis=0, keepdims=True) for x in s])
        p = [jnp.exp2(x - top) for x in s]
        total = sum(jnp.sum(x, axis=0, keepdims=True) for x in p)
        inv = 1.0 / total
        o = sum(mm(v_ref[:, ki * QB:(ki + 1) * QB], (x * inv).astype(BF16), 1, 0) for ki, x in enumerate(p))
        o_ref[:, lanes] = o.astype(BF16)
        lse_ref[0, :, lanes] = top + jnp.log2(total)


def attn_bwd_body(q_ref, kn_ref, kp_ref, v_ref, cos_ref, sin_ref, lse_ref, do_ref, dq_ref, dkn_ref, dv_ref, dkp_ref, dk_acc, dv_acc):
    nope, half = kn_ref.shape[0], cos_ref.shape[0]
    raw = q_ref.shape[0] ** -0.5
    q_all, k_all = heads_of(q_ref, kn_ref, kp_ref, cos_ref, sin_ref, nope, half)
    dk_acc[...] = jnp.zeros_like(dk_acc)
    dv_acc[...] = jnp.zeros_like(dv_acc)
    for qi in range(q_ref.shape[1] // QB):
        lanes = slice(qi * QB, (qi + 1) * QB)
        q_b, do_b, lse = q_all[:, lanes], do_ref[:, lanes], lse_ref[0, :, lanes]
        p = [jnp.exp2(scores_of(k_all, q_all, ki, qi, raw * LOG2E) - lse) for ki in range(qi + 1)]
        dp = [mm(v_ref[:, ki * QB:(ki + 1) * QB], do_b, 0, 0) for ki in range(qi + 1)]
        delta = sum(jnp.sum(a * b, axis=0, keepdims=True) for a, b in zip(p, dp))
        dq = None
        for ki in range(qi + 1):
            keys = slice(ki * QB, (ki + 1) * QB)
            ds = (p[ki] * (dp[ki] - delta) * raw).astype(BF16)
            part = mm(k_all[:, keys], ds, 1, 0)
            dq = part if dq is None else dq + part
            dk_acc[:, keys] += mm(q_b, ds, 1, 1)
            dv_acc[:, keys] += mm(do_b, p[ki].astype(BF16), 1, 1)
        cos_t, sin_t = cos_ref[:, lanes], sin_ref[:, lanes]
        lo, hi = dq[nope:nope + half], dq[nope + half:]
        dq_ref[:nope, lanes] = dq[:nope].astype(BF16)
        dq_ref[nope:nope + half, lanes] = (lo * cos_t + hi * sin_t).astype(BF16)
        dq_ref[nope + half:, lanes] = (hi * cos_t - lo * sin_t).astype(BF16)
    dkn_ref[...] = dk_acc[:nope, :].astype(BF16)
    dv_ref[...] = dv_acc[...].astype(BF16)

    @pl.when(pl.program_id(0) == 0)
    def _():
        dkp_ref[...] = jnp.zeros_like(dkp_ref)
    dkp_ref[...] += dk_acc[nope:, :]


def attn_specs(heads, qd, nope, rope, vd, seq):
    per = lambda r: pl.BlockSpec((r, seq), lambda h: (h, 0))
    one = lambda r: pl.BlockSpec((r, seq), lambda h: (0, 0))
    return [per(qd), per(nope), one(rope), per(vd), one(rope // 2), one(rope // 2)], per, one, pl.BlockSpec((1, 1, seq), lambda h: (h, 0, 0))


def attend_fwd(q, kn, kp, v, cos_t, sin_t, heads):
    seq, qd, nope, vd, rope = q.shape[1], q.shape[0] // heads, kn.shape[0] // heads, v.shape[0] // heads, kp.shape[0]
    ins, per, one, lse = attn_specs(heads, qd, nope, rope, vd, seq)
    return pl.pallas_call(
        attn_fwd_body, grid=(heads,), in_specs=ins, out_specs=[per(vd), lse],
        out_shape=[jax.ShapeDtypeStruct((heads * vd, seq), BF16), jax.ShapeDtypeStruct((heads, 1, seq), F32)],
        compiler_params=pltpu.CompilerParams(vmem_limit_bytes=40 << 20), name='attend_fwd',
    )(q, kn, kp, v, cos_t, sin_t)


def attend_bwd(q, kn, kp, v, cos_t, sin_t, lse, do, heads):
    seq, qd, nope, vd, rope = q.shape[1], q.shape[0] // heads, kn.shape[0] // heads, v.shape[0] // heads, kp.shape[0]
    ins, per, one, lse_spec = attn_specs(heads, qd, nope, rope, vd, seq)
    return pl.pallas_call(
        attn_bwd_body, grid=(heads,), in_specs=ins + [lse_spec, per(vd)], out_specs=[per(qd), per(nope), per(vd), one(rope)],
        out_shape=[jax.ShapeDtypeStruct(q.shape, BF16), jax.ShapeDtypeStruct(kn.shape, BF16), jax.ShapeDtypeStruct(v.shape, BF16), jax.ShapeDtypeStruct(kp.shape, F32)],
        scratch_shapes=[VM((qd, seq), F32), VM((vd, seq), F32)],
        compiler_params=pltpu.CompilerParams(vmem_limit_bytes=40 << 20), name='attend_bwd',
    )(q, kn, kp, v, cos_t, sin_t, lse, do)


def gather(x):
    return lax.all_gather(x, 'tp', axis=0, tiled=True)


def scatter(x):
    return lax.psum_scatter(x, 'tp', scatter_dimension=0, tiled=True)


class Exchange:
    def __init__(self, widths, pieces):
        self.widths, self.pieces = widths, pieces

    def rs_scratch(self, rows):
        n = len(self.pieces)
        out = []
        for w in self.widths:
            out += [VM((4, rows, w), BF16), VM((2, rows, w), BF16), VM((2, rows, w), BF16), VM((rows, w), BF16), VM((rows, w), BF16)]
        dma = pltpu.SemaphoreType.DMA
        return out + [dma((4, n)), dma((4, n)), dma((n,)), dma((n,)), dma((n,)), dma((n,))]

    def ag_scratch(self):
        n = len(self.pieces)
        dma = pltpu.SemaphoreType.DMA
        return [dma((3, n)), dma((2, n)), dma((n,)), dma((n,)), dma((4, n)), dma((4, n))]

    def place(self, rows):
        me = lax.axis_index('tp')
        core, x, y = me % 2, (me // 2) % 2, me // 4
        dev = lambda yy, xx, cc: (yy * 2 + xx) * 2 + cc
        self.me, self.rows = me, rows
        self.pn, self.xn, self.yn = dev(y, x, 1 - core), dev(y, 1 - x, core), dev(1 - y, x, core)
        chips = [(y, x), (y, 1 - x), (1 - y, x), (1 - y, 1 - x)]
        at = lambda d: pl.ds(pl.multiple_of(d * rows, rows), rows)
        self.mine = [at(dev(*ch, core)) for ch in chips]
        self.theirs = [at(dev(*ch, 1 - core)) for ch in chips]
        self.chip_rows = [pl.ds(pl.multiple_of((ch[0] * 2 + ch[1]) * 2 * rows, 2 * rows), 2 * rows) for ch in chips]

    def enter(self):
        sem = pltpu.get_barrier_semaphore()
        for d in (self.pn, self.xn, self.yn):
            pl.semaphore_signal(sem, inc=1, device_id={'tp': d}, device_id_type=pl.DeviceIdType.MESH)
        pl.semaphore_wait(sem, 3)

    def copy(self, src, dst, ssem, rsem, dev):
        return pltpu.make_async_remote_copy(src_ref=src, dst_ref=dst, send_sem=ssem, recv_sem=rsem, device_id={'tp': dev}, device_id_type=pl.DeviceIdType.MESH)

    def reduce_scatter(self, parts, accs, scratch, produce=None):
        na = len(self.widths)
        bufs = [scratch[5 * a:5 * a + 5] for a in range(na)]
        ds, dr, s1, r1, s2, r2 = scratch[5 * na:]
        order = range(len(self.pieces))
        pair, hop1, hop2 = {}, {}, {}
        for i, (h, a, c0, cn) in enumerate(self.pieces):
            cols = pl.ds(c0, cn)
            dbuf, sb1, rb1, sb2, rb2 = bufs[a]
            for j in range(4):
                pair[j, i] = self.copy(parts[a].at[self.theirs[j], cols], dbuf.at[j, :, cols], ds.at[j, i], dr.at[j, i], self.pn)
            to1, to2 = (self.xn, self.yn) if h == 0 else (self.yn, self.xn)
            hop1[i] = self.copy(sb1.at[:, :, cols], rb1.at[:, :, cols], s1.at[i], r1.at[i], to1)
            hop2[i] = self.copy(sb2.at[:, cols], rb2.at[:, cols], s2.at[i], r2.at[i], to2)

        def chip_sum(j, i):
            h, a, c0, cn = self.pieces[i]
            pair[j, i].wait_recv()
            return parts[a][self.mine[j], c0:c0 + cn].astype(F32) + bufs[a][0][j, :, c0:c0 + cn].astype(F32)

        if produce is None:
            for i in order:
                pair[3, i].start()
                pair[1 if self.pieces[i][0] == 0 else 2, i].start()
            for i in order:
                pair[2 if self.pieces[i][0] == 0 else 1, i].start()
                pair[0, i].start()
            first = list(order)
        else:
            first = []
            for j in (3, 1, 2, 0):
                produce(j)
                for i in order:
                    pair[j, i].start()
                if j in (1, 2):
                    for i in order:
                        if self.pieces[i][0] == j - 1:
                            self.send1(i, chip_sum, bufs, hop1)
        for i in first:
            self.send1(i, chip_sum, bufs, hop1)
        for i in order:
            h, a, c0, cn = self.pieces[i]
            hop1[i].wait_recv()
            bufs[a][3][:, c0:c0 + cn] = (chip_sum(2 if h == 0 else 1, i) + bufs[a][2][1, :, c0:c0 + cn].astype(F32)).astype(BF16)
            hop2[i].start()
        for i in order:
            h, a, c0, cn = self.pieces[i]
            own = chip_sum(0, i) + bufs[a][2][0, :, c0:c0 + cn].astype(F32)
            hop2[i].wait_recv()
            accs[a][:, c0:c0 + cn] = own + bufs[a][4][:, c0:c0 + cn].astype(F32)
        self.pending = list(pair.values()) + list(hop1.values()) + list(hop2.values())

    def send1(self, i, chip_sum, bufs, hop1):
        h, a, c0, cn = self.pieces[i]
        bufs[a][1][0, :, c0:c0 + cn] = chip_sum(1 if h == 0 else 2, i).astype(BF16)
        bufs[a][1][1, :, c0:c0 + cn] = chip_sum(3, i).astype(BF16)
        hop1[i].start()

    def drain(self):
        for cp in self.pending:
            cp.wait_send()
        self.pending = []

    def all_gather(self, fulls, scratch, consume=None):
        os_, xr, fs, fr, ps, pr = scratch
        half0 = [i for i, p in enumerate(self.pieces) if p[0] == 0]
        half1 = [i for i, p in enumerate(self.pieces) if p[0] == 1]

        def block(i, j):
            h, a, c0, cn = self.pieces[i]
            return fulls[a].at[self.mine[j], pl.ds(c0, cn)]

        def to(i, j, ssem, rsem, dev):
            return self.copy(block(i, j), block(i, j), ssem, rsem, dev)

        own = [[to(i, 0, os_.at[k, i], xr.at[k, i], dev) for i in range(len(self.pieces))] for k, dev in enumerate((self.xn, self.yn))]
        from_n = [[to(i, 1 + k, os_.at[k, i], xr.at[k, i], dev) for i in range(len(self.pieces))] for k, dev in enumerate((self.xn, self.yn))]
        fwd = {i: to(i, 2 if self.pieces[i][0] == 0 else 1, fs.at[i], fr.at[i], self.xn if self.pieces[i][0] == 0 else self.yn) for i in half0 + half1}
        diag = {i: to(i, 3, fs.at[i], fr.at[i], self.xn) for i in half0 + half1}
        give = [[to(i, j, ps.at[j, i], pr.at[j, i], self.pn) for i in range(len(self.pieces))] for j in range(4)]
        for a, b in zip(half1, half0):
            own[0][a].start()
            own[1][b].start()
        for a, b in zip(half0, half1):
            own[0][a].start()
            own[1][b].start()
        for i in half0 + half1:
            give[0][i].start()
        take = lambda j: [self.take(i, j, fulls, ps, pr).wait_recv() for i in range(len(self.pieces))]
        take(0)
        if consume is not None:
            consume(0)
        for a, b in zip(half1, half0):
            from_n[1][b].wait_recv()
            fwd[b].start()
            give[2][b].start()
            from_n[0][a].wait_recv()
            fwd[a].start()
            give[1][a].start()
        for a, b in zip(half1, half0):
            from_n[1][a].wait_recv()
            give[2][a].start()
            from_n[0][b].wait_recv()
            give[1][b].start()
        for j in (1, 2):
            take(j)
            if consume is not None:
                consume(j)
        for a, b in zip(half1, half0):
            for i in (b, a):
                diag[i].wait_recv()
                give[3][i].start()
        take(3)
        if consume is not None:
            consume(3)
        for cp in own[0] + own[1] + list(fwd.values()) + [c for g in give for c in g]:
            cp.wait_send()

    def take(self, i, j, fulls, ps, pr):
        h, a, c0, cn = self.pieces[i]
        ref = fulls[a].at[self.theirs[j], pl.ds(c0, cn)]
        return self.copy(ref, ref, ps.at[j, i], pr.at[j, i], self.pn)


def halves(width, n):
    step = width // (2 * n)
    return [(h, 0, (h * n + k) * step, step) for k in range(n) for h in range(2)]


MAIN = halves(2560, 2)


def norm_rows(x, gain):
    return x * lax.rsqrt(jnp.mean(x * x, axis=-1, keepdims=True) + EPSILON) * gain


def norm_rows_vjp(x, gain, dy):
    r = lax.rsqrt(jnp.mean(x * x, axis=-1, keepdims=True) + EPSILON)
    gd = dy * gain
    dot = jnp.mean(gd * x, axis=-1, keepdims=True)
    return r * gd - x * (r * r * r * dot), jnp.sum(dy * x * r, axis=0, keepdims=True)


def exchange_call(body, name, cid, ins, out_shape, scratch):
    vmem = pl.BlockSpec(memory_space=VM)
    return pl.pallas_call(
        body, out_shape=out_shape, in_specs=[vmem] * len(ins), out_specs=[vmem] * len(out_shape), scratch_shapes=scratch,
        compiler_params=pltpu.CompilerParams(vmem_limit_bytes=48 << 20, collective_id=cid, has_side_effects=True), name=name)(*ins)


def shape(dims, dtype):
    return jax.ShapeDtypeStruct(dims, dtype)


def embed_body(part, gain, e_ref, full, acc, *scratch):
    ex = Exchange([part.shape[1]], MAIN)
    ex.place(acc.shape[0])
    ex.enter()
    ex.reduce_scatter([part], [acc], scratch[:11])
    e = acc[...].astype(BF16)
    e_ref[...] = e
    full[ex.mine[0], :] = norm_rows(e.astype(F32), gain[...]).astype(BF16)
    ex.all_gather([full], scratch[11:])
    ex.drain()


def attn_out_body(part, e_ref, gain, h_ref, full, acc, *scratch):
    ex = Exchange([part.shape[1]], MAIN)
    ex.place(acc.shape[0])
    ex.enter()
    ex.reduce_scatter([part], [acc], scratch[:11])
    h = (e_ref[...].astype(F32) + acc[...].astype(BF16).astype(F32)).astype(BF16)
    h_ref[...] = h
    full[ex.mine[0], :] = norm_rows(h.astype(F32), gain[...]).astype(BF16)
    ex.all_gather([full], scratch[11:])
    ex.drain()


def mlp_back_body(part, h_ref, dy_ref, gain, dres_ref, dg_ref, full, acc, *scratch):
    ex = Exchange([part.shape[1]], MAIN)
    ex.place(acc.shape[0])
    ex.enter()
    ex.reduce_scatter([part], [acc], scratch[:11])
    dx, dg = norm_rows_vjp(h_ref[...].astype(F32), gain[...], acc[...])
    dg_ref[...] = dg
    dres = dy_ref[...].astype(F32) + dx
    dres_ref[...] = dres
    full[ex.mine[0], :] = dres.astype(BF16)
    ex.all_gather([full], scratch[11:])
    ex.drain()


LAST = MAIN + [(0, 1, 0, 256), (1, 1, 256, 128)]


def attn_back_body(part, lat, e_ref, dres_ref, gain, dgm_ref, dgk_ref, dg_ref, full, full_lat, acc, acc_lat, gsum, gs, gr, *scratch):
    ex = Exchange([part.shape[1], lat.shape[1]], LAST)
    ex.place(acc.shape[0])
    width, lora = part.shape[1], dgk_ref.shape[1]
    me = lax.axis_index('tp')
    sem = pltpu.get_barrier_semaphore()
    for k in range(1, 8):
        pl.semaphore_signal(sem, inc=1, device_id={'tp': (me + k) % 8}, device_id_type=pl.DeviceIdType.MESH)
    pl.semaphore_wait(sem, 7)
    ex.reduce_scatter([part, lat], [acc, acc_lat], scratch[:16])
    dx, dg = norm_rows_vjp(e_ref[...].astype(F32), gain[...], acc[...])
    full[ex.mine[0], :] = (dres_ref[...] + dx).astype(BF16)
    full_lat[ex.mine[0], :] = acc_lat[...].astype(BF16)
    gsum[me, :, :width] = dg
    gsum[me, :, width:2 * width] = dgm_ref[...]
    gsum[me, :, 2 * width:] = dgk_ref[...]
    sends = [ex.copy(gsum.at[me], gsum.at[me], gs.at[k - 1], gr.at[k - 1], (me + k) % 8) for k in range(1, 8)]
    for cp in sends:
        cp.start()
    ex.all_gather([full, full_lat], scratch[16:])
    for k in range(1, 8):
        frm = (me + 8 - k) % 8
        ex.copy(gsum.at[frm], gsum.at[frm], gs.at[k - 1], gr.at[k - 1], frm).wait_recv()
    dg_ref[...] = jnp.sum(gsum[...], axis=0)
    for cp in sends:
        cp.wait_send()
    ex.drain()


def ex_scratch(widths, pieces, rows):
    ex = Exchange(widths, pieces)
    return ex.rs_scratch(rows) + ex.ag_scratch()


def layer_pass(rows, d_out, w_q, w_dkv, g_kv, w_uk, w_uv, w_o, g_attn, g_mlp, w_gate, w_up, w_down):
    w_q, heads = w_q
    seq, width = rows.shape
    local = d_out.shape[0]
    lora = g_kv.shape[0]
    rope = w_dkv.shape[0] - lora
    main = [VM((local, width), F32)] + ex_scratch([width], MAIN, local)
    loc, fullb = shape((local, width), BF16), shape((seq, width), BF16)
    ga, gm = g_attn[None, :], g_mlp[None, :]
    embedded, x_attn = exchange_call(embed_body, 'embed_exchange', 1, [rows, ga], [loc, fullb], main)
    d_out_late, x_attn = lax.optimization_barrier((d_out, x_attn))
    cos_t, sin_t = (t.T for t in rope_tables(seq, rope))
    query = mm(w_q, x_attn, 1, 1).astype(BF16)
    latent = mm(x_attn, w_dkv, 1, 1)
    (c_kv, k_pe), kv_pull = jax.vjp(kv_prep, latent, g_kv)
    k_nope = mm(w_uk, c_kv, 1, 1).astype(BF16)
    value = mm(w_uv, c_kv, 1, 1).astype(BF16)
    k_pe_t = k_pe.T
    attn_out, lse = attend_fwd(query, k_nope, k_pe_t, value, cos_t, sin_t, heads)
    attn_part = mm(attn_out, w_o, 0, 0).astype(BF16)
    dy_full = gather(d_out_late)
    attn_part, dy_full = lax.optimization_barrier((attn_part, dy_full))
    residual, x_mlp = exchange_call(attn_out_body, 'attn_exchange', 2, [attn_part, embedded, gm], [loc, fullb], main)
    gate = mm(x_mlp, w_gate, 1, 1)
    up_proj = mm(x_mlp, w_up, 1, 1)
    gate_sig = jax.nn.sigmoid(gate)
    hidden = (gate * gate_sig * up_proj).astype(BF16)

    d_hidden = mm(dy_full, w_down, 1, 1)
    dw_down = mm(hidden, dy_full, 0, 0)
    d_up = (d_hidden * gate * gate_sig).astype(BF16)
    d_gate = (d_hidden * up_proj * gate_sig * (1.0 + gate * (1.0 - gate_sig))).astype(BF16)
    dw_gate = mm(d_gate, x_mlp, 0, 0)
    dw_up = mm(d_up, x_mlp, 0, 0)
    dx_part = (mm(d_gate, w_gate, 1, 0) + mm(d_up, w_up, 1, 0)).astype(BF16)
    d_residual, dg_mlp_part, d_attn_full = exchange_call(
        mlp_back_body, 'mlp_exchange', 3, [dx_part, residual, d_out, gm],
        [shape((local, width), F32), shape((1, width), F32), fullb], main)
    hidden_late, d_attn_full = lax.optimization_barrier((hidden, d_attn_full))
    mlp_loc = scatter(mm(hidden_late, w_down, 1, 0).astype(BF16))
    dw_o = mm(attn_out, d_attn_full, 1, 0)
    d_attn_out = mm(w_o, d_attn_full, 1, 1).astype(BF16)
    d_query, d_knope, d_value, d_kpe = attend_bwd(query, k_nope, k_pe_t, value, cos_t, sin_t, lse, d_attn_out, heads)
    dw_uk = mm(d_knope, c_kv, 1, 0)
    dw_uv = mm(d_value, c_kv, 1, 0)
    d_ckv = (mm(d_knope, w_uk, 0, 0) + mm(d_value, w_uv, 0, 0)).astype(BF16)
    d_latent, dg_kv_part = kv_pull((d_ckv, d_kpe.T.astype(BF16)))
    d_latent = d_latent.astype(BF16)
    dw_q = mm(d_query, x_attn, 1, 0)
    dx_part = (mm(d_query, w_q, 0, 0) + mm(d_latent, w_dkv, 1, 0)).astype(BF16)
    dx_part, mlp_loc = lax.optimization_barrier((dx_part, mlp_loc))
    layer_out = (residual.astype(F32) + mlp_loc.astype(F32)).astype(BF16)
    lat_w = 384
    lat_part = jnp.pad(d_latent, ((0, 0), (0, lat_w - d_latent.shape[1])))
    dma = pltpu.SemaphoreType.DMA
    dg, de_full, lat_full = exchange_call(
        attn_back_body, 'back_exchange', 4, [dx_part, lat_part, embedded, d_residual, ga, dg_mlp_part, dg_kv_part[None, :]],
        [shape((1, 2 * width + lora), F32), fullb, shape((seq, lat_w), BF16)],
        [VM((local, width), F32), VM((local, lat_w), F32), VM((8, 1, 2 * width + lora), F32), dma((7,)), dma((7,))] + ex_scratch([width, lat_w], LAST, local))
    dw_dkv = mm(lat_full[:, :lora + rope], x_attn, 0, 0)
    dg_attn, dg_mlp, dg_kv = dg[0, :width], dg[0, width:2 * width], dg[0, 2 * width:]
    return layer_out, de_full, (dw_q, dw_dkv, dg_kv, dw_uk, dw_uv, dw_o, dg_attn, dg_mlp, dw_gate, dw_up, dw_down)


def rows_of(w):
    return jnp.transpose(w, (1, 2, 0)).reshape(-1, w.shape[0])


def unrows(g, heads):
    return jnp.transpose(g.reshape(heads, -1, g.shape[1]), (2, 0, 1))


def solution(mesh):
    def device_step(tokens, embed_table, w_q, w_dkv, g_kv, w_uk, w_uv, w_o, g_attn, g_mlp, w_gate, w_up, w_down, d_out):
        vocab_local, model_dim = embed_table.shape
        heads = w_q.shape[1]
        key, blocks, count = block_index(tokens, vocab_local)
        rows = gather_rows(key, blocks, count, embed_table)
        layer_out, de_full, grads = layer_pass(
            rows, d_out[0], (rows_of(w_q), heads), w_dkv.T, g_kv, rows_of(w_uk), rows_of(w_uv), w_o.reshape(-1, model_dim),
            g_attn, g_mlp, w_gate.T, w_up.T, w_down)
        d_table = table_grad(key, blocks, count, de_full, vocab_local)
        dw_q, dw_dkv, dg_kv, dw_uk, dw_uv, dw_o, dg_attn, dg_mlp, dw_gate, dw_up, dw_down = grads
        return (layer_out[None], d_table, unrows(dw_q, heads), dw_dkv.T, dg_kv, unrows(dw_uk, heads), unrows(dw_uv, heads),
                dw_o.reshape(w_o.shape), dg_attn, dg_mlp, dw_gate.T, dw_up.T, dw_down)

    row_spec = P('dp', 'tp', None)
    head_spec = P(None, 'tp', None)
    in_specs = (P('dp', None), P('tp', None), head_spec, P(None, None), P(None), head_spec, head_spec, P('tp', None, None), P(None), P(None), P(None, 'tp'), P(None, 'tp'), P('tp', None), row_spec)
    out_specs = (row_spec, P(('dp', 'tp'), None), P('dp', 'tp', None), P('dp', None), P('dp'), P('dp', 'tp', None), P('dp', 'tp', None), P(('dp', 'tp'), None, None), P('dp'), P('dp'), P('dp', 'tp'), P('dp', 'tp'), P(('dp', 'tp'), None))
    return jax.shard_map(device_step, mesh=mesh, in_specs=in_specs, out_specs=out_specs, check_vma=False)
```

```python
import functools

import jax
import jax.numpy as jnp
from jax import lax
from jax.experimental import pallas as pl
from jax.experimental.pallas import tpu as pltpu
from jax.sharding import PartitionSpec as P

EPSILON = 1e-6
ROPE_BASE = 10000.0
F32, BF16 = jnp.float32, jnp.bfloat16
LOG2E = 1.4426950408889634
VM = pltpu.VMEM
ZR = 248
GB = 64
QB = 256


def mm(lhs, rhs, lc, rc):
    return lax.dot_general(lhs, rhs, (((lc,), (rc,)), ((), ())), preferred_element_type=F32)


def nn(a, b):
    return mm(a, b, 1, 0)


def nt(a, b):
    return mm(a, b, 1, 1)


def tn(a, b):
    return mm(a, b, 0, 0)


def rope_tables(seq_len, rope_dim):
    inv_freq = ROPE_BASE ** (-jnp.arange(0, rope_dim, 2, dtype=F32) / rope_dim)
    angles = jnp.arange(seq_len, dtype=F32)[:, None] * inv_freq[None, :]
    return jnp.cos(angles), jnp.sin(angles)


def apply_rope(x_in, cos_t, sin_t):
    half_dim = x_in.shape[-1] // 2
    x_lo, x_hi = x_in[..., :half_dim], x_in[..., half_dim:]
    return jnp.concatenate([x_lo * cos_t - x_hi * sin_t, x_hi * cos_t + x_lo * sin_t], axis=-1)


def rms_norm(x_in, gain):
    inv_rms = lax.rsqrt(jnp.mean(x_in * x_in, axis=-1, keepdims=True) + EPSILON)
    return (x_in * inv_rms * gain).astype(BF16)


def kv_prep(latent, g_kv):
    lora = g_kv.shape[0]
    cos_t, sin_t = rope_tables(latent.shape[0], latent.shape[-1] - lora)
    k_pe = apply_rope(latent[:, lora:], cos_t, sin_t).astype(BF16)
    return rms_norm(latent[:, :lora], g_kv), k_pe


def block_index(tokens, vocab_local):
    ids = tokens.reshape(-1) - lax.axis_index('tp') * vocab_local
    n = ids.shape[0]
    owned = (ids >= 0) & (ids < vocab_local)
    blk = jnp.where(owned, ids >> 3, -1)
    pos = jnp.arange(n, dtype=jnp.int32)
    eq = (blk[:, None] == blk[None, :])
    first = jnp.min(jnp.where(eq, pos[None, :], n), axis=1)
    isf = owned & (first == pos)
    slot = jnp.sum((isf[None, :] & (pos[None, :] < first[:, None])).astype(jnp.int32), axis=1)
    key = jnp.where(owned, slot * 8 + (ids & 7), -1)
    blocks = jnp.sum(jnp.where(isf[None, :] & (slot[None, :] == pos[:, None]), blk[None, :], 0), axis=1)
    count = jnp.sum(isf.astype(jnp.int32)).reshape(1)
    return key, blocks, count


def gather_body(count_ref, blocks_ref, key_ref, tail_ref, table_ref, out_ref, stage, sem):
    rows, width = out_ref.shape
    full = table_ref.shape[0] // 8
    stage[...] = jnp.zeros_like(stage)
    out_ref[...] = jnp.zeros_like(out_ref)
    count = count_ref[0]

    def fetch(b, i):
        return pltpu.make_async_copy(table_ref.at[pl.ds(pl.multiple_of(b * 8, 8), 8), :], stage.at[i], sem)

    def chunk(ci, carry):
        base = ci * GB
        n = jnp.minimum(GB, count - base)

        def start(i, c):
            b = blocks_ref[base + i]

            @pl.when(b < full)
            def _():
                fetch(b, i).start()

            @pl.when(b >= full)
            def _():
                stage[i] = tail_ref[...]
            return c

        def wait(i, c):
            b = blocks_ref[base + i]

            @pl.when(b < full)
            def _():
                fetch(b, i).wait()
            return c

        lax.fori_loop(0, n, start, 0)
        lax.fori_loop(0, n, wait, 0)
        cols = lax.broadcasted_iota(jnp.int32, (rows, GB * 8), 1) + base * 8
        hot = jnp.where(cols == key_ref[...], 1.0, 0.0).astype(BF16)
        for c in range(0, width, 512):
            got = nn(hot, stage[:, :, c:c + 512].reshape(GB * 8, 512))
            out_ref[:, c:c + 512] += got.astype(BF16)
        return carry

    lax.fori_loop(0, (count + GB - 1) // GB, chunk, 0)


def gather_rows(key, blocks, count, table):
    rows, (vocab, width) = key.shape[0], table.shape
    full = vocab // 8 * 8
    tail = jnp.pad(table[full:], ((0, 8 - (vocab - full)), (0, 0)))
    smem = pl.BlockSpec(memory_space=pltpu.SMEM)
    return pl.pallas_call(
        gather_body, out_shape=jax.ShapeDtypeStruct((rows, width), BF16),
        in_specs=[smem, smem, pl.BlockSpec(memory_space=VM), pl.BlockSpec(memory_space=VM), pl.BlockSpec(memory_space=pl.ANY)],
        out_specs=pl.BlockSpec(memory_space=VM),
        scratch_shapes=[VM((GB, 8, width), BF16), pltpu.SemaphoreType.DMA],
        compiler_params=pltpu.CompilerParams(vmem_limit_bytes=40 << 20), name='gather_rows',
    )(count, blocks, key[:, None], tail, table)


def table_grad_body(count_ref, blocks_ref, key_ref, de_ref, zeros_ref, out_ref, tail_ref, stage, sem):
    rows, width = de_ref.shape
    vocab = out_ref.shape[0]
    full = vocab // 8
    tail_ref[...] = jnp.zeros_like(tail_ref)
    count = count_ref[0]

    def put(b, i):
        return pltpu.make_async_copy(stage.at[i], out_ref.at[pl.ds(pl.multiple_of(b * 8, 8), 8), :], sem)

    def sums(ci):
        ids = lax.broadcasted_iota(jnp.int32, (GB * 8, rows), 0) + ci * (GB * 8)
        hot = jnp.where(ids == key_ref[...], 1.0, 0.0).astype(BF16)
        for c in range(0, width, 512):
            got = nn(hot, de_ref[:, c:c + 512])
            stage[:, :, c:c + 512] = got.astype(BF16).reshape(GB, 8, 512)

    def move(ci, go):
        base = ci * GB

        def one(i, c):
            b = blocks_ref[base + i]

            @pl.when(b < full)
            def _():
                go(put(b, i))
            @pl.when(b >= full)
            def _():
                tail_ref[...] = stage[i]
            return c

        lax.fori_loop(0, jnp.minimum(GB, count - base), one, 0)

    def chunk(ci, carry):
        sums(ci)
        move(ci, lambda cp: cp.start())
        move(ci, lambda cp: cp.wait())
        return carry

    lax.fori_loop(0, (count + GB - 1) // GB, chunk, 0)


def table_grad(key, blocks, count, de_full, table):
    vocab, width = table.shape
    smem = pl.BlockSpec(memory_space=pltpu.SMEM)
    full = vocab // 8 * 8
    out, tail = pl.pallas_call(
        table_grad_body, out_shape=[jax.ShapeDtypeStruct((vocab, width), BF16), jax.ShapeDtypeStruct((8, width), BF16)],
        in_specs=[smem, smem, pl.BlockSpec(memory_space=VM), pl.BlockSpec(memory_space=VM), pl.BlockSpec(memory_space=pl.ANY)], input_output_aliases={4: 0},
        out_specs=[pl.BlockSpec(memory_space=pl.ANY), pl.BlockSpec(memory_space=VM)],
        scratch_shapes=[VM((GB, 8, width), BF16), pltpu.SemaphoreType.DMA],
        compiler_params=pltpu.CompilerParams(vmem_limit_bytes=40 << 20), name='table_grad',
    )(count, blocks, key[None, :], de_full, table)
    return lax.dynamic_update_slice(out, tail[:vocab - full], (full, 0))


def heads_of(q_ref, kn_ref, kp_ref, cos_ref, sin_ref, nope, half):
    q_pe = q_ref[nope:, :].astype(F32)
    lo, hi, cos_t, sin_t = q_pe[:half], q_pe[half:], cos_ref[...], sin_ref[...]
    q_all = jnp.concatenate([q_ref[:nope, :], (lo * cos_t - hi * sin_t).astype(BF16), (hi * cos_t + lo * sin_t).astype(BF16)], axis=0)
    return q_all, jnp.concatenate([kn_ref[...], kp_ref[...]], axis=0)


def scores_of(k_all, q_all, ki, qi, scale):
    s = tn(k_all[:, ki * QB:(ki + 1) * QB], q_all[:, qi * QB:(qi + 1) * QB]) * scale
    if ki == qi:
        keys = lax.broadcasted_iota(jnp.int32, (QB, QB), 0)
        s = jnp.where(keys <= lax.broadcasted_iota(jnp.int32, (QB, QB), 1), s, -1e30)
    return s


def attn_fwd_body(q_ref, kn_ref, kp_ref, v_ref, cos_ref, sin_ref, o_ref, lse_ref):
    nope, half = kn_ref.shape[0], cos_ref.shape[0]
    scale = q_ref.shape[0] ** -0.5 * LOG2E
    q_all, k_all = heads_of(q_ref, kn_ref, kp_ref, cos_ref, sin_ref, nope, half)
    for qi in range(q_ref.shape[1] // QB):
        lanes = slice(qi * QB, (qi + 1) * QB)
        s = [scores_of(k_all, q_all, ki, qi, scale) for ki in range(qi + 1)]
        top = functools.reduce(jnp.maximum, [jnp.max(x, axis=0, keepdims=True) for x in s])
        p = [jnp.exp2(x - top) for x in s]
        total = sum(jnp.sum(x, axis=0, keepdims=True) for x in p)
        inv = 1.0 / total
        o = sum(nn(v_ref[:, ki * QB:(ki + 1) * QB], (x * inv).astype(BF16)) for ki, x in enumerate(p))
        o_ref[:, lanes] = o.astype(BF16)
        lse_ref[0, :, lanes] = top + jnp.log2(total)


def attn_bwd_body(q_ref, kn_ref, kp_ref, v_ref, cos_ref, sin_ref, lse_ref, do_ref, dq_ref, dkn_ref, dv_ref, dkp_ref, table_ref, dk_acc, dv_acc, zero, zsem):
    full = table_ref.shape[0] // 8 * 8
    fills = [pltpu.make_async_copy(zero.at[pl.ds(0, n), :], table_ref.at[pl.ds(r, n), :], zsem.at[k])
             for k, (r, n) in enumerate((r, min(ZR, full - r)) for r in range(0, full, ZR))]

    @pl.when(pl.program_id(0) == 0)
    def _():
        zero[...] = jnp.zeros_like(zero)
        for cp in fills:
            cp.start()

    nope, half = kn_ref.shape[0], cos_ref.shape[0]
    raw = q_ref.shape[0] ** -0.5
    q_all, k_all = heads_of(q_ref, kn_ref, kp_ref, cos_ref, sin_ref, nope, half)
    dk_acc[...] = jnp.zeros_like(dk_acc)
    dv_acc[...] = jnp.zeros_like(dv_acc)
    for qi in range(q_ref.shape[1] // QB):
        lanes = slice(qi * QB, (qi + 1) * QB)
        q_b, do_b, lse = q_all[:, lanes], do_ref[:, lanes], lse_ref[0, :, lanes]
        p = [jnp.exp2(scores_of(k_all, q_all, ki, qi, raw * LOG2E) - lse) for ki in range(qi + 1)]
        dp = [tn(v_ref[:, ki * QB:(ki + 1) * QB], do_b) for ki in range(qi + 1)]
        delta = sum(jnp.sum(a * b, axis=0, keepdims=True) for a, b in zip(p, dp))
        dq = None
        for ki in range(qi + 1):
            keys = slice(ki * QB, (ki + 1) * QB)
            ds = (p[ki] * (dp[ki] - delta) * raw).astype(BF16)
            part = nn(k_all[:, keys], ds)
            dq = part if dq is None else dq + part
            dk_acc[:, keys] += nt(q_b, ds)
            dv_acc[:, keys] += nt(do_b, p[ki].astype(BF16))
        cos_t, sin_t = cos_ref[:, lanes], sin_ref[:, lanes]
        lo, hi = dq[nope:nope + half], dq[nope + half:]
        dq_ref[:nope, lanes] = dq[:nope].astype(BF16)
        dq_ref[nope:nope + half, lanes] = (lo * cos_t + hi * sin_t).astype(BF16)
        dq_ref[nope + half:, lanes] = (hi * cos_t - lo * sin_t).astype(BF16)
    dkn_ref[...] = dk_acc[:nope, :].astype(BF16)
    dv_ref[...] = dv_acc[...].astype(BF16)

    @pl.when(pl.program_id(0) == 0)
    def _():
        dkp_ref[...] = jnp.zeros_like(dkp_ref)
    dkp_ref[...] += dk_acc[nope:, :]

    @pl.when(pl.program_id(0) == pl.num_programs(0) - 1)
    def _():
        for cp in fills:
            cp.wait()


def attn_specs(heads, qd, nope, rope, vd, seq):
    per = lambda r: pl.BlockSpec((r, seq), lambda h: (h, 0))
    one = lambda r: pl.BlockSpec((r, seq), lambda h: (0, 0))
    return [per(qd), per(nope), one(rope), per(vd), one(rope // 2), one(rope // 2)], per, one, pl.BlockSpec((1, 1, seq), lambda h: (h, 0, 0))


def attend_fwd(q, kn, kp, v, cos_t, sin_t, heads):
    seq, qd, nope, vd, rope = q.shape[1], q.shape[0] // heads, kn.shape[0] // heads, v.shape[0] // heads, kp.shape[0]
    ins, per, one, lse = attn_specs(heads, qd, nope, rope, vd, seq)
    return pl.pallas_call(
        attn_fwd_body, grid=(heads,), in_specs=ins, out_specs=[per(vd), lse],
        out_shape=[jax.ShapeDtypeStruct((heads * vd, seq), BF16), jax.ShapeDtypeStruct((heads, 1, seq), F32)],
        compiler_params=pltpu.CompilerParams(vmem_limit_bytes=40 << 20), name='attend_fwd',
    )(q, kn, kp, v, cos_t, sin_t)


def attend_bwd(q, kn, kp, v, cos_t, sin_t, lse, do, heads, table):
    seq, qd, nope, vd, rope = q.shape[1], q.shape[0] // heads, kn.shape[0] // heads, v.shape[0] // heads, kp.shape[0]
    ins, per, one, lse_spec = attn_specs(heads, qd, nope, rope, vd, seq)
    return pl.pallas_call(
        attn_bwd_body, grid=(heads,), in_specs=ins + [lse_spec, per(vd)], out_specs=[per(qd), per(nope), per(vd), one(rope), pl.BlockSpec(memory_space=pl.ANY)],
        out_shape=[jax.ShapeDtypeStruct(q.shape, BF16), jax.ShapeDtypeStruct(kn.shape, BF16), jax.ShapeDtypeStruct(v.shape, BF16), jax.ShapeDtypeStruct(kp.shape, F32), jax.ShapeDtypeStruct(table, BF16)],
        scratch_shapes=[VM((qd, seq), F32), VM((vd, seq), F32), VM((ZR, table[1]), BF16), pltpu.SemaphoreType.DMA((-(-table[0] // ZR),))],
        compiler_params=pltpu.CompilerParams(vmem_limit_bytes=40 << 20), name='attend_bwd',
    )(q, kn, kp, v, cos_t, sin_t, lse, do)


def shift(x, bit):
    return lax.ppermute(x, 'tp', [(d, d ^ bit) for d in range(8)])


PAIR, XBIT, YBIT = 1, 2, 4


def coords():
    me = lax.axis_index('tp')
    return me // YBIT, (me // XBIT) % 2, me % 2


def pick(x, i, axis):
    return lax.dynamic_index_in_dim(x, i, axis, keepdims=False)


def added(a, b):
    return (a.astype(F32) + b.astype(F32)).astype(BF16)


def scatter_hops(part, local):
    y, x, core = coords()
    half = part.shape[1] // 2
    p = part.reshape(2, 2, 2, local, part.shape[1])
    q = added(pick(p, core, 2), shift(pick(p, 1 - core, 2), PAIR))
    a, b = q[..., :half], q[..., half:]
    a = added(pick(a, x, 1), shift(pick(a, 1 - x, 1), XBIT))
    b = added(pick(b, y, 0), shift(pick(b, 1 - y, 0), YBIT))
    a = pick(a, y, 0).astype(F32) + shift(pick(a, 1 - y, 0), YBIT).astype(F32)
    b = pick(b, x, 0).astype(F32) + shift(pick(b, 1 - x, 0), XBIT).astype(F32)
    return jnp.concatenate([a, b], axis=1)


def gather_hops(blk):
    half = blk.shape[1] // 2
    bx, by = shift(blk, XBIT), shift(blk, YBIT)
    near = jnp.concatenate([blk, bx, by])
    diag = jnp.concatenate([shift(by[:, :half], XBIT), shift(bx[:, half:], YBIT)], axis=1)
    return jnp.concatenate([near, diag, shift(near, PAIR), shift(diag, PAIR)])


def hop_order():
    me = lax.axis_index('tp')
    flip = lambda v, bit: v + bit - 2 * bit * ((v // bit) % 2)
    own = [me, flip(me, XBIT), flip(me, YBIT), flip(flip(me, XBIT), YBIT)]
    return own + [flip(d, PAIR) for d in own]


def to_hop_order(x, axis):
    n = x.shape[axis] // 8
    return jnp.concatenate([lax.dynamic_slice_in_dim(x, d * n, n, axis) for d in hop_order()], axis=axis)


def from_hop_order(x):
    n = x.shape[0] // 8
    out = jnp.zeros_like(x)
    for k, d in enumerate(hop_order()):
        out = lax.dynamic_update_slice_in_dim(out, x[k * n:(k + 1) * n], d * n, 0)
    return out


def sum_hops(x):
    for bit in (PAIR, XBIT, YBIT):
        x = x + shift(x, bit)
    return x


class Exchange:
    def __init__(self, widths, pieces):
        self.widths, self.pieces = widths, pieces
        self.order = range(len(pieces))

    def rs_scratch(self, rows):
        n = len(self.pieces)
        out = []
        for w in self.widths:
            out += [VM((4, rows, w), BF16), VM((2, rows, w), BF16), VM((2, rows, w), BF16), VM((rows, w), BF16), VM((rows, w), BF16)]
        dma = pltpu.SemaphoreType.DMA
        return out + [dma((4, n)), dma((4, n)), dma((2, n)), dma((2, n)), dma((n,)), dma((n,))]

    def ag_scratch(self):
        n = len(self.pieces)
        dma = pltpu.SemaphoreType.DMA
        return [dma((2, n)), dma((2, n)), dma((n,)), dma((n,)), dma((4, n)), dma((4, n))]

    def place(self, rows):
        me = lax.axis_index('tp')
        core, x, y = me % 2, (me // 2) % 2, me // 4
        dev = lambda yy, xx, cc: (yy * 2 + xx) * 2 + cc
        self.me, self.rows = me, rows
        self.pn, self.xn, self.yn = dev(y, x, 1 - core), dev(y, 1 - x, core), dev(1 - y, x, core)
        chips = [(y, x), (y, 1 - x), (1 - y, x), (1 - y, 1 - x)]
        at = lambda d: pl.ds(pl.multiple_of(d * rows, rows), rows)
        self.mine = [at(dev(*ch, core)) for ch in chips]
        self.theirs = [at(dev(*ch, 1 - core)) for ch in chips]
        self.chip = [pl.ds(pl.multiple_of(dev(*ch, 0) * rows, 2 * rows), 2 * rows) for ch in chips]

    def enter(self):
        sem = pltpu.get_barrier_semaphore()
        near = (self.pn, self.xn, self.yn)
        for d in near:
            pl.semaphore_signal(sem, inc=1, device_id={'tp': d}, device_id_type=pl.DeviceIdType.MESH)
        pl.semaphore_wait(sem, len(near))

    def copy(self, src, dst, ssem, rsem, dev):
        return pltpu.make_async_remote_copy(src_ref=src, dst_ref=dst, send_sem=ssem, recv_sem=rsem, device_id={'tp': dev}, device_id_type=pl.DeviceIdType.MESH)

    def rs_begin(self, parts, scratch):
        na = len(self.widths)
        self.parts = parts
        self.bufs = [scratch[5 * a:5 * a + 5] for a in range(na)]
        ds, dr, s1, r1, s2, r2 = scratch[5 * na:5 * na + 6]
        self.pair, self.hop1, self.hop2 = {}, {}, {}
        for i, (h, a, c0, cn) in enumerate(self.pieces):
            cols = pl.ds(c0, cn)
            dbuf, sb1, rb1, sb2, rb2 = self.bufs[a]
            for j in range(4):
                self.pair[j, i] = self.copy(parts[a].at[self.theirs[j], cols], dbuf.at[j, :, cols], ds.at[j, i], dr.at[j, i], self.pn)
            to1, to2 = (self.xn, self.yn) if h == 0 else (self.yn, self.xn)
            for k in range(2):
                self.hop1[k, i] = self.copy(sb1.at[k, :, cols], rb1.at[k, :, cols], s1.at[k, i], r1.at[k, i], to1)
            self.hop2[i] = self.copy(sb2.at[:, cols], rb2.at[:, cols], s2.at[i], r2.at[i], to2)

    def ready(self, j):
        for i in self.order:
            self.pair[j, i].start()

    def chip_sum(self, j, i):
        h, a, c0, cn = self.pieces[i]
        self.pair[j, i].wait_recv()
        return self.parts[a][self.mine[j], c0:c0 + cn].astype(F32) + self.bufs[a][0][j, :, c0:c0 + cn].astype(F32)

    def push(self, j):
        for i in self.order:
            h, a, c0, cn = self.pieces[i]
            if j == 3 or j == 1 + h:
                k = 1 if j == 3 else 0
                self.bufs[a][1][k, :, c0:c0 + cn] = self.chip_sum(j, i).astype(BF16)
                self.hop1[k, i].start()

    def relay(self):
        for i in self.order:
            h, a, c0, cn = self.pieces[i]
            own = self.chip_sum(2 - h, i)
            self.hop1[1, i].wait_recv()
            self.bufs[a][3][:, c0:c0 + cn] = (own + self.bufs[a][2][1, :, c0:c0 + cn].astype(F32)).astype(BF16)
            self.hop2[i].start()

    def land(self, accs):
        for i in self.order:
            h, a, c0, cn = self.pieces[i]
            own = self.chip_sum(0, i)
            self.hop1[0, i].wait_recv()
            own = own + self.bufs[a][2][0, :, c0:c0 + cn].astype(F32)
            self.hop2[i].wait_recv()
            accs[a][:, c0:c0 + cn] = own + self.bufs[a][4][:, c0:c0 + cn].astype(F32)

    def drain(self):
        for cp in list(self.pair.values()) + list(self.hop1.values()) + list(self.hop2.values()):
            cp.wait_send()

    def reduce_scatter(self, accs, produce):
        late = None
        for j in (3, 1, 2, 0):
            produce(j)
            self.ready(j)
            if late:
                self.push(late)
            late = j
        self.relay()
        self.land(accs)

    def all_gather(self, fulls, scratch, arrive):
        os_, xr, fs, fr, ps, pr = scratch
        half0 = [i for i in self.order if self.pieces[i][0] == 0]
        half1 = [i for i in self.order if self.pieces[i][0] == 1]

        def to(i, j, ssem, rsem, dev, rows=None):
            h, a, c0, cn = self.pieces[i]
            ref = fulls[a].at[(rows or self.mine)[j], pl.ds(c0, cn)]
            return self.copy(ref, ref, ssem, rsem, dev)

        near = (self.xn, self.yn)
        own = [[to(i, 0, os_.at[k, i], xr.at[k, i], dev) for i in self.order] for k, dev in enumerate(near)]
        from_n = [[to(i, 1 + k, os_.at[k, i], xr.at[k, i], dev) for i in self.order] for k, dev in enumerate(near)]
        fwd = [to(i, 2 - self.pieces[i][0], fs.at[i], fr.at[i], near[self.pieces[i][0]]) for i in self.order]
        diag = [to(i, 3, fs.at[i], fr.at[i], self.xn) for i in self.order]
        give = [[to(i, j, ps.at[j, i], pr.at[j, i], self.pn) for i in self.order] for j in range(4)]
        take = [[to(i, j, ps.at[j, i], pr.at[j, i], self.pn, self.theirs) for i in self.order] for j in range(4)]
        for i0, i1 in zip(half0, half1):
            own[0][i1].start()
            own[1][i0].start()
        for i0, i1 in zip(half0, half1):
            own[0][i0].start()
            own[1][i1].start()
        for cp in give[0]:
            cp.start()
        for cp in take[0]:
            cp.wait_recv()
        arrive(0)
        for i0, i1 in zip(half0, half1):
            from_n[1][i0].wait_recv()
            fwd[i0].start()
            give[2][i0].start()
            from_n[0][i1].wait_recv()
            fwd[i1].start()
            give[1][i1].start()
        for i0, i1 in zip(half0, half1):
            from_n[1][i1].wait_recv()
            give[2][i1].start()
            from_n[0][i0].wait_recv()
            give[1][i0].start()
        for j in (1, 2):
            for cp in take[j]:
                cp.wait_recv()
            arrive(j)
        for i in self.order:
            diag[i].wait_recv()
            give[3][i].start()
        for cp in take[3]:
            cp.wait_recv()
        arrive(3)
        for cp in own[0] + own[1] + fwd + [c for g in give for c in g]:
            cp.wait_send()


def halves(width, n):
    step = width // (2 * n)
    return [(h, 0, (h * n + k) * step, step) for k in range(n) for h in range(2)]


MAIN = halves(2560, 2)
LAST = MAIN + [(0, 1, 0, 256), (1, 1, 256, 128)]
NRS = 11


def norm_rows(x, gain):
    return x * lax.rsqrt(jnp.mean(x * x, axis=-1, keepdims=True) + EPSILON) * gain


def norm_rows_vjp(x, gain, dy):
    r = lax.rsqrt(jnp.mean(x * x, axis=-1, keepdims=True) + EPSILON)
    gd = dy * gain
    dot = jnp.mean(gd * x, axis=-1, keepdims=True)
    return r * gd - x * (r * r * r * dot), jnp.sum(dy * x * r, axis=0, keepdims=True)


def exchange_call(body, name, cid, ins, out_shape, scratch):
    vmem = pl.BlockSpec(memory_space=VM)
    return pl.pallas_call(
        body, out_shape=out_shape, in_specs=[vmem] * len(ins), out_specs=[vmem] * len(out_shape), scratch_shapes=scratch,
        compiler_params=pltpu.CompilerParams(vmem_limit_bytes=50 << 20, collective_id=cid, has_side_effects=True), name=name)(*ins)


def shape(dims, dtype):
    return jax.ShapeDtypeStruct(dims, dtype)


def idle(j):
    pass


def embed_body(part, gain, wq, wdkv, e_ref, full, q_ref, lat_ref, acc, *scratch):
    ex = Exchange([part.shape[1]], MAIN)
    ex.place(acc.shape[0])
    ex.enter()
    ex.rs_begin([part], scratch)
    ex.reduce_scatter([acc], idle)
    e = acc[...].astype(BF16)
    e_ref[...] = e
    full[ex.mine[0], :] = norm_rows(e.astype(F32), gain[...]).astype(BF16)

    def arrive(j):
        u = full[ex.chip[j], :]
        q_ref[:, ex.chip[j]] = nt(wq[...], u).astype(BF16)
        lat_ref[ex.chip[j], :] = nt(u, wdkv[...])

    ex.all_gather([full], scratch[NRS:], arrive)
    ex.drain()


def attn_out_body(o_ref, wo, e_ref, gain, h_ref, full, part, acc, *scratch):
    ex = Exchange([part.shape[1]], MAIN)
    ex.place(acc.shape[0])
    ex.enter()
    ex.rs_begin([part], scratch)

    def produce(j):
        part[ex.chip[j], :] = tn(o_ref[:, ex.chip[j]], wo[...]).astype(BF16)

    ex.reduce_scatter([acc], produce)
    h = (e_ref[...].astype(F32) + acc[...].astype(BF16).astype(F32)).astype(BF16)
    h_ref[...] = h
    full[ex.mine[0], :] = norm_rows(h.astype(F32), gain[...]).astype(BF16)
    ex.all_gather([full], scratch[NRS:], idle)
    ex.drain()


def mlp_back_body(part, h_ref, dy_ref, gain, wo, dres_ref, dg_ref, full, do_ref, acc, *scratch):
    ex = Exchange([part.shape[1]], MAIN)
    ex.place(acc.shape[0])
    ex.enter()
    ex.rs_begin([part], scratch)
    ex.reduce_scatter([acc], idle)
    dx, dg = norm_rows_vjp(h_ref[...].astype(F32), gain[...], acc[...])
    dg_ref[...] = dg
    dres = dy_ref[...].astype(F32) + dx
    dres_ref[...] = dres
    full[ex.mine[0], :] = dres.astype(BF16)

    def arrive(j):
        do_ref[:, ex.chip[j]] = nt(wo[...], full[ex.chip[j], :]).astype(BF16)

    ex.all_gather([full], scratch[NRS:], arrive)
    ex.drain()


def attn_back_body(dq_ref, lat, wq, wdkv, e_ref, dres_ref, gain, de_ref, dlat_ref, dg_ref, part, acc, acc_lat, *scratch):
    ex = Exchange([part.shape[1], lat.shape[1]], LAST)
    ex.place(acc.shape[0])
    ex.enter()
    ex.rs_begin([part, lat], scratch)
    lw = wdkv.shape[0]

    def produce(j):
        rows = ex.chip[j]
        part[rows, :] = (tn(dq_ref[:, rows], wq[...]) + nn(lat[rows, :lw], wdkv[...])).astype(BF16)

    ex.reduce_scatter([acc, acc_lat], produce)
    dx, dg_ref[...] = norm_rows_vjp(e_ref[...].astype(F32), gain[...], acc[...])
    de_ref[...] = (dres_ref[...] + dx).astype(BF16)
    dlat_ref[...] = acc_lat[...].astype(BF16)
    ex.drain()


def layer_pass(rows, d_out, w_q, w_dkv, g_kv, w_uk, w_uv, w_o, g_attn, g_mlp, w_gate, w_up, w_down, vocab):
    w_q, heads = w_q
    seq, width = rows.shape
    local = d_out.shape[0]
    lora = g_kv.shape[0]
    latw = w_dkv.shape[0]
    one = Exchange([width], MAIN)
    main = [VM((local, width), F32)] + one.rs_scratch(local) + one.ag_scratch()
    partb = [VM((seq, width), BF16)]
    loc, fullb = shape((local, width), BF16), shape((seq, width), BF16)
    ga, gm = g_attn[None, :], g_mlp[None, :]
    embedded, x_attn, query, latent = exchange_call(
        embed_body, 'embed_exchange', 1, [rows, ga, w_q, w_dkv], [loc, fullb, shape((w_q.shape[0], seq), BF16), shape((seq, latw), F32)], main)
    d_out_late, latent = lax.optimization_barrier((d_out, latent))
    dy_full = from_hop_order(gather_hops(d_out_late))
    cos_t, sin_t = (t.T for t in rope_tables(seq, latw - lora))
    (c_kv, k_pe), kv_pull = jax.vjp(kv_prep, latent, g_kv)
    k_nope = nt(w_uk, c_kv).astype(BF16)
    value = nt(w_uv, c_kv).astype(BF16)
    k_pe_t = k_pe.T
    attn_out, lse = attend_fwd(query, k_nope, k_pe_t, value, cos_t, sin_t, heads)
    residual, x_mlp = exchange_call(attn_out_body, 'attn_exchange', 2, [attn_out, w_o, embedded, gm], [loc, fullb], partb + main)
    gate = nt(x_mlp, w_gate)
    up_proj = nt(x_mlp, w_up)
    gate_sig = jax.nn.sigmoid(gate)
    hidden = (gate * gate_sig * up_proj).astype(BF16)

    d_hidden = nt(dy_full, w_down)
    d_up = (d_hidden * gate * gate_sig).astype(BF16)
    d_gate = (d_hidden * up_proj * gate_sig * (1.0 + gate * (1.0 - gate_sig))).astype(BF16)
    dx_part = (nn(d_gate, w_gate) + nn(d_up, w_up)).astype(BF16)
    d_residual, dg_mlp, d_attn_full, d_attn_out = exchange_call(
        mlp_back_body, 'mlp_exchange', 3, [dx_part, residual, d_out, gm, w_o],
        [shape((local, width), F32), shape((1, width), F32), fullb, shape((w_o.shape[0], seq), BF16)], main)
    hidden_late, d_attn_full = lax.optimization_barrier((hidden, d_attn_full))
    mlp_loc = scatter_hops(nn(hidden_late, w_down).astype(BF16), local)
    layer_out = (residual.astype(F32) + mlp_loc.astype(BF16).astype(F32)).astype(BF16)
    d_query, d_knope, d_value, d_kpe, table0 = attend_bwd(query, k_nope, k_pe_t, value, cos_t, sin_t, lse, d_attn_out, heads, (vocab, width))
    d_ckv = (tn(d_knope, w_uk) + tn(d_value, w_uv)).astype(BF16)
    d_latent, dg_kv = kv_pull((d_ckv, d_kpe.T.astype(BF16)))
    lat_part = jnp.pad(d_latent.astype(BF16), ((0, 0), (0, -latw % 128)))
    padw = lat_part.shape[1]
    two = Exchange([width, padw], LAST)
    de, dlat, dg_attn = exchange_call(
        attn_back_body, 'back_exchange', 4, [d_query, lat_part, w_q, w_dkv, embedded, d_residual, ga],
        [loc, shape((local, padw), BF16), shape((1, width), F32)],
        partb + [VM((local, width), F32), VM((local, padw), F32)] + two.rs_scratch(local))
    hidden, d_gate, d_up, d_query_l, d_knope, d_value, attn_out, de = lax.optimization_barrier((hidden, d_gate, d_up, d_query, d_knope, d_value, attn_out, de))
    de_full = gather_hops(de)
    lat_full = from_hop_order(gather_hops(dlat))
    dw_down = tn(hidden, dy_full)
    dw_gate = tn(d_gate, x_mlp)
    dw_up = tn(d_up, x_mlp)
    dw_o = nn(attn_out, d_attn_full)
    dw_uk = nn(d_knope, c_kv)
    dw_uv = nn(d_value, c_kv)
    dw_q = nn(d_query_l, x_attn)
    dw_dkv = tn(lat_full[:, :latw], x_attn)
    dg = sum_hops(jnp.concatenate([dg_attn[0], dg_mlp[0], dg_kv]))
    dg_attn, dg_mlp, dg_kv = dg[:width], dg[width:2 * width], dg[2 * width:]
    return layer_out, de_full, table0, (dw_q, dw_dkv, dg_kv, dw_uk, dw_uv, dw_o, dg_attn, dg_mlp, dw_gate, dw_up, dw_down)


def rows_of(w):
    return jnp.transpose(w, (1, 2, 0)).reshape(-1, w.shape[0])


def unrows(g, heads):
    return jnp.transpose(g.reshape(heads, -1, g.shape[1]), (2, 0, 1))


def solution(mesh):
    def device_step(tokens, embed_table, w_q, w_dkv, g_kv, w_uk, w_uv, w_o, g_attn, g_mlp, w_gate, w_up, w_down, d_out):
        vocab_local, model_dim = embed_table.shape
        heads = w_q.shape[1]
        key, blocks, count = block_index(tokens, vocab_local)
        rows = gather_rows(key, blocks, count, embed_table)
        layer_out, de_full, table0, grads = layer_pass(
            rows, d_out[0], (rows_of(w_q), heads), w_dkv.T, g_kv, rows_of(w_uk), rows_of(w_uv), w_o.reshape(-1, model_dim),
            g_attn, g_mlp, w_gate.T, w_up.T, w_down, vocab_local)
        d_table = table_grad(to_hop_order(key, 0), blocks, count, de_full, table0)
        dw_q, dw_dkv, dg_kv, dw_uk, dw_uv, dw_o, dg_attn, dg_mlp, dw_gate, dw_up, dw_down = grads
        return (layer_out[None], d_table, unrows(dw_q, heads), dw_dkv.T, dg_kv, unrows(dw_uk, heads), unrows(dw_uv, heads),
                dw_o.reshape(w_o.shape), dg_attn, dg_mlp, dw_gate.T, dw_up.T, dw_down)

    row_spec = P('dp', 'tp', None)
    head_spec = P(None, 'tp', None)
    in_specs = (P('dp', None), P('tp', None), head_spec, P(None, None), P(None), head_spec, head_spec, P('tp', None, None), P(None), P(None), P(None, 'tp'), P(None, 'tp'), P('tp', None), row_spec)
    out_specs = (row_spec, P(('dp', 'tp'), None), P('dp', 'tp', None), P('dp', None), P('dp'), P('dp', 'tp', None), P('dp', 'tp', None), P(('dp', 'tp'), None, None), P('dp'), P('dp'), P('dp', 'tp'), P('dp', 'tp'), P(('dp', 'tp'), None))
    return jax.shard_map(device_step, mesh=mesh, in_specs=in_specs, out_specs=out_specs, check_vma=False)
```

```python
import functools

import jax
import jax.numpy as jnp
from jax import lax
from jax.experimental import pallas as pl
from jax.experimental.pallas import tpu as pltpu
from jax.sharding import PartitionSpec as P

EPSILON = 1e-6
ROPE_BASE = 10000.0
F32, BF16 = jnp.float32, jnp.bfloat16
LOG2E = 1.4426950408889634
VM = pltpu.VMEM
ZR = 248
GB = 64
QB = 256


def mm(lhs, rhs, lc, rc):
    return lax.dot_general(lhs, rhs, (((lc,), (rc,)), ((), ())), preferred_element_type=F32)


def nn(a, b):
    return mm(a, b, 1, 0)


def nt(a, b):
    return mm(a, b, 1, 1)


def tn(a, b):
    return mm(a, b, 0, 0)


mean_last = functools.partial(jnp.mean, axis=-1, keepdims=True)
sum_rows = functools.partial(jnp.sum, axis=0, keepdims=True)


def rope_tables(seq_len, rope_dim):
    inv_freq = ROPE_BASE ** (-jnp.arange(0, rope_dim, 2, dtype=F32) / rope_dim)
    angles = jnp.arange(seq_len, dtype=F32)[:, None] * inv_freq[None, :]
    return jnp.cos(angles), jnp.sin(angles)


def apply_rope(x_in, cos_t, sin_t):
    half_dim = x_in.shape[-1] // 2
    x_lo, x_hi = x_in[..., :half_dim], x_in[..., half_dim:]
    return jnp.concatenate([x_lo * cos_t - x_hi * sin_t, x_hi * cos_t + x_lo * sin_t], axis=-1)


def rms_norm(x_in, gain):
    inv_rms = lax.rsqrt(mean_last(x_in * x_in) + EPSILON)
    return (x_in * inv_rms * gain).astype(BF16)


def kv_prep(latent, g_kv):
    lora = g_kv.shape[0]
    cos_t, sin_t = rope_tables(latent.shape[0], latent.shape[-1] - lora)
    k_pe = apply_rope(latent[:, lora:], cos_t, sin_t).astype(BF16)
    return rms_norm(latent[:, :lora], g_kv), k_pe


def block_index(tokens, vocab_local):
    ids = tokens.reshape(-1) - lax.axis_index('tp') * vocab_local
    n = ids.shape[0]
    owned = (ids >= 0) & (ids < vocab_local)
    blk = jnp.where(owned, ids >> 3, -1)
    pos = jnp.arange(n, dtype=jnp.int32)
    eq = (blk[:, None] == blk[None, :])
    first = jnp.min(jnp.where(eq, pos[None, :], n), axis=1)
    isf = owned & (first == pos)
    slot = jnp.sum((isf[None, :] & (pos[None, :] < first[:, None])).astype(jnp.int32), axis=1)
    key = jnp.where(owned, slot * 8 + (ids & 7), -1)
    blocks = jnp.sum(jnp.where(isf[None, :] & (slot[None, :] == pos[:, None]), blk[None, :], 0), axis=1)
    count = jnp.sum(isf.astype(jnp.int32)).reshape(1)
    return key, blocks, count


def gather_body(count_ref, blocks_ref, key_ref, tail_ref, table_ref, out_ref, stage, sem):
    rows, width = out_ref.shape
    full = table_ref.shape[0] // 8
    stage[...] = jnp.zeros_like(stage)
    out_ref[...] = jnp.zeros_like(out_ref)
    count = count_ref[0]

    def fetch(b, i):
        return pltpu.make_async_copy(table_ref.at[pl.ds(pl.multiple_of(b * 8, 8), 8), :], stage.at[i], sem)

    def chunk(ci, carry):
        base = ci * GB
        n = jnp.minimum(GB, count - base)

        def start(i, c):
            b = blocks_ref[base + i]

            @pl.when(b < full)
            def _():
                fetch(b, i).start()

            @pl.when(b >= full)
            def _():
                stage[i] = tail_ref[...]
            return c

        def wait(i, c):
            b = blocks_ref[base + i]

            @pl.when(b < full)
            def _():
                fetch(b, i).wait()
            return c

        lax.fori_loop(0, n, start, 0)
        lax.fori_loop(0, n, wait, 0)
        cols = lax.broadcasted_iota(jnp.int32, (rows, GB * 8), 1) + base * 8
        hot = jnp.where(cols == key_ref[...], 1.0, 0.0).astype(BF16)
        for c in range(0, width, 512):
            got = nn(hot, stage[:, :, c:c + 512].reshape(GB * 8, 512))
            out_ref[:, c:c + 512] += got.astype(BF16)
        return carry

    lax.fori_loop(0, (count + GB - 1) // GB, chunk, 0)


def gather_rows(key, blocks, count, table):
    rows, (vocab, width) = key.shape[0], table.shape
    full = vocab // 8 * 8
    tail = jnp.pad(table[full:], ((0, 8 - (vocab - full)), (0, 0)))
    smem = pl.BlockSpec(memory_space=pltpu.SMEM)
    return pl.pallas_call(
        gather_body, out_shape=jax.ShapeDtypeStruct((rows, width), BF16),
        in_specs=[smem, smem, pl.BlockSpec(memory_space=VM), pl.BlockSpec(memory_space=VM), pl.BlockSpec(memory_space=pl.ANY)],
        out_specs=pl.BlockSpec(memory_space=VM),
        scratch_shapes=[VM((GB, 8, width), BF16), pltpu.SemaphoreType.DMA],
        compiler_params=pltpu.CompilerParams(vmem_limit_bytes=40 << 20), name='gather_rows',
    )(count, blocks, key[:, None], tail, table)


def table_grad_body(count_ref, blocks_ref, key_ref, de_ref, zeros_ref, out_ref, tail_ref, stage, sem):
    rows, width = de_ref.shape
    vocab = out_ref.shape[0]
    full = vocab // 8
    tail_ref[...] = jnp.zeros_like(tail_ref)
    count = count_ref[0]

    def put(b, i):
        return pltpu.make_async_copy(stage.at[i], out_ref.at[pl.ds(pl.multiple_of(b * 8, 8), 8), :], sem)

    def sums(ci):
        ids = lax.broadcasted_iota(jnp.int32, (GB * 8, rows), 0) + ci * (GB * 8)
        hot = jnp.where(ids == key_ref[...], 1.0, 0.0).astype(BF16)
        for c in range(0, width, 512):
            got = nn(hot, de_ref[:, c:c + 512])
            stage[:, :, c:c + 512] = got.astype(BF16).reshape(GB, 8, 512)

    def move(ci, go):
        base = ci * GB

        def one(i, c):
            b = blocks_ref[base + i]

            @pl.when(b < full)
            def _():
                go(put(b, i))
            @pl.when(b >= full)
            def _():
                tail_ref[...] = stage[i]
            return c

        lax.fori_loop(0, jnp.minimum(GB, count - base), one, 0)

    def chunk(ci, carry):
        sums(ci)
        move(ci, lambda cp: cp.start())
        move(ci, lambda cp: cp.wait())
        return carry

    lax.fori_loop(0, (count + GB - 1) // GB, chunk, 0)


def table_grad(key, blocks, count, de_full, table):
    vocab, width = table.shape
    smem = pl.BlockSpec(memory_space=pltpu.SMEM)
    full = vocab // 8 * 8
    out, tail = pl.pallas_call(
        table_grad_body, out_shape=[jax.ShapeDtypeStruct((vocab, width), BF16), jax.ShapeDtypeStruct((8, width), BF16)],
        in_specs=[smem, smem, pl.BlockSpec(memory_space=VM), pl.BlockSpec(memory_space=VM), pl.BlockSpec(memory_space=pl.ANY)], input_output_aliases={4: 0},
        out_specs=[pl.BlockSpec(memory_space=pl.ANY), pl.BlockSpec(memory_space=VM)],
        scratch_shapes=[VM((GB, 8, width), BF16), pltpu.SemaphoreType.DMA],
        compiler_params=pltpu.CompilerParams(vmem_limit_bytes=40 << 20), name='table_grad',
    )(count, blocks, key[None, :], de_full, table)
    return lax.dynamic_update_slice(out, tail[:vocab - full], (full, 0))


def heads_of(q_ref, kn_ref, kp_ref, cos_ref, sin_ref, nope, half):
    q_pe = q_ref[nope:, :].astype(F32)
    lo, hi, cos_t, sin_t = q_pe[:half], q_pe[half:], cos_ref[...], sin_ref[...]
    q_all = jnp.concatenate([q_ref[:nope, :], (lo * cos_t - hi * sin_t).astype(BF16), (hi * cos_t + lo * sin_t).astype(BF16)], axis=0)
    return q_all, jnp.concatenate([kn_ref[...], kp_ref[...]], axis=0)


def scores_of(k_all, q_all, ki, qi, scale):
    s = tn(k_all[:, ki * QB:(ki + 1) * QB], q_all[:, qi * QB:(qi + 1) * QB]) * scale
    if ki == qi:
        keys = lax.broadcasted_iota(jnp.int32, (QB, QB), 0)
        s = jnp.where(keys <= lax.broadcasted_iota(jnp.int32, (QB, QB), 1), s, -1e30)
    return s


def attn_fwd_body(q_ref, kn_ref, kp_ref, v_ref, cos_ref, sin_ref, o_ref, lse_ref):
    nope, half = kn_ref.shape[0], cos_ref.shape[0]
    scale = q_ref.shape[0] ** -0.5 * LOG2E
    q_all, k_all = heads_of(q_ref, kn_ref, kp_ref, cos_ref, sin_ref, nope, half)
    for qi in range(q_ref.shape[1] // QB):
        lanes = slice(qi * QB, (qi + 1) * QB)
        s = [scores_of(k_all, q_all, ki, qi, scale) for ki in range(qi + 1)]
        top = functools.reduce(jnp.maximum, [jnp.max(x, axis=0, keepdims=True) for x in s])
        p = [jnp.exp2(x - top) for x in s]
        total = sum(sum_rows(x) for x in p)
        inv = 1.0 / total
        o = sum(nn(v_ref[:, ki * QB:(ki + 1) * QB], (x * inv).astype(BF16)) for ki, x in enumerate(p))
        o_ref[:, lanes] = o.astype(BF16)
        lse_ref[0, :, lanes] = top + jnp.log2(total)


def attn_bwd_body(q_ref, kn_ref, kp_ref, v_ref, cos_ref, sin_ref, lse_ref, do_ref, dq_ref, dkn_ref, dv_ref, dkp_ref, table_ref, dk_acc, dv_acc, zero, zsem):
    full = table_ref.shape[0] // 8 * 8
    fills = [pltpu.make_async_copy(zero.at[pl.ds(0, n), :], table_ref.at[pl.ds(r, n), :], zsem.at[k])
             for k, (r, n) in enumerate((r, min(ZR, full - r)) for r in range(0, full, ZR))]

    @pl.when(pl.program_id(0) == 0)
    def _():
        zero[...] = jnp.zeros_like(zero)
        for cp in fills:
            cp.start()

    nope, half = kn_ref.shape[0], cos_ref.shape[0]
    raw = q_ref.shape[0] ** -0.5
    q_all, k_all = heads_of(q_ref, kn_ref, kp_ref, cos_ref, sin_ref, nope, half)
    dk_acc[...] = jnp.zeros_like(dk_acc)
    dv_acc[...] = jnp.zeros_like(dv_acc)
    for qi in range(q_ref.shape[1] // QB):
        lanes = slice(qi * QB, (qi + 1) * QB)
        q_b, do_b, lse = q_all[:, lanes], do_ref[:, lanes], lse_ref[0, :, lanes]
        p = [jnp.exp2(scores_of(k_all, q_all, ki, qi, raw * LOG2E) - lse) for ki in range(qi + 1)]
        dp = [tn(v_ref[:, ki * QB:(ki + 1) * QB], do_b) for ki in range(qi + 1)]
        delta = sum(sum_rows(a * b) for a, b in zip(p, dp))
        dq = None
        for ki in range(qi + 1):
            keys = slice(ki * QB, (ki + 1) * QB)
            ds = (p[ki] * (dp[ki] - delta) * raw).astype(BF16)
            part = nn(k_all[:, keys], ds)
            dq = part if dq is None else dq + part
            dk_acc[:, keys] += nt(q_b, ds)
            dv_acc[:, keys] += nt(do_b, p[ki].astype(BF16))
        cos_t, sin_t = cos_ref[:, lanes], sin_ref[:, lanes]
        lo, hi = dq[nope:nope + half], dq[nope + half:]
        dq_ref[:nope, lanes] = dq[:nope].astype(BF16)
        dq_ref[nope:nope + half, lanes] = (lo * cos_t + hi * sin_t).astype(BF16)
        dq_ref[nope + half:, lanes] = (hi * cos_t - lo * sin_t).astype(BF16)
    dkn_ref[...] = dk_acc[:nope, :].astype(BF16)
    dv_ref[...] = dv_acc[...].astype(BF16)

    @pl.when(pl.program_id(0) == 0)
    def _():
        dkp_ref[...] = jnp.zeros_like(dkp_ref)
    dkp_ref[...] += dk_acc[nope:, :]

    @pl.when(pl.program_id(0) == pl.num_programs(0) - 1)
    def _():
        for cp in fills:
            cp.wait()


def attn_specs(heads, qd, nope, rope, vd, seq):
    per = lambda r: pl.BlockSpec((r, seq), lambda h: (h, 0))
    one = lambda r: pl.BlockSpec((r, seq), lambda h: (0, 0))
    return [per(qd), per(nope), one(rope), per(vd), one(rope // 2), one(rope // 2)], per, one, pl.BlockSpec((1, 1, seq), lambda h: (h, 0, 0))


def attend_bwd(q, kn, kp, v, cos_t, sin_t, lse, do, heads, table):
    seq, qd, nope, vd, rope = q.shape[1], q.shape[0] // heads, kn.shape[0] // heads, v.shape[0] // heads, kp.shape[0]
    ins, per, one, lse_spec = attn_specs(heads, qd, nope, rope, vd, seq)
    return pl.pallas_call(
        attn_bwd_body, grid=(heads,), in_specs=ins + [lse_spec, per(vd)], out_specs=[per(qd), per(nope), per(vd), one(rope), pl.BlockSpec(memory_space=pl.ANY)],
        out_shape=[jax.ShapeDtypeStruct(q.shape, BF16), jax.ShapeDtypeStruct(kn.shape, BF16), jax.ShapeDtypeStruct(v.shape, BF16), jax.ShapeDtypeStruct(kp.shape, F32), jax.ShapeDtypeStruct(table, BF16)],
        scratch_shapes=[VM((qd, seq), F32), VM((vd, seq), F32), VM((ZR, table[1]), BF16), pltpu.SemaphoreType.DMA((-(-table[0] // ZR),))],
        compiler_params=pltpu.CompilerParams(vmem_limit_bytes=40 << 20), name='attend_bwd',
    )(q, kn, kp, v, cos_t, sin_t, lse, do)


def shift(x, bit):
    return lax.ppermute(x, 'tp', [(d, d ^ bit) for d in range(8)])


PAIR, XBIT, YBIT = 1, 2, 4


def coords():
    me = lax.axis_index('tp')
    return me // YBIT, (me // XBIT) % 2, me % 2


def pick(x, i, axis):
    return lax.dynamic_index_in_dim(x, i, axis, keepdims=False)


def added(a, b):
    return (a.astype(F32) + b.astype(F32)).astype(BF16)


def scatter_hops(part, local):
    y, x, core = coords()
    half = part.shape[1] // 2
    p = part.reshape(2, 2, 2, local, part.shape[1])
    q = added(pick(p, core, 2), shift(pick(p, 1 - core, 2), PAIR))
    a, b = q[..., :half], q[..., half:]
    a = added(pick(a, x, 1), shift(pick(a, 1 - x, 1), XBIT))
    b = added(pick(b, y, 0), shift(pick(b, 1 - y, 0), YBIT))
    a = pick(a, y, 0).astype(F32) + shift(pick(a, 1 - y, 0), YBIT).astype(F32)
    b = pick(b, x, 0).astype(F32) + shift(pick(b, 1 - x, 0), XBIT).astype(F32)
    return jnp.concatenate([a, b], axis=1)


def gather_hops(blk):
    half = blk.shape[1] // 2
    bx, by = shift(blk, XBIT), shift(blk, YBIT)
    near = jnp.concatenate([blk, bx, by])
    diag = jnp.concatenate([shift(by[:, :half], XBIT), shift(bx[:, half:], YBIT)], axis=1)
    return jnp.concatenate([near, diag, shift(near, PAIR), shift(diag, PAIR)])


def hop_order():
    me = lax.axis_index('tp')
    flip = lambda v, bit: v + bit - 2 * bit * ((v // bit) % 2)
    own = [me, flip(me, XBIT), flip(me, YBIT), flip(flip(me, XBIT), YBIT)]
    return own + [flip(d, PAIR) for d in own]


def to_hop_order(x, axis):
    n = x.shape[axis] // 8
    return jnp.concatenate([lax.dynamic_slice_in_dim(x, d * n, n, axis) for d in hop_order()], axis=axis)


def from_hop_order(x):
    n = x.shape[0] // 8
    out = jnp.zeros_like(x)
    for k, d in enumerate(hop_order()):
        out = lax.dynamic_update_slice_in_dim(out, x[k * n:(k + 1) * n], d * n, 0)
    return out


def sum_hops(x):
    for bit in (PAIR, XBIT, YBIT):
        x = x + shift(x, bit)
    return x


class Exchange:
    def __init__(self, widths, pieces):
        self.widths, self.pieces = widths, pieces
        self.order = range(len(pieces))

    def rs_scratch(self, rows):
        n = len(self.pieces)
        out = []
        for w in self.widths:
            out += [VM((4, rows, w), BF16), VM((2, rows, w), BF16), VM((2, rows, w), BF16), VM((rows, w), BF16), VM((rows, w), BF16)]
        dma = pltpu.SemaphoreType.DMA
        return out + [dma((4, n)), dma((4, n)), dma((2, n)), dma((2, n)), dma((n,)), dma((n,))]

    def ag_scratch(self):
        n = len(self.pieces)
        dma = pltpu.SemaphoreType.DMA
        return [dma((2, n)), dma((2, n)), dma((n,)), dma((n,)), dma((4, n)), dma((4, n))]

    def place(self, rows):
        me = lax.axis_index('tp')
        core, x, y = me % 2, (me // 2) % 2, me // 4
        dev = lambda yy, xx, cc: (yy * 2 + xx) * 2 + cc
        self.me, self.rows = me, rows
        self.pn, self.xn, self.yn = dev(y, x, 1 - core), dev(y, 1 - x, core), dev(1 - y, x, core)
        chips = [(y, x), (y, 1 - x), (1 - y, x), (1 - y, 1 - x)]
        at = lambda d: pl.ds(pl.multiple_of(d * rows, rows), rows)
        self.mine = [at(dev(*ch, core)) for ch in chips]
        self.theirs = [at(dev(*ch, 1 - core)) for ch in chips]
        self.chip = [pl.ds(pl.multiple_of(dev(*ch, 0) * rows, 2 * rows), 2 * rows) for ch in chips]

    def enter(self):
        sem = pltpu.get_barrier_semaphore()
        near = (self.pn, self.xn, self.yn)
        for d in near:
            pl.semaphore_signal(sem, inc=1, device_id={'tp': d}, device_id_type=pl.DeviceIdType.MESH)
        pl.semaphore_wait(sem, len(near))

    def copy(self, src, dst, ssem, rsem, dev):
        return pltpu.make_async_remote_copy(src_ref=src, dst_ref=dst, send_sem=ssem, recv_sem=rsem, device_id={'tp': dev}, device_id_type=pl.DeviceIdType.MESH)

    def rs_begin(self, parts, scratch):
        na = len(self.widths)
        self.parts = parts
        self.bufs = [scratch[5 * a:5 * a + 5] for a in range(na)]
        ds, dr, s1, r1, s2, r2 = scratch[5 * na:5 * na + 6]
        self.pair, self.hop1, self.hop2 = {}, {}, {}
        for i, (h, a, c0, cn) in enumerate(self.pieces):
            cols = pl.ds(c0, cn)
            dbuf, sb1, rb1, sb2, rb2 = self.bufs[a]
            for j in range(4):
                self.pair[j, i] = self.copy(parts[a].at[self.theirs[j], cols], dbuf.at[j, :, cols], ds.at[j, i], dr.at[j, i], self.pn)
            to1, to2 = (self.xn, self.yn) if h == 0 else (self.yn, self.xn)
            for k in range(2):
                self.hop1[k, i] = self.copy(sb1.at[k, :, cols], rb1.at[k, :, cols], s1.at[k, i], r1.at[k, i], to1)
            self.hop2[i] = self.copy(sb2.at[:, cols], rb2.at[:, cols], s2.at[i], r2.at[i], to2)

    def ready(self, j):
        for i in self.order:
            self.pair[j, i].start()

    def chip_sum(self, j, i):
        h, a, c0, cn = self.pieces[i]
        self.pair[j, i].wait_recv()
        return self.parts[a][self.mine[j], c0:c0 + cn].astype(F32) + self.bufs[a][0][j, :, c0:c0 + cn].astype(F32)

    def push(self, j):
        for i in self.order:
            h, a, c0, cn = self.pieces[i]
            if j == 3 or j == 1 + h:
                k = 1 if j == 3 else 0
                self.bufs[a][1][k, :, c0:c0 + cn] = self.chip_sum(j, i).astype(BF16)
                self.hop1[k, i].start()

    def relay(self):
        for i in self.order:
            h, a, c0, cn = self.pieces[i]
            own = self.chip_sum(2 - h, i)
            self.hop1[1, i].wait_recv()
            self.bufs[a][3][:, c0:c0 + cn] = (own + self.bufs[a][2][1, :, c0:c0 + cn].astype(F32)).astype(BF16)
            self.hop2[i].start()

    def land(self, accs):
        for i in self.order:
            h, a, c0, cn = self.pieces[i]
            own = self.chip_sum(0, i)
            self.hop1[0, i].wait_recv()
            own = own + self.bufs[a][2][0, :, c0:c0 + cn].astype(F32)
            self.hop2[i].wait_recv()
            accs[a][:, c0:c0 + cn] = own + self.bufs[a][4][:, c0:c0 + cn].astype(F32)

    def drain(self):
        for cp in list(self.pair.values()) + list(self.hop1.values()) + list(self.hop2.values()):
            cp.wait_send()

    def reduce_scatter(self, accs, produce):
        late = None
        for j in (3, 1, 2, 0):
            produce(j)
            self.ready(j)
            if late:
                self.push(late)
            late = j
        self.relay()
        self.land(accs)

    def all_gather(self, fulls, scratch, arrive, slow=False):
        os_, xr, fs, fr, ps, pr = scratch
        half0 = [i for i in self.order if self.pieces[i][0] == 0]
        half1 = [i for i in self.order if self.pieces[i][0] == 1]

        def to(i, j, ssem, rsem, dev, rows=None):
            h, a, c0, cn = self.pieces[i]
            ref = fulls[a].at[(rows or self.mine)[j], pl.ds(c0, cn)]
            return self.copy(ref, ref, ssem, rsem, dev)

        near = (self.xn, self.yn)
        own = [[to(i, 0, os_.at[k, i], xr.at[k, i], dev) for i in self.order] for k, dev in enumerate(near)]
        from_n = [[to(i, 1 + k, os_.at[k, i], xr.at[k, i], dev) for i in self.order] for k, dev in enumerate(near)]
        fwd = [to(i, 2 - self.pieces[i][0], fs.at[i], fr.at[i], near[self.pieces[i][0]]) for i in self.order]
        diag = [to(i, 3, fs.at[i], fr.at[i], self.xn) for i in self.order]
        give = [[to(i, j, ps.at[j, i], pr.at[j, i], self.pn) for i in self.order] for j in range(4)]
        take = [[to(i, j, ps.at[j, i], pr.at[j, i], self.pn, self.theirs) for i in self.order] for j in range(4)]
        for i0, i1 in zip(half0, half1):
            own[0][i1].start()
            own[1][i0].start()
        for i0, i1 in zip(half0, half1):
            own[0][i0].start()
            own[1][i1].start()
        for cp in give[0]:
            cp.start()
        for cp in take[0]:
            cp.wait_recv()
        arrive(0)
        for i0, i1 in zip(half0, half1):
            from_n[1][i0].wait_recv()
            fwd[i0].start()
            give[2][i0].start()
            from_n[0][i1].wait_recv()
            fwd[i1].start()
            give[1][i1].start()
        for i0, i1 in zip(half0, half1):
            from_n[1][i1].wait_recv()
            give[2][i1].start()
            from_n[0][i0].wait_recv()
            give[1][i0].start()
        def diagonal():
            for i in self.order:
                diag[i].wait_recv()
                give[3][i].start()

        for j in (1, 2):
            for cp in take[j]:
                cp.wait_recv()
            arrive(j)
            if slow == (j == 1):
                diagonal()
        for cp in take[3]:
            cp.wait_recv()
        arrive(3)
        for cp in own[0] + own[1] + fwd + [c for g in give for c in g]:
            cp.wait_send()


def halves(width, n):
    step = width // (2 * n)
    return [(h, 0, (h * n + k) * step, step) for k in range(n) for h in range(2)]


MAIN = halves(2560, 2)
LAST = MAIN + [(0, 1, 0, 256), (1, 1, 256, 128)]
NRS, NAG = 11, 6
COLS = 512


def norm_rows(x, gain):
    return x * lax.rsqrt(mean_last(x * x) + EPSILON) * gain


def norm_rows_vjp(x, gain, dy):
    r = lax.rsqrt(mean_last(x * x) + EPSILON)
    gd = dy * gain
    dot = mean_last(gd * x)
    return r * gd - x * (r * r * r * dot), sum_rows(dy * x * r)


def exchange_call(body, name, cid, ins, out_shape, scratch, far=0, limit=50):
    vmem, hbm = pl.BlockSpec(memory_space=VM), pl.BlockSpec(memory_space=pltpu.HBM)
    return pl.pallas_call(
        body, out_shape=out_shape, in_specs=[vmem] * (len(ins) - far) + [hbm] * far, out_specs=[vmem] * len(out_shape), scratch_shapes=scratch,
        compiler_params=pltpu.CompilerParams(vmem_limit_bytes=limit << 20, collective_id=cid, has_side_effects=True), name=name)(*ins)


def shape(dims, dtype):
    return jax.ShapeDtypeStruct(dims, dtype)


def idle(j):
    pass


def embed_body(part, gain, wq, wdkv, e_ref, full, q_ref, lat_ref, acc, *scratch):
    ex = Exchange([part.shape[1]], MAIN)
    ex.place(acc.shape[0])
    ex.enter()
    ex.rs_begin([part], scratch)
    ex.reduce_scatter([acc], idle)
    e = acc[...].astype(BF16)
    e_ref[...] = e
    full[ex.mine[0], :] = norm_rows(e.astype(F32), gain[...]).astype(BF16)

    def arrive(j):
        u = full[ex.chip[j], :]
        q_ref[:, ex.chip[j]] = nt(wq[...], u).astype(BF16)
        lat_ref[ex.chip[j], :] = nt(u, wdkv[...])

    ex.all_gather([full], scratch[NRS:], arrive)
    ex.drain()


def attn_body(lat, g_kv, wuk, wuv, q_ref, cos_ref, sin_ref, dy_ref, c_ref, kn_ref, kp_ref, v_ref, o_ref, lse_ref, dyf, *scratch):
    ex = Exchange([dyf.shape[1]], MAIN)
    ex.place(dy_ref.shape[0])
    ex.enter()
    dyf[ex.mine[0], :] = dy_ref[...]
    lora, half, heads = c_ref.shape[1], cos_ref.shape[0], lse_ref.shape[0]
    per = lambda ref, h: ref.at[pl.ds(h * (ref.shape[0] // heads), ref.shape[0] // heads), :]

    def arrive(j):
        if j:
            return
        c = norm_rows(lat[:, :lora], g_kv[...]).astype(BF16)
        c_ref[...] = c
        pe = lat[:, lora:].T
        lo, hi, cos_t, sin_t = pe[:half], pe[half:], cos_ref[...], sin_ref[...]
        kp_ref[...] = jnp.concatenate([lo * cos_t - hi * sin_t, hi * cos_t + lo * sin_t], axis=0).astype(BF16)
        kn_ref[...] = nt(wuk[...], c).astype(BF16)
        v_ref[...] = nt(wuv[...], c).astype(BF16)
        for h in range(heads):
            attn_fwd_body(per(q_ref, h), per(kn_ref, h), kp_ref, per(v_ref, h), cos_ref, sin_ref, per(o_ref, h), lse_ref.at[pl.ds(h, 1)])

    ex.all_gather([dyf], scratch, arrive)


def middle_body(o_ref, wo, e_ref, gain, dyl_ref, dy_hbm, wg_hbm, wu_hbm, wd_hbm,
                h_ref, z, y_ref, hid_ref, dgate_ref, dup_ref, dres_ref, dgain_ref, dfull, do_ref,
                wg, wu, wd, dyb, part, acc, wsem, dsem, *scratch):
    ex = Exchange([part.shape[1]], MAIN)
    ex.place(acc.shape[0])
    ex.enter()
    loads = [pltpu.make_async_copy(a, b, wsem.at[k]) for k, (a, b) in enumerate(((wg_hbm, wg), (wu_hbm, wu), (wd_hbm, wd)))]
    dy_in = [pltpu.make_async_copy(dy_hbm.at[ex.chip[j], :], dyb.at[j % 2], dsem.at[j % 2]) for j in range(4)]
    for cp in loads + dy_in[:2]:
        cp.start()
    ex.rs_begin([part], scratch)
    width = part.shape[1]

    def attn_part(j):
        part[ex.chip[j], :] = tn(o_ref[:, ex.chip[j]], wo[...]).astype(BF16)

    ex.reduce_scatter([acc], attn_part)
    h = (e_ref[...].astype(F32) + acc[...].astype(BF16).astype(F32)).astype(BF16)
    h_ref[...] = h
    z[ex.mine[0], :] = norm_rows(h.astype(F32), gain[...]).astype(BF16)

    def mlp(j):
        rows = ex.chip[j]
        gate, up = nt(z[rows, :], wg[...]), nt(z[rows, :], wu[...])
        sig = jax.nn.sigmoid(gate)
        hid = (gate * sig * up).astype(BF16)
        hid_ref[rows, :] = hid
        dh = nt(dyb[j % 2], wd[...])
        dup = (dh * gate * sig).astype(BF16)
        dgate = (dh * up * sig * (1.0 + gate * (1.0 - sig))).astype(BF16)
        dup_ref[rows, :] = dup
        dgate_ref[rows, :] = dgate
        for c in range(0, width, COLS):
            part[rows, c:c + COLS] = (nn(dgate, wg[:, c:c + COLS]) + nn(dup, wu[:, c:c + COLS])).astype(BF16)
            y_ref[rows, c:c + COLS] = nn(hid, wd[:, c:c + COLS]).astype(BF16)

    def arrive_z(j):
        if j == 0:
            ex.drain()
            for cp in loads:
                cp.wait()
        dy_in[j].wait()
        mlp(j)
        if j < 2:
            dy_in[j + 2].start()
        ex.ready(j)
        if j == 2:
            ex.push(1)
        if j == 3:
            ex.push(2)
            ex.push(3)

    ex.all_gather([z], scratch[NRS:NRS + NAG], arrive_z, slow=True)
    ex.relay()
    ex.land([acc])
    dx, dgain_ref[...] = norm_rows_vjp(h_ref[...].astype(F32), gain[...], acc[...])
    dres = dyl_ref[...].astype(F32) + dx
    dres_ref[...] = dres
    dfull[ex.mine[0], :] = dres.astype(BF16)

    def arrive_d(j):
        do_ref[:, ex.chip[j]] = nt(wo[...], dfull[ex.chip[j], :]).astype(BF16)

    ex.all_gather([dfull], scratch[NRS + NAG:], arrive_d)
    ex.drain()


def attn_back_body(dq_ref, lat, wq, wdkv, e_ref, dres_ref, gain, de_ref, dlat_ref, dg_ref, part, acc, acc_lat, *scratch):
    ex = Exchange([part.shape[1], lat.shape[1]], LAST)
    ex.place(acc.shape[0])
    ex.enter()
    ex.rs_begin([part, lat], scratch)
    lw = wdkv.shape[0]

    def produce(j):
        rows = ex.chip[j]
        part[rows, :] = (tn(dq_ref[:, rows], wq[...]) + nn(lat[rows, :lw], wdkv[...])).astype(BF16)

    ex.reduce_scatter([acc, acc_lat], produce)
    dx, dg_ref[...] = norm_rows_vjp(e_ref[...].astype(F32), gain[...], acc[...])
    de_ref[...] = (dres_ref[...] + dx).astype(BF16)
    dlat_ref[...] = acc_lat[...].astype(BF16)
    ex.drain()


def layer_pass(rows, d_out, w_q, w_dkv, g_kv, w_uk, w_uv, w_o, g_attn, g_mlp, w_gate, w_up, w_down, vocab):
    w_q, heads = w_q
    seq, width = rows.shape
    local = d_out.shape[0]
    lora = g_kv.shape[0]
    latw = w_dkv.shape[0]
    one = Exchange([width], MAIN)
    main = [VM((local, width), F32)] + one.rs_scratch(local) + one.ag_scratch()
    partb = [VM((seq, width), BF16)]
    loc, fullb = shape((local, width), BF16), shape((seq, width), BF16)
    ga, gm = g_attn[None, :], g_mlp[None, :]
    embedded, x_attn, query, latent = exchange_call(
        embed_body, 'embed_exchange', 1, [rows, ga, w_q, w_dkv], [loc, fullb, shape((w_q.shape[0], seq), BF16), shape((seq, latw), F32)], main)
    cos_t, sin_t = (t.T for t in rope_tables(seq, latw - lora))
    nq, nk, nv = w_q.shape[0], w_uk.shape[0], w_uv.shape[0]
    c_kv, k_nope, k_pe_t, value, attn_out, lse, dy_full = exchange_call(
        attn_body, 'attend_fwd', 2, [latent, g_kv[None, :], w_uk, w_uv, query, cos_t, sin_t, d_out],
        [shape((seq, lora), BF16), shape((nk, seq), BF16), shape((latw - lora, seq), BF16), shape((nv, seq), BF16), shape((nv, seq), BF16),
         shape((heads, 1, seq), F32), fullb], one.ag_scratch())
    kv_pull = jax.vjp(kv_prep, latent, g_kv)[1]
    ffn = w_gate.shape[0]
    dma = pltpu.SemaphoreType.DMA
    act, wide = shape((seq, ffn), BF16), VM((ffn, width), BF16)
    residual, x_mlp, y_part, hidden, d_gate, d_up, d_residual, dg_mlp, d_attn_full, d_attn_out = exchange_call(
        middle_body, 'middle', 3, [attn_out, w_o, embedded, gm, d_out, dy_full, w_gate, w_up, w_down],
        [loc, fullb, fullb, act, act, act, shape((local, width), F32), shape((1, width), F32), fullb, shape((w_o.shape[0], seq), BF16)],
        [wide, wide, wide, VM((2, seq // 4, width), BF16)] + partb + [VM((local, width), F32), dma((3,)), dma((2,))] + one.rs_scratch(local) + one.ag_scratch() + one.ag_scratch(),
        far=4, limit=63)
    mlp_loc = scatter_hops(y_part, local)
    layer_out = (residual.astype(F32) + mlp_loc.astype(BF16).astype(F32)).astype(BF16)
    d_query, d_knope, d_value, d_kpe, table0 = attend_bwd(query, k_nope, k_pe_t, value, cos_t, sin_t, lse, d_attn_out, heads, (vocab, width))
    d_ckv = (tn(d_knope, w_uk) + tn(d_value, w_uv)).astype(BF16)
    d_latent, dg_kv = kv_pull((d_ckv, d_kpe.T.astype(BF16)))
    lat_part = jnp.pad(d_latent.astype(BF16), ((0, 0), (0, -latw % 128)))
    padw = lat_part.shape[1]
    two = Exchange([width, padw], LAST)
    de, dlat, dg_attn = exchange_call(
        attn_back_body, 'back_exchange', 4, [d_query, lat_part, w_q, w_dkv, embedded, d_residual, ga],
        [loc, shape((local, padw), BF16), shape((1, width), F32)],
        partb + [VM((local, width), F32), VM((local, padw), F32)] + two.rs_scratch(local))
    hidden, d_gate, d_up, d_query_l, d_knope, d_value, attn_out, de = lax.optimization_barrier((hidden, d_gate, d_up, d_query, d_knope, d_value, attn_out, de))
    de_full = gather_hops(de)
    lat_full = from_hop_order(gather_hops(dlat))
    dw_down = tn(hidden, dy_full)
    dw_gate = tn(d_gate, x_mlp)
    dw_up = tn(d_up, x_mlp)
    dw_o = nn(attn_out, d_attn_full)
    dw_uk = nn(d_knope, c_kv)
    dw_uv = nn(d_value, c_kv)
    dw_q = nn(d_query_l, x_attn)
    dw_dkv = tn(lat_full[:, :latw], x_attn)
    dg = sum_hops(jnp.concatenate([dg_attn[0], dg_mlp[0], dg_kv]))
    dg_attn, dg_mlp, dg_kv = dg[:width], dg[width:2 * width], dg[2 * width:]
    return layer_out, de_full, table0, (dw_q, dw_dkv, dg_kv, dw_uk, dw_uv, dw_o, dg_attn, dg_mlp, dw_gate, dw_up, dw_down)


def rows_of(w):
    return jnp.transpose(w, (1, 2, 0)).reshape(-1, w.shape[0])


def unrows(g, heads):
    return jnp.transpose(g.reshape(heads, -1, g.shape[1]), (2, 0, 1))


def solution(mesh):
    def device_step(tokens, embed_table, w_q, w_dkv, g_kv, w_uk, w_uv, w_o, g_attn, g_mlp, w_gate, w_up, w_down, d_out):
        vocab_local, model_dim = embed_table.shape
        heads = w_q.shape[1]
        key, blocks, count = block_index(tokens, vocab_local)
        rows = gather_rows(key, blocks, count, embed_table)
        layer_out, de_full, table0, grads = layer_pass(
            rows, d_out[0], (rows_of(w_q), heads), w_dkv.T, g_kv, rows_of(w_uk), rows_of(w_uv), w_o.reshape(-1, model_dim),
            g_attn, g_mlp, w_gate.T, w_up.T, w_down, vocab_local)
        d_table = table_grad(to_hop_order(key, 0), blocks, count, de_full, table0)
        dw_q, dw_dkv, dg_kv, dw_uk, dw_uv, dw_o, dg_attn, dg_mlp, dw_gate, dw_up, dw_down = grads
        return (layer_out[None], d_table, unrows(dw_q, heads), dw_dkv.T, dg_kv, unrows(dw_uk, heads), unrows(dw_uv, heads),
                dw_o.reshape(w_o.shape), dg_attn, dg_mlp, dw_gate.T, dw_up.T, dw_down)

    row_spec = P('dp', 'tp', None)
    head_spec = P(None, 'tp', None)
    in_specs = (P('dp', None), P('tp', None), head_spec, P(None, None), P(None), head_spec, head_spec, P('tp', None, None), P(None), P(None), P(None, 'tp'), P(None, 'tp'), P('tp', None), row_spec)
    out_specs = (row_spec, P(('dp', 'tp'), None), P('dp', 'tp', None), P('dp', None), P('dp'), P('dp', 'tp', None), P('dp', 'tp', None), P(('dp', 'tp'), None, None), P('dp'), P('dp'), P('dp', 'tp'), P('dp', 'tp'), P(('dp', 'tp'), None))
    return jax.shard_map(device_step, mesh=mesh, in_specs=in_specs, out_specs=out_specs, check_vma=False)
```

```python
import functools

import jax
import jax.numpy as jnp
from jax import lax
from jax.experimental import pallas as pl
from jax.experimental.pallas import tpu as pltpu
from jax.sharding import PartitionSpec as P

EPSILON = 1e-6
ROPE_BASE = 10000.0
F32, BF16 = jnp.float32, jnp.bfloat16
LOG2E = 1.4426950408889634
VM = pltpu.VMEM
ZR = 248
GB = 64
GR = GB * 8
LIMIT = 40 << 20
QB = 256


def mm(lhs, rhs, lc, rc):
    return lax.dot_general(lhs, rhs, (((lc,), (rc,)), ((), ())), preferred_element_type=F32)


def nn(a, b):
    return mm(a, b, 1, 0)


def nt(a, b):
    return mm(a, b, 1, 1)


def tn(a, b):
    return mm(a, b, 0, 0)


mean_last = functools.partial(jnp.mean, axis=-1, keepdims=True)
sum_rows = functools.partial(jnp.sum, axis=0, keepdims=True)


def rope_tables(seq_len, rope_dim):
    inv_freq = ROPE_BASE ** (-jnp.arange(0, rope_dim, 2, dtype=F32) / rope_dim)
    angles = jnp.arange(seq_len, dtype=F32)[:, None] * inv_freq[None, :]
    return jnp.cos(angles), jnp.sin(angles)


def apply_rope(x_in, cos_t, sin_t):
    half_dim = x_in.shape[-1] // 2
    x_lo, x_hi = x_in[..., :half_dim], x_in[..., half_dim:]
    return jnp.concatenate([x_lo * cos_t - x_hi * sin_t, x_hi * cos_t + x_lo * sin_t], axis=-1)


def rms_norm(x_in, gain):
    inv_rms = lax.rsqrt(mean_last(x_in * x_in) + EPSILON)
    return (x_in * inv_rms * gain).astype(BF16)


def kv_prep(latent, g_kv):
    lora = g_kv.shape[0]
    cos_t, sin_t = rope_tables(latent.shape[0], latent.shape[-1] - lora)
    k_pe = apply_rope(latent[:, lora:], cos_t, sin_t).astype(BF16)
    return rms_norm(latent[:, :lora], g_kv), k_pe


def block_index(tokens, vocab_local):
    ids = tokens.reshape(-1) - lax.axis_index('tp') * vocab_local
    n = ids.shape[0]
    owned = (ids >= 0) & (ids < vocab_local)
    blk = jnp.where(owned, ids >> 3, -1)
    pos = jnp.arange(n, dtype=jnp.int32)
    eq = (blk[:, None] == blk[None, :])
    first = jnp.min(jnp.where(eq, pos[None, :], n), axis=1)
    isf = owned & (first == pos)
    slot = jnp.sum((isf[None, :] & (pos[None, :] < first[:, None])).astype(jnp.int32), axis=1)
    key = jnp.where(owned, slot * 8 + (ids & 7), -1)
    blocks = jnp.sum(jnp.where(isf[None, :] & (slot[None, :] == pos[:, None]), blk[None, :], 0), axis=1)
    count = jnp.sum(isf.astype(jnp.int32)).reshape(1)
    return key, blocks, count


def gather_body(count_ref, blocks_ref, key_ref, tail_ref, table_ref, out_ref, stage, sem):
    rows, width = out_ref.shape
    full = table_ref.shape[0] // 8
    stage[...] = jnp.zeros_like(stage)
    out_ref[...] = jnp.zeros_like(out_ref)
    count = count_ref[0]

    def fetch(b, i):
        return pltpu.make_async_copy(table_ref.at[pl.ds(pl.multiple_of(b * 8, 8), 8), :], stage.at[i], sem)

    def chunk(ci, carry):
        base = ci * GB
        n = jnp.minimum(GB, count - base)

        def start(i, c):
            b = blocks_ref[base + i]

            @pl.when(b < full)
            def _():
                fetch(b, i).start()

            @pl.when(b >= full)
            def _():
                stage[i] = tail_ref[...]
            return c

        def wait(i, c):
            b = blocks_ref[base + i]

            @pl.when(b < full)
            def _():
                fetch(b, i).wait()
            return c

        lax.fori_loop(0, n, start, 0)
        lax.fori_loop(0, n, wait, 0)
        cols = lax.broadcasted_iota(jnp.int32, (rows, GR), 1) + base * 8
        hot = jnp.where(cols == key_ref[...], 1.0, 0.0).astype(BF16)
        for c in range(0, width, COLS):
            got = nn(hot, stage[:, :, c:c + COLS].reshape(GR, COLS))
            out_ref[:, c:c + COLS] += got.astype(BF16)
        return carry

    lax.fori_loop(0, (count + GB - 1) // GB, chunk, 0)


def gather_rows(key, blocks, count, table):
    rows, (vocab, width) = key.shape[0], table.shape
    full = vocab // 8 * 8
    tail = jnp.pad(table[full:], ((0, 8 - (vocab - full)), (0, 0)))
    smem = pl.BlockSpec(memory_space=pltpu.SMEM)
    return pl.pallas_call(
        gather_body, out_shape=jax.ShapeDtypeStruct((rows, width), BF16),
        in_specs=[smem, smem, pl.BlockSpec(memory_space=VM), pl.BlockSpec(memory_space=VM), pl.BlockSpec(memory_space=pl.ANY)],
        out_specs=pl.BlockSpec(memory_space=VM),
        scratch_shapes=[VM((GB, 8, width), BF16), pltpu.SemaphoreType.DMA],
        compiler_params=pltpu.CompilerParams(vmem_limit_bytes=LIMIT), name='gather_rows',
    )(count, blocks, key[:, None], tail, table)


def table_grad_body(count_ref, blocks_ref, key_ref, zeros_ref, *refs):
    pieces, (out_ref, tail_ref, lat_ref, de_ref, stage, sem) = refs[:-6], refs[-6:]
    rows, width = de_ref.shape
    local = rows // len(pieces)
    for k, (piece, d) in enumerate(zip(pieces, hop_order())):
        de_ref[k * local:(k + 1) * local, :] = piece[:, :width]
        lat_ref[pl.ds(pl.multiple_of(d * local, local), local), :] = piece[:, width:]
    full = out_ref.shape[0] // 8
    tail_ref[...] = jnp.zeros_like(tail_ref)
    count = count_ref[0]

    def put(b, i):
        return pltpu.make_async_copy(stage.at[i], out_ref.at[pl.ds(pl.multiple_of(b * 8, 8), 8), :], sem)

    def sums(ci):
        ids = lax.broadcasted_iota(jnp.int32, (GR, rows), 0) + ci * GR
        hot = jnp.where(ids == key_ref[...], 1.0, 0.0).astype(BF16)
        for c in range(0, width, COLS):
            got = nn(hot, de_ref[:, c:c + COLS])
            stage[:, :, c:c + COLS] = got.astype(BF16).reshape(GB, 8, COLS)

    def move(ci, go):
        base = ci * GB

        def one(i, c):
            b = blocks_ref[base + i]

            @pl.when(b < full)
            def _():
                go(put(b, i))
            @pl.when(b >= full)
            def _():
                tail_ref[...] = stage[i]
            return c

        lax.fori_loop(0, jnp.minimum(GB, count - base), one, 0)

    def chunk(ci, carry):
        sums(ci)
        move(ci, lambda cp: cp.start())
        move(ci, lambda cp: cp.wait())
        return carry

    lax.fori_loop(0, (count + GB - 1) // GB, chunk, 0)


def table_grad(key, blocks, count, pieces, table):
    (vocab, width), rows = table.shape, key.shape[0]
    latw = pieces[0].shape[1] - width
    smem, vmem, anym = (pl.BlockSpec(memory_space=m) for m in (pltpu.SMEM, VM, pl.ANY))
    full = vocab // 8 * 8
    out, tail, lat = pl.pallas_call(
        table_grad_body, out_shape=[shape((vocab, width), BF16), shape((8, width), BF16), shape((rows, latw), BF16)],
        in_specs=[smem, smem, vmem, anym] + [vmem] * len(pieces), input_output_aliases={3: 0},
        out_specs=[anym, vmem, vmem],
        scratch_shapes=[VM((rows, width), BF16), VM((GB, 8, width), BF16), pltpu.SemaphoreType.DMA],
        compiler_params=pltpu.CompilerParams(vmem_limit_bytes=LIMIT), name='table_grad',
    )(count, blocks, key[None, :], table, *pieces)
    return lax.dynamic_update_slice(out, tail[:vocab - full], (full, 0)), lat


def heads_of(q_ref, kn_ref, kp_ref, cos_ref, sin_ref, nope, half):
    q_pe = q_ref[nope:, :].astype(F32)
    lo, hi, cos_t, sin_t = q_pe[:half], q_pe[half:], cos_ref[...], sin_ref[...]
    q_all = jnp.concatenate([q_ref[:nope, :], (lo * cos_t - hi * sin_t).astype(BF16), (hi * cos_t + lo * sin_t).astype(BF16)], axis=0)
    return q_all, jnp.concatenate([kn_ref[...], kp_ref[...]], axis=0)


def scores_of(k_all, q_all, ki, qi, scale):
    s = tn(k_all[:, ki * QB:(ki + 1) * QB], q_all[:, qi * QB:(qi + 1) * QB]) * scale
    if ki == qi:
        keys = lax.broadcasted_iota(jnp.int32, (QB, QB), 0)
        s = jnp.where(keys <= lax.broadcasted_iota(jnp.int32, (QB, QB), 1), s, -1e30)
    return s


def attn_fwd_body(q_ref, kn_ref, kp_ref, v_ref, cos_ref, sin_ref, o_ref, lse_ref):
    nope, half = kn_ref.shape[0], cos_ref.shape[0]
    scale = q_ref.shape[0] ** -0.5 * LOG2E
    q_all, k_all = heads_of(q_ref, kn_ref, kp_ref, cos_ref, sin_ref, nope, half)
    for qi in range(q_ref.shape[1] // QB):
        lanes = slice(qi * QB, (qi + 1) * QB)
        s = [scores_of(k_all, q_all, ki, qi, scale) for ki in range(qi + 1)]
        top = functools.reduce(jnp.maximum, [jnp.max(x, axis=0, keepdims=True) for x in s])
        p = [jnp.exp2(x - top) for x in s]
        total = sum(sum_rows(x) for x in p)
        inv = 1.0 / total
        o = sum(nn(v_ref[:, ki * QB:(ki + 1) * QB], (x * inv).astype(BF16)) for ki, x in enumerate(p))
        o_ref[:, lanes] = o.astype(BF16)
        lse_ref[0, :, lanes] = top + jnp.log2(total)


def attn_bwd_body(q_ref, kn_ref, kp_ref, v_ref, cos_ref, sin_ref, lse_ref, do_ref, dq_ref, dkn_ref, dv_ref, dkp_ref, table_ref, dk_acc, dv_acc, zero, zsem):
    full = table_ref.shape[0] // 8 * 8
    fills = [pltpu.make_async_copy(zero.at[pl.ds(0, n), :], table_ref.at[pl.ds(r, n), :], zsem.at[k])
             for k, (r, n) in enumerate((r, min(ZR, full - r)) for r in range(0, full, ZR))]

    @pl.when(pl.program_id(0) == 0)
    def _():
        zero[...] = jnp.zeros_like(zero)
        for cp in fills:
            cp.start()

    nope, half = kn_ref.shape[0], cos_ref.shape[0]
    raw = q_ref.shape[0] ** -0.5
    q_all, k_all = heads_of(q_ref, kn_ref, kp_ref, cos_ref, sin_ref, nope, half)
    dk_acc[...] = jnp.zeros_like(dk_acc)
    dv_acc[...] = jnp.zeros_like(dv_acc)
    for qi in range(q_ref.shape[1] // QB):
        lanes = slice(qi * QB, (qi + 1) * QB)
        q_b, do_b, lse = q_all[:, lanes], do_ref[:, lanes], lse_ref[0, :, lanes]
        p = [jnp.exp2(scores_of(k_all, q_all, ki, qi, raw * LOG2E) - lse) for ki in range(qi + 1)]
        dp = [tn(v_ref[:, ki * QB:(ki + 1) * QB], do_b) for ki in range(qi + 1)]
        delta = sum(sum_rows(a * b) for a, b in zip(p, dp))
        dq = None
        for ki in range(qi + 1):
            keys = slice(ki * QB, (ki + 1) * QB)
            ds = (p[ki] * (dp[ki] - delta) * raw).astype(BF16)
            part = nn(k_all[:, keys], ds)
            dq = part if dq is None else dq + part
            dk_acc[:, keys] += nt(q_b, ds)
            dv_acc[:, keys] += nt(do_b, p[ki].astype(BF16))
        cos_t, sin_t = cos_ref[:, lanes], sin_ref[:, lanes]
        lo, hi = dq[nope:nope + half], dq[nope + half:]
        dq_ref[:nope, lanes] = dq[:nope].astype(BF16)
        dq_ref[nope:nope + half, lanes] = (lo * cos_t + hi * sin_t).astype(BF16)
        dq_ref[nope + half:, lanes] = (hi * cos_t - lo * sin_t).astype(BF16)
    dkn_ref[...] = dk_acc[:nope, :].astype(BF16)
    dv_ref[...] = dv_acc[...].astype(BF16)

    @pl.when(pl.program_id(0) == 0)
    def _():
        dkp_ref[...] = jnp.zeros_like(dkp_ref)
    dkp_ref[...] += dk_acc[nope:, :]

    @pl.when(pl.program_id(0) == pl.num_programs(0) - 1)
    def _():
        for cp in fills:
            cp.wait()


def attn_specs(heads, qd, nope, rope, vd, seq):
    per = lambda r: pl.BlockSpec((r, seq), lambda h: (h, 0))
    one = lambda r: pl.BlockSpec((r, seq), lambda h: (0, 0))
    return [per(qd), per(nope), one(rope), per(vd), one(rope // 2), one(rope // 2)], per, one, pl.BlockSpec((1, 1, seq), lambda h: (h, 0, 0))


def attend_bwd(q, kn, kp, v, cos_t, sin_t, lse, do, heads, table):
    seq, qd, nope, vd, rope = q.shape[1], q.shape[0] // heads, kn.shape[0] // heads, v.shape[0] // heads, kp.shape[0]
    ins, per, one, lse_spec = attn_specs(heads, qd, nope, rope, vd, seq)
    return pl.pallas_call(
        attn_bwd_body, grid=(heads,), in_specs=ins + [lse_spec, per(vd)], out_specs=[per(qd), per(nope), per(vd), one(rope), pl.BlockSpec(memory_space=pl.ANY)],
        out_shape=[jax.ShapeDtypeStruct(q.shape, BF16), jax.ShapeDtypeStruct(kn.shape, BF16), jax.ShapeDtypeStruct(v.shape, BF16), jax.ShapeDtypeStruct(kp.shape, F32), jax.ShapeDtypeStruct(table, BF16)],
        scratch_shapes=[VM((qd, seq), F32), VM((vd, seq), F32), VM((ZR, table[1]), BF16), pltpu.SemaphoreType.DMA((-(-table[0] // ZR),))],
        compiler_params=pltpu.CompilerParams(vmem_limit_bytes=LIMIT), name='attend_bwd',
    )(q, kn, kp, v, cos_t, sin_t, lse, do)


def shift(x, bit):
    return lax.ppermute(x, 'tp', [(d, d ^ bit) for d in range(8)])


PAIR, XBIT, YBIT = 1, 2, 4


def hop_order():
    me = lax.axis_index('tp')
    flip = lambda v, bit: v + bit - 2 * bit * ((v // bit) % 2)
    own = [me, flip(me, XBIT), flip(me, YBIT), flip(flip(me, XBIT), YBIT)]
    return own + [flip(d, PAIR) for d in own]


def to_hop_order(x, axis):
    n = x.shape[axis] // 8
    return jnp.concatenate([lax.dynamic_slice_in_dim(x, d * n, n, axis) for d in hop_order()], axis=axis)


class Exchange:
    def __init__(self, widths, pieces):
        self.widths, self.pieces = widths, pieces
        self.order = range(len(pieces))

    def rs_scratch(self, rows):
        n = len(self.pieces)
        out = []
        for w in self.widths:
            out += [VM((4, rows, w), BF16), VM((2, rows, w), BF16), VM((2, rows, w), BF16), VM((rows, w), BF16), VM((rows, w), BF16)]
        dma = pltpu.SemaphoreType.DMA
        return out + [dma((4, n)), dma((4, n)), dma((2, n)), dma((2, n)), dma((n,)), dma((n,))]

    def ag_scratch(self):
        n = len(self.pieces)
        dma = pltpu.SemaphoreType.DMA
        return [dma((2, n)), dma((2, n)), dma((n,)), dma((n,)), dma((4, n)), dma((4, n))]

    def place(self, rows):
        me = lax.axis_index('tp')
        core, x, y = me % 2, (me // 2) % 2, me // 4
        dev = lambda yy, xx, cc: (yy * 2 + xx) * 2 + cc
        self.me, self.rows = me, rows
        self.pn, self.xn, self.yn = dev(y, x, 1 - core), dev(y, 1 - x, core), dev(1 - y, x, core)
        chips = [(y, x), (y, 1 - x), (1 - y, x), (1 - y, 1 - x)]
        at = lambda d: pl.ds(pl.multiple_of(d * rows, rows), rows)
        self.mine = [at(dev(*ch, core)) for ch in chips]
        self.theirs = [at(dev(*ch, 1 - core)) for ch in chips]
        self.chip = [pl.ds(pl.multiple_of(dev(*ch, 0) * rows, 2 * rows), 2 * rows) for ch in chips]

    def enter(self):
        sem = pltpu.get_barrier_semaphore()
        near = (self.pn, self.xn, self.yn)
        for d in near:
            pl.semaphore_signal(sem, inc=1, device_id={'tp': d}, device_id_type=pl.DeviceIdType.MESH)
        pl.semaphore_wait(sem, len(near))

    def copy(self, src, dst, ssem, rsem, dev):
        return pltpu.make_async_remote_copy(src_ref=src, dst_ref=dst, send_sem=ssem, recv_sem=rsem, device_id={'tp': dev}, device_id_type=pl.DeviceIdType.MESH)

    def saver(self, src, dst, sem):
        return [pltpu.make_async_copy(src.at[rows, :], dst.at[rows, :], sem.at[j]) for j, rows in enumerate(self.chip)]

    def rs_begin(self, parts, scratch):
        na = len(self.widths)
        self.parts = parts
        self.bufs = [scratch[5 * a:5 * a + 5] for a in range(na)]
        ds, dr, s1, r1, s2, r2 = scratch[5 * na:5 * na + 6]
        self.pair, self.hop1, self.hop2 = {}, {}, {}
        for i, (h, a, c0, cn) in enumerate(self.pieces):
            cols = pl.ds(c0, cn)
            dbuf, sb1, rb1, sb2, rb2 = self.bufs[a]
            for j in range(4):
                self.pair[j, i] = self.copy(parts[a].at[self.theirs[j], cols], dbuf.at[j, :, cols], ds.at[j, i], dr.at[j, i], self.pn)
            to1, to2 = (self.xn, self.yn) if h == 0 else (self.yn, self.xn)
            for k in range(2):
                self.hop1[k, i] = self.copy(sb1.at[k, :, cols], rb1.at[k, :, cols], s1.at[k, i], r1.at[k, i], to1)
            self.hop2[i] = self.copy(sb2.at[:, cols], rb2.at[:, cols], s2.at[i], r2.at[i], to2)

    def ready(self, j):
        for i in self.order:
            self.pair[j, i].start()

    def chip_sum(self, j, i):
        h, a, c0, cn = self.pieces[i]
        self.pair[j, i].wait_recv()
        return self.parts[a][self.mine[j], c0:c0 + cn].astype(F32) + self.bufs[a][0][j, :, c0:c0 + cn].astype(F32)

    def push(self, j):
        for i in self.order:
            h, a, c0, cn = self.pieces[i]
            if j == 3 or j == 1 + h:
                k = 1 if j == 3 else 0
                self.bufs[a][1][k, :, c0:c0 + cn] = self.chip_sum(j, i).astype(BF16)
                self.hop1[k, i].start()

    def relay(self):
        for i in self.order:
            h, a, c0, cn = self.pieces[i]
            own = self.chip_sum(2 - h, i)
            self.hop1[1, i].wait_recv()
            self.bufs[a][3][:, c0:c0 + cn] = (own + self.bufs[a][2][1, :, c0:c0 + cn].astype(F32)).astype(BF16)
            self.hop2[i].start()

    def land(self, accs):
        for i in self.order:
            h, a, c0, cn = self.pieces[i]
            own = self.chip_sum(0, i)
            self.hop1[0, i].wait_recv()
            own = own + self.bufs[a][2][0, :, c0:c0 + cn].astype(F32)
            self.hop2[i].wait_recv()
            accs[a][:, c0:c0 + cn] = own + self.bufs[a][4][:, c0:c0 + cn].astype(F32)

    def drain(self):
        for cp in list(self.pair.values()) + list(self.hop1.values()) + list(self.hop2.values()):
            cp.wait_send()

    def reduce_scatter(self, accs, produce):
        late = None
        for j in (3, 1, 2, 0):
            produce(j)
            self.ready(j)
            if late:
                self.push(late)
            late = j
        self.relay()
        self.land(accs)

    def all_gather(self, fulls, scratch, arrive, slow=False):
        os_, xr, fs, fr, ps, pr = scratch
        half0 = [i for i in self.order if self.pieces[i][0] == 0]
        half1 = [i for i in self.order if self.pieces[i][0] == 1]

        def to(i, j, ssem, rsem, dev, rows=None):
            h, a, c0, cn = self.pieces[i]
            ref = fulls[a].at[(rows or self.mine)[j], pl.ds(c0, cn)]
            return self.copy(ref, ref, ssem, rsem, dev)

        near = (self.xn, self.yn)
        own = [[to(i, 0, os_.at[k, i], xr.at[k, i], dev) for i in self.order] for k, dev in enumerate(near)]
        from_n = [[to(i, 1 + k, os_.at[k, i], xr.at[k, i], dev) for i in self.order] for k, dev in enumerate(near)]
        fwd = [to(i, 2 - self.pieces[i][0], fs.at[i], fr.at[i], near[self.pieces[i][0]]) for i in self.order]
        diag = [to(i, 3, fs.at[i], fr.at[i], self.xn) for i in self.order]
        give = [[to(i, j, ps.at[j, i], pr.at[j, i], self.pn) for i in self.order] for j in range(4)]
        take = [[to(i, j, ps.at[j, i], pr.at[j, i], self.pn, self.theirs) for i in self.order] for j in range(4)]
        for i0, i1 in zip(half0, half1):
            own[0][i1].start()
            own[1][i0].start()
        for i0, i1 in zip(half0, half1):
            own[0][i0].start()
            own[1][i1].start()
        for cp in give[0]:
            cp.start()
        for cp in take[0]:
            cp.wait_recv()
        arrive(0)
        for i0, i1 in zip(half0, half1):
            from_n[1][i0].wait_recv()
            fwd[i0].start()
            give[2][i0].start()
            from_n[0][i1].wait_recv()
            fwd[i1].start()
            give[1][i1].start()
        for i0, i1 in zip(half0, half1):
            from_n[1][i1].wait_recv()
            give[2][i1].start()
            from_n[0][i0].wait_recv()
            give[1][i0].start()
        def diagonal():
            for i in self.order:
                diag[i].wait_recv()
                give[3][i].start()

        for j in (1, 2):
            for cp in take[j]:
                cp.wait_recv()
            arrive(j)
            if slow == (j == 1):
                diagonal()
        for cp in take[3]:
            cp.wait_recv()
        arrive(3)
        for cp in own[0] + own[1] + fwd + [c for g in give for c in g]:
            cp.wait_send()


def halves(width, n):
    step = width // (2 * n)
    return [(h, 0, (h * n + k) * step, step) for k in range(n) for h in range(2)]


MAIN = halves(2560, 2)
LAST = MAIN + [(0, 1, 0, 256), (1, 1, 256, 128)]
NRS, NAG = 11, 6
COLS = 512


def norm_rows(x, gain):
    return x * lax.rsqrt(mean_last(x * x) + EPSILON) * gain


def norm_rows_vjp(x, gain, dy):
    r = lax.rsqrt(mean_last(x * x) + EPSILON)
    gd = dy * gain
    dot = mean_last(gd * x)
    return r * gd - x * (r * r * r * dot), sum_rows(dy * x * r)


def exchange_call(body, name, cid, ins, out_shape, scratch, far=0, out=0, limit=50):
    vmem, hbm = pl.BlockSpec(memory_space=VM), pl.BlockSpec(memory_space=pltpu.HBM)
    return pl.pallas_call(
        body, out_shape=out_shape, in_specs=[vmem] * (len(ins) - far) + [hbm] * far, out_specs=[vmem] * (len(out_shape) - out) + [hbm] * out, scratch_shapes=scratch,
        compiler_params=pltpu.CompilerParams(vmem_limit_bytes=limit << 20, collective_id=cid, has_side_effects=True), name=name)(*ins)


def shape(dims, dtype):
    return jax.ShapeDtypeStruct(dims, dtype)


def idle(j):
    pass


def embed_body(part, gain, wq, wdkv, e_ref, q_ref, lat_ref, u_out, full, usem, acc, *scratch):
    ex = Exchange([part.shape[1]], MAIN)
    ex.place(acc.shape[0])
    ex.enter()
    ex.rs_begin([part], scratch)
    ex.reduce_scatter([acc], idle)
    e = acc[...].astype(BF16)
    e_ref[...] = e
    full[ex.mine[0], :] = norm_rows(e.astype(F32), gain[...]).astype(BF16)

    def arrive(j):
        u = full[ex.chip[j], :]
        q_ref[:, ex.chip[j]] = nt(wq[...], u).astype(BF16)
        lat_ref[ex.chip[j], :] = nt(u, wdkv[...])
        save[j].start()

    save = ex.saver(full, u_out, usem)
    ex.all_gather([full], scratch[NRS:], arrive)
    ex.drain()
    for cp in save:
        cp.wait()


def attn_body(lat, g_kv, wuk, wuv, q_ref, cos_ref, sin_ref, dy_ref, c_ref, kn_ref, kp_ref, v_ref, o_ref, lse_ref, dy_out, dyf, dsem, *scratch):
    ex = Exchange([dyf.shape[1]], MAIN)
    ex.place(dy_ref.shape[0])
    ex.enter()
    dyf[ex.mine[0], :] = dy_ref[...]
    lora, half, heads = c_ref.shape[1], cos_ref.shape[0], lse_ref.shape[0]
    per = lambda ref, h: ref.at[pl.ds(h * (ref.shape[0] // heads), ref.shape[0] // heads), :]

    save = ex.saver(dyf, dy_out, dsem)

    def arrive(j):
        save[j].start()
        if j:
            return
        c = norm_rows(lat[:, :lora], g_kv[...]).astype(BF16)
        c_ref[...] = c
        pe = lat[:, lora:].T
        lo, hi, cos_t, sin_t = pe[:half], pe[half:], cos_ref[...], sin_ref[...]
        kp_ref[...] = jnp.concatenate([lo * cos_t - hi * sin_t, hi * cos_t + lo * sin_t], axis=0).astype(BF16)
        kn_ref[...] = nt(wuk[...], c).astype(BF16)
        v_ref[...] = nt(wuv[...], c).astype(BF16)
        for h in range(heads):
            attn_fwd_body(per(q_ref, h), per(kn_ref, h), kp_ref, per(v_ref, h), cos_ref, sin_ref, per(o_ref, h), lse_ref.at[pl.ds(h, 1)])

    ex.all_gather([dyf], scratch, arrive)
    for cp in save:
        cp.wait()


def middle_body(o_ref, wo, e_ref, gain, dyl_ref, dy_hbm, wg_hbm, wu_hbm, wd_hbm,
                h_ref, y_ref, dres_ref, dgain_ref, do_ref, z_out, hid_out, dgate_out, dup_out, dfull_out,
                wall, dyb, act, part, ypart, z, acc, wsem, dsem, asem, zsem, fsem, *scratch):
    ex, ey = Exchange([part.shape[1]], MAIN), Exchange([part.shape[1]], MAIN)
    for e in (ex, ey):
        e.place(acc.shape[0])
    ex.enter()
    ffn = wd_hbm.shape[0]
    wg, wu, wd = (wall.at[pl.ds(k * ffn, ffn), :] for k in range(3))
    dfull = wall.at[pl.ds(0, part.shape[0]), :]
    loads = [pltpu.make_async_copy(a, b, wsem.at[k]) for k, (a, b) in enumerate(((wg_hbm, wg), (wu_hbm, wu), (wd_hbm, wd)))]
    dy_in = [pltpu.make_async_copy(dy_hbm.at[ex.chip[j], :], dyb.at[j % 2], dsem.at[j % 2]) for j in range(4)]
    for cp in loads + dy_in[:2]:
        cp.start()
    rs = 2 * NRS
    ex.rs_begin([part], scratch)
    ey.rs_begin([ypart], scratch[NRS:])
    width = part.shape[1]

    def attn_part(j):
        part[ex.chip[j], :] = tn(o_ref[:, ex.chip[j]], wo[...]).astype(BF16)

    ex.reduce_scatter([acc], attn_part)
    h = (e_ref[...].astype(F32) + acc[...].astype(BF16).astype(F32)).astype(BF16)
    h_ref[...] = h
    z[ex.mine[0], :] = norm_rows(h.astype(F32), gain[...]).astype(BF16)
    save_z, save_d = ex.saver(z, z_out, zsem), ex.saver(dfull, dfull_out, fsem)
    save_a = [[pltpu.make_async_copy(act.at[j % 2, k], dst.at[ex.chip[j], :], asem.at[j % 2, k]) for k, dst in enumerate((hid_out, dgate_out, dup_out))]
              for j in range(4)]

    def mlp(j):
        rows = ex.chip[j]
        gate, up = nt(z[rows, :], wg[...]), nt(z[rows, :], wu[...])
        sig = jax.nn.sigmoid(gate)
        hid = (gate * sig * up).astype(BF16)
        dh = nt(dyb[j % 2], wd[...])
        dup = (dh * gate * sig).astype(BF16)
        dgate = (dh * up * sig * (1.0 + gate * (1.0 - sig))).astype(BF16)
        if j > 1:
            for cp in save_a[j - 2]:
                cp.wait()
        for k, value in enumerate((hid, dgate, dup)):
            act[j % 2, k] = value
        for c in range(0, width, COLS):
            cols = slice(c, c + COLS)
            part[rows, cols] = (nn(dgate, wg[:, cols]) + nn(dup, wu[:, cols])).astype(BF16)
            ypart[rows, cols] = nn(hid, wd[:, cols]).astype(BF16)
        for cp in save_a[j]:
            cp.start()

    def arrive_z(j):
        if j == 0:
            ex.drain()
            for cp in loads:
                cp.wait()
        save_z[j].start()
        dy_in[j].wait()
        mlp(j)
        if j < 2:
            dy_in[j + 2].start()
        ex.ready(j)
        ey.ready(j)
        if j == 2:
            ex.push(1)
            ey.push(1)
        if j == 3:
            ex.push(2)
            ex.push(3)

    ex.all_gather([z], scratch[rs:rs + NAG], arrive_z, slow=True)
    ex.relay()
    ey.push(2)
    ey.push(3)
    ex.land([acc])
    ey.relay()
    dx, dgain_ref[...] = norm_rows_vjp(h_ref[...].astype(F32), gain[...], acc[...])
    dres = dyl_ref[...].astype(F32) + dx
    dres_ref[...] = dres
    dfull[ex.mine[0], :] = dres.astype(BF16)

    def arrive_d(j):
        do_ref[:, ex.chip[j]] = nt(wo[...], dfull[ex.chip[j], :]).astype(BF16)
        save_d[j].start()
        if j == 2:
            ey.land([acc])
            y_ref[...] = (h_ref[...].astype(F32) + acc[...].astype(BF16).astype(F32)).astype(BF16)

    ex.all_gather([dfull], scratch[rs + NAG:], arrive_d)
    ex.drain()
    ey.drain()
    for cp in save_z + save_d + save_a[2] + save_a[3]:
        cp.wait()


def attn_back_body(dq_ref, lat, wq, wdkv, e_ref, dres_ref, gain, de_ref, dg_ref, part, acc, acc_lat, *scratch):
    ex = Exchange([part.shape[1], lat.shape[1]], LAST)
    ex.place(acc.shape[0])
    ex.enter()
    ex.rs_begin([part, lat], scratch)
    lw = wdkv.shape[0]

    def produce(j):
        rows = ex.chip[j]
        part[rows, :] = (tn(dq_ref[:, rows], wq[...]) + nn(lat[rows, :lw], wdkv[...])).astype(BF16)

    ex.reduce_scatter([acc, acc_lat], produce)
    dx, dg_ref[...] = norm_rows_vjp(e_ref[...].astype(F32), gain[...], acc[...])
    de_ref[:, :dx.shape[1]] = (dres_ref[...] + dx).astype(BF16)
    de_ref[:, dx.shape[1]:] = acc_lat[...].astype(BF16)
    ex.drain()


def layer_pass(rows, d_out, w_q, w_dkv, g_kv, w_uk, w_uv, w_o, g_attn, g_mlp, w_gate, w_up, w_down, vocab, key, blocks, count):
    w_q, heads = w_q
    seq, width = rows.shape
    local = d_out.shape[0]
    lora = g_kv.shape[0]
    latw = w_dkv.shape[0]
    one = Exchange([width], MAIN)
    main = [VM((local, width), F32)] + one.rs_scratch(local) + one.ag_scratch()
    partb = [VM((seq, width), BF16)]
    dma = pltpu.SemaphoreType.DMA
    saved = partb + [dma((4,))]
    loc, fullb = shape((local, width), BF16), shape((seq, width), BF16)
    ga, gm = g_attn[None, :], g_mlp[None, :]
    embedded, query, latent, x_attn = exchange_call(
        embed_body, 'embed_exchange', 1, [rows, ga, w_q, w_dkv], [loc, shape((w_q.shape[0], seq), BF16), shape((seq, latw), F32), fullb], saved + main, out=1)
    cos_t, sin_t = (t.T for t in rope_tables(seq, latw - lora))
    nq, nk, nv = w_q.shape[0], w_uk.shape[0], w_uv.shape[0]
    c_kv, k_nope, k_pe_t, value, attn_out, lse, dy_full = exchange_call(
        attn_body, 'attend_fwd', 2, [latent, g_kv[None, :], w_uk, w_uv, query, cos_t, sin_t, d_out],
        [shape((seq, lora), BF16), shape((nk, seq), BF16), shape((latw - lora, seq), BF16), shape((nv, seq), BF16), shape((nv, seq), BF16),
         shape((heads, 1, seq), F32), fullb], saved + one.ag_scratch(), out=1)
    kv_pull = jax.vjp(kv_prep, latent, g_kv)[1]
    ffn = w_gate.shape[0]
    act = shape((seq, ffn), BF16)
    residual, layer_out, d_residual, dg_mlp, d_attn_out, x_mlp, hidden, d_gate, d_up, d_attn_full = exchange_call(
        middle_body, 'middle', 3, [attn_out, w_o, embedded, gm, d_out, dy_full, w_gate, w_up, w_down],
        [loc, loc, shape((local, width), F32), shape((1, width), F32), shape((w_o.shape[0], seq), BF16), fullb, act, act, act, fullb],
        [VM((3 * ffn, width), BF16), VM((2, seq // 4, width), BF16), VM((2, 3, seq // 4, ffn), BF16)] + partb * 3
        + [VM((local, width), F32), dma((3,)), dma((2,)), dma((2, 3)), dma((4,)), dma((4,))]
        + one.rs_scratch(local) * 2 + one.ag_scratch() * 2, far=4, out=5, limit=63)
    d_query, d_knope, d_value, d_kpe, table0 = attend_bwd(query, k_nope, k_pe_t, value, cos_t, sin_t, lse, d_attn_out, heads, (vocab, width))
    d_ckv = (tn(d_knope, w_uk) + tn(d_value, w_uv)).astype(BF16)
    d_latent, dg_kv = kv_pull((d_ckv, d_kpe.T.astype(BF16)))
    lat_part = jnp.pad(d_latent.astype(BF16), ((0, 0), (0, -latw % 128)))
    padw = lat_part.shape[1]
    two = Exchange([width, padw], LAST)
    de, dg_attn = exchange_call(
        attn_back_body, 'back_exchange', 4, [d_query, lat_part, w_q, w_dkv, embedded, d_residual, ga],
        [shape((local, width + padw), BF16), shape((1, width), F32)],
        partb + [VM((local, width), F32), VM((local, padw), F32)] + two.rs_scratch(local))
    later = lax.optimization_barrier
    dg = jnp.concatenate([dg_attn[0], dg_mlp[0], dg_kv])
    hidden, d_gate, d_up, d_query, de, dg = later((hidden, d_gate, d_up, d_query, de, dg))
    near = [shift(de, XBIT), shift(de, YBIT), shift(de, XBIT + YBIT)]
    pair = shift(de, PAIR)
    dg = dg + shift(dg, PAIR)
    dw_down, dw_gate, dw_up, dw_q = tn(hidden, dy_full), tn(d_gate, x_mlp), tn(d_up, x_mlp), nn(d_query, x_attn)
    dw_down, dw_gate, dw_up, dw_q, near, pair, dg, attn_out = later((dw_down, dw_gate, dw_up, dw_q, near, pair, dg, attn_out))
    far = [shift(b, PAIR) for b in near]
    dg = dg + shift(dg, XBIT)
    dw_o = nn(attn_out, d_attn_full)
    dw_o, far, dg, d_knope, d_value = later((dw_o, far, dg, d_knope, d_value))
    dg = dg + shift(dg, YBIT)
    dw_uk, dw_uv = nn(d_knope, c_kv), nn(d_value, c_kv)
    d_table, lat_full = table_grad(to_hop_order(key, 0), blocks, count, [de, *near, pair, *far], table0)
    dw_dkv = tn(lat_full[:, :latw], x_attn)
    dg_attn, dg_mlp, dg_kv = dg[:width], dg[width:2 * width], dg[2 * width:]
    return layer_out, d_table, (dw_q, dw_dkv, dg_kv, dw_uk, dw_uv, dw_o, dg_attn, dg_mlp, dw_gate, dw_up, dw_down)


def rows_of(w):
    return jnp.transpose(w, (1, 2, 0)).reshape(-1, w.shape[0])


def unrows(g, heads):
    return jnp.transpose(g.reshape(heads, -1, g.shape[1]), (2, 0, 1))


def solution(mesh):
    def device_step(tokens, embed_table, w_q, w_dkv, g_kv, w_uk, w_uv, w_o, g_attn, g_mlp, w_gate, w_up, w_down, d_out):
        vocab_local, model_dim = embed_table.shape
        heads = w_q.shape[1]
        key, blocks, count = block_index(tokens, vocab_local)
        rows = gather_rows(key, blocks, count, embed_table)
        layer_out, d_table, grads = layer_pass(
            rows, d_out[0], (rows_of(w_q), heads), w_dkv.T, g_kv, rows_of(w_uk), rows_of(w_uv), w_o.reshape(-1, model_dim),
            g_attn, g_mlp, w_gate.T, w_up.T, w_down, vocab_local, key, blocks, count)
        dw_q, dw_dkv, dg_kv, dw_uk, dw_uv, dw_o, dg_attn, dg_mlp, dw_gate, dw_up, dw_down = grads
        return (layer_out[None], d_table, unrows(dw_q, heads), dw_dkv.T, dg_kv, unrows(dw_uk, heads), unrows(dw_uv, heads),
                dw_o.reshape(w_o.shape), dg_attn, dg_mlp, dw_gate.T, dw_up.T, dw_down)

    row_spec = P('dp', 'tp', None)
    head_spec = P(None, 'tp', None)
    in_specs = (P('dp', None), P('tp', None), head_spec, P(None, None), P(None), head_spec, head_spec, P('tp', None, None), P(None), P(None), P(None, 'tp'), P(None, 'tp'), P('tp', None), row_spec)
    out_specs = (row_spec, P(('dp', 'tp'), None), P('dp', 'tp', None), P('dp', None), P('dp'), P('dp', 'tp', None), P('dp', 'tp', None), P(('dp', 'tp'), None, None), P('dp'), P('dp'), P('dp', 'tp'), P('dp', 'tp'), P(('dp', 'tp'), None))
    return jax.shard_map(device_step, mesh=mesh, in_specs=in_specs, out_specs=out_specs, check_vma=False)
```

```python
import functools

import jax
import jax.numpy as jnp
from jax import lax
from jax.experimental import pallas as pl
from jax.experimental.pallas import tpu as pltpu
from jax.sharding import PartitionSpec as P

EPSILON = 1e-6
ROPE_BASE = 10000.0
F32, BF16 = jnp.float32, jnp.bfloat16
LOG2E = 1.4426950408889634
VM = pltpu.VMEM
ZR = 248
GB = 64
GR = GB * 8
LIMIT = 40 << 20
ALL = 63
QB = 256


def mm(lhs, rhs, lc, rc):
    return lax.dot_general(lhs, rhs, (((lc,), (rc,)), ((), ())), preferred_element_type=F32)


def nn(a, b):
    return mm(a, b, 1, 0)


def nt(a, b):
    return mm(a, b, 1, 1)


def tn(a, b):
    return mm(a, b, 0, 0)


mean_last = functools.partial(jnp.mean, axis=-1, keepdims=True)
sum_rows = functools.partial(jnp.sum, axis=0, keepdims=True)


def rope_tables(seq_len, rope_dim):
    inv_freq = ROPE_BASE ** (-jnp.arange(0, rope_dim, 2, dtype=F32) / rope_dim)
    angles = jnp.arange(seq_len, dtype=F32)[:, None] * inv_freq[None, :]
    return jnp.cos(angles), jnp.sin(angles)


def apply_rope(x_in, cos_t, sin_t):
    half_dim = x_in.shape[-1] // 2
    x_lo, x_hi = x_in[..., :half_dim], x_in[..., half_dim:]
    return jnp.concatenate([x_lo * cos_t - x_hi * sin_t, x_hi * cos_t + x_lo * sin_t], axis=-1)


def rms_norm(x_in, gain):
    inv_rms = lax.rsqrt(mean_last(x_in * x_in) + EPSILON)
    return (x_in * inv_rms * gain).astype(BF16)


def kv_prep(latent, g_kv):
    lora = g_kv.shape[0]
    cos_t, sin_t = rope_tables(latent.shape[0], latent.shape[-1] - lora)
    k_pe = apply_rope(latent[:, lora:], cos_t, sin_t).astype(BF16)
    return rms_norm(latent[:, :lora], g_kv), k_pe


def block_index(tokens, vocab_local):
    ids = tokens.reshape(-1) - lax.axis_index('tp') * vocab_local
    n = ids.shape[0]
    owned = (ids >= 0) & (ids < vocab_local)
    blk = jnp.where(owned, ids >> 3, -1)
    pos = jnp.arange(n, dtype=jnp.int32)
    eq = (blk[:, None] == blk[None, :])
    first = jnp.min(jnp.where(eq, pos[None, :], n), axis=1)
    isf = owned & (first == pos)
    slot = jnp.sum((isf[None, :] & (pos[None, :] < first[:, None])).astype(jnp.int32), axis=1)
    key = jnp.where(owned, slot * 8 + (ids & 7), -1)
    blocks = jnp.sum(jnp.where(isf[None, :] & (slot[None, :] == pos[:, None]), blk[None, :], 0), axis=1)
    count = jnp.sum(isf.astype(jnp.int32)).reshape(1)
    return key, blocks, count


def gather_body(count_ref, blocks_ref, key_ref, tail_ref, table_ref, out_ref, stage, sem):
    rows, width = out_ref.shape
    full = table_ref.shape[0] // 8
    stage[...] = jnp.zeros_like(stage)
    out_ref[...] = jnp.zeros_like(out_ref)
    count = count_ref[0]

    def fetch(b, i):
        return pltpu.make_async_copy(table_ref.at[pl.ds(pl.multiple_of(b * 8, 8), 8), :], stage.at[i], sem)

    def chunk(ci, carry):
        base = ci * GB
        n = jnp.minimum(GB, count - base)

        def start(i, c):
            b = blocks_ref[base + i]

            @pl.when(b < full)
            def _():
                fetch(b, i).start()

            @pl.when(b >= full)
            def _():
                stage[i] = tail_ref[...]
            return c

        def wait(i, c):
            b = blocks_ref[base + i]

            @pl.when(b < full)
            def _():
                fetch(b, i).wait()
            return c

        lax.fori_loop(0, n, start, 0)
        lax.fori_loop(0, n, wait, 0)
        cols = lax.broadcasted_iota(jnp.int32, (rows, GR), 1) + base * 8
        hot = jnp.where(cols == key_ref[...], 1.0, 0.0).astype(BF16)
        for c in range(0, width, COLS):
            got = nn(hot, stage[:, :, c:c + COLS].reshape(GR, COLS))
            out_ref[:, c:c + COLS] += got.astype(BF16)
        return carry

    lax.fori_loop(0, (count + GB - 1) // GB, chunk, 0)


def gather_rows(key, blocks, count, table):
    rows, (vocab, width) = key.shape[0], table.shape
    full = vocab // 8 * 8
    tail = jnp.pad(table[full:], ((0, 8 - (vocab - full)), (0, 0)))
    smem = pl.BlockSpec(memory_space=pltpu.SMEM)
    return pl.pallas_call(
        gather_body, out_shape=jax.ShapeDtypeStruct((rows, width), BF16),
        in_specs=[smem, smem, pl.BlockSpec(memory_space=VM), pl.BlockSpec(memory_space=VM), pl.BlockSpec(memory_space=pl.ANY)],
        out_specs=pl.BlockSpec(memory_space=VM),
        scratch_shapes=[VM((GB, 8, width), BF16), pltpu.SemaphoreType.DMA],
        compiler_params=pltpu.CompilerParams(vmem_limit_bytes=LIMIT), name='gather_rows',
    )(count, blocks, key[:, None], tail, table)


def table_grad_body(count_ref, blocks_ref, key_ref, zeros_ref, *refs):
    pieces, (out_ref, tail_ref, lat_ref, de_ref, stage, sem) = refs[:-6], refs[-6:]
    rows, width = de_ref.shape
    local = rows // len(pieces)
    for k, (piece, d) in enumerate(zip(pieces, hop_order())):
        de_ref[k * local:(k + 1) * local, :] = piece[:, :width]
        lat_ref[pl.ds(pl.multiple_of(d * local, local), local), :] = piece[:, width:]
    full = out_ref.shape[0] // 8
    tail_ref[...] = jnp.zeros_like(tail_ref)
    count = count_ref[0]

    def put(b, i):
        return pltpu.make_async_copy(stage.at[i], out_ref.at[pl.ds(pl.multiple_of(b * 8, 8), 8), :], sem)

    def sums(ci):
        ids = lax.broadcasted_iota(jnp.int32, (GR, rows), 0) + ci * GR
        hot = jnp.where(ids == key_ref[...], 1.0, 0.0).astype(BF16)
        for c in range(0, width, COLS):
            got = nn(hot, de_ref[:, c:c + COLS])
            stage[:, :, c:c + COLS] = got.astype(BF16).reshape(GB, 8, COLS)

    def move(ci, go):
        base = ci * GB

        def one(i, c):
            b = blocks_ref[base + i]

            @pl.when(b < full)
            def _():
                go(put(b, i))
            @pl.when(b >= full)
            def _():
                tail_ref[...] = stage[i]
            return c

        lax.fori_loop(0, jnp.minimum(GB, count - base), one, 0)

    def chunk(ci, carry):
        sums(ci)
        move(ci, lambda cp: cp.start())
        move(ci, lambda cp: cp.wait())
        return carry

    lax.fori_loop(0, (count + GB - 1) // GB, chunk, 0)


def table_grad(key, blocks, count, pieces, table):
    (vocab, width), rows = table.shape, key.shape[0]
    latw = pieces[0].shape[1] - width
    smem, vmem, anym = (pl.BlockSpec(memory_space=m) for m in (pltpu.SMEM, VM, pl.ANY))
    full = vocab // 8 * 8
    out, tail, lat = pl.pallas_call(
        table_grad_body, out_shape=[shape((vocab, width), BF16), shape((8, width), BF16), shape((rows, latw), BF16)],
        in_specs=[smem, smem, vmem, anym] + [vmem] * len(pieces), input_output_aliases={3: 0},
        out_specs=[anym, vmem, vmem],
        scratch_shapes=[VM((rows, width), BF16), VM((GB, 8, width), BF16), pltpu.SemaphoreType.DMA],
        compiler_params=pltpu.CompilerParams(vmem_limit_bytes=LIMIT), name='table_grad',
    )(count, blocks, key[None, :], table, *pieces)
    return lax.dynamic_update_slice(out, tail[:vocab - full], (full, 0)), lat


def heads_of(q_ref, kn_ref, kp_ref, cos_ref, sin_ref, nope, half):
    q_pe = q_ref[nope:, :].astype(F32)
    lo, hi, cos_t, sin_t = q_pe[:half], q_pe[half:], cos_ref[...], sin_ref[...]
    q_all = jnp.concatenate([q_ref[:nope, :], (lo * cos_t - hi * sin_t).astype(BF16), (hi * cos_t + lo * sin_t).astype(BF16)], axis=0)
    return q_all, jnp.concatenate([kn_ref[...], kp_ref[...]], axis=0)


def scores_of(k_all, q_all, ki, qi, scale):
    s = tn(k_all[:, ki * QB:(ki + 1) * QB], q_all[:, qi * QB:(qi + 1) * QB]) * scale
    if ki == qi:
        keys = lax.broadcasted_iota(jnp.int32, (QB, QB), 0)
        s = jnp.where(keys <= lax.broadcasted_iota(jnp.int32, (QB, QB), 1), s, -1e30)
    return s


def attn_fwd_body(q_ref, kn_ref, kp_ref, v_ref, cos_ref, sin_ref, o_ref, lse_ref):
    nope, half = kn_ref.shape[0], cos_ref.shape[0]
    scale = q_ref.shape[0] ** -0.5 * LOG2E
    q_all, k_all = heads_of(q_ref, kn_ref, kp_ref, cos_ref, sin_ref, nope, half)
    for qi in range(q_ref.shape[1] // QB):
        lanes = slice(qi * QB, (qi + 1) * QB)
        s = [scores_of(k_all, q_all, ki, qi, scale) for ki in range(qi + 1)]
        top = functools.reduce(jnp.maximum, [jnp.max(x, axis=0, keepdims=True) for x in s])
        p = [jnp.exp2(x - top) for x in s]
        total = sum(sum_rows(x) for x in p)
        inv = 1.0 / total
        o = sum(nn(v_ref[:, ki * QB:(ki + 1) * QB], (x * inv).astype(BF16)) for ki, x in enumerate(p))
        o_ref[:, lanes] = o.astype(BF16)
        lse_ref[0, :, lanes] = top + jnp.log2(total)


def attn_bwd_body(q_ref, kn_ref, kp_ref, v_ref, cos_ref, sin_ref, lse_ref, do_ref, dq_ref, dkn_ref, dv_ref, dkp_ref, table_ref, dk_acc, dv_acc, zero, zsem):
    full = table_ref.shape[0] // 8 * 8
    fills = [pltpu.make_async_copy(zero.at[pl.ds(0, n), :], table_ref.at[pl.ds(r, n), :], zsem.at[k])
             for k, (r, n) in enumerate((r, min(ZR, full - r)) for r in range(0, full, ZR))]

    @pl.when(pl.program_id(0) == 0)
    def _():
        zero[...] = jnp.zeros_like(zero)
        for cp in fills:
            cp.start()

    nope, half = kn_ref.shape[0], cos_ref.shape[0]
    raw = q_ref.shape[0] ** -0.5
    q_all, k_all = heads_of(q_ref, kn_ref, kp_ref, cos_ref, sin_ref, nope, half)
    dk_acc[...] = jnp.zeros_like(dk_acc)
    dv_acc[...] = jnp.zeros_like(dv_acc)
    for qi in range(q_ref.shape[1] // QB):
        lanes = slice(qi * QB, (qi + 1) * QB)
        q_b, do_b, lse = q_all[:, lanes], do_ref[:, lanes], lse_ref[0, :, lanes]
        p = [jnp.exp2(scores_of(k_all, q_all, ki, qi, raw * LOG2E) - lse) for ki in range(qi + 1)]
        dp = [tn(v_ref[:, ki * QB:(ki + 1) * QB], do_b) for ki in range(qi + 1)]
        delta = sum(sum_rows(a * b) for a, b in zip(p, dp))
        dq = None
        for ki in range(qi + 1):
            keys = slice(ki * QB, (ki + 1) * QB)
            ds = (p[ki] * (dp[ki] - delta) * raw).astype(BF16)
            part = nn(k_all[:, keys], ds)
            dq = part if dq is None else dq + part
            dk_acc[:, keys] += nt(q_b, ds)
            dv_acc[:, keys] += nt(do_b, p[ki].astype(BF16))
        cos_t, sin_t = cos_ref[:, lanes], sin_ref[:, lanes]
        lo, hi = dq[nope:nope + half], dq[nope + half:]
        dq_ref[:nope, lanes] = dq[:nope].astype(BF16)
        dq_ref[nope:nope + half, lanes] = (lo * cos_t + hi * sin_t).astype(BF16)
        dq_ref[nope + half:, lanes] = (hi * cos_t - lo * sin_t).astype(BF16)
    dkn_ref[...] = dk_acc[:nope, :].astype(BF16)
    dv_ref[...] = dv_acc[...].astype(BF16)

    @pl.when(pl.program_id(0) == 0)
    def _():
        dkp_ref[...] = jnp.zeros_like(dkp_ref)
    dkp_ref[...] += dk_acc[nope:, :]

    @pl.when(pl.program_id(0) == pl.num_programs(0) - 1)
    def _():
        for cp in fills:
            cp.wait()


def attn_specs(heads, qd, nope, rope, vd, seq):
    per = lambda r: pl.BlockSpec((r, seq), lambda h: (h, 0))
    one = lambda r: pl.BlockSpec((r, seq), lambda h: (0, 0))
    return [per(qd), per(nope), one(rope), per(vd), one(rope // 2), one(rope // 2)], per, one, pl.BlockSpec((1, 1, seq), lambda h: (h, 0, 0))


def attend_bwd(q, kn, kp, v, cos_t, sin_t, lse, do, heads, table):
    seq, qd, nope, vd, rope = q.shape[1], q.shape[0] // heads, kn.shape[0] // heads, v.shape[0] // heads, kp.shape[0]
    ins, per, one, lse_spec = attn_specs(heads, qd, nope, rope, vd, seq)
    return pl.pallas_call(
        attn_bwd_body, grid=(heads,), in_specs=ins + [lse_spec, per(vd)], out_specs=[per(qd), per(nope), per(vd), one(rope), pl.BlockSpec(memory_space=pl.ANY)],
        out_shape=[jax.ShapeDtypeStruct(q.shape, BF16), jax.ShapeDtypeStruct(kn.shape, BF16), jax.ShapeDtypeStruct(v.shape, BF16), jax.ShapeDtypeStruct(kp.shape, F32), jax.ShapeDtypeStruct(table, BF16)],
        scratch_shapes=[VM((qd, seq), F32), VM((vd, seq), F32), VM((ZR, table[1]), BF16), pltpu.SemaphoreType.DMA((-(-table[0] // ZR),))],
        compiler_params=pltpu.CompilerParams(vmem_limit_bytes=ALL << 20), name='attend_bwd',
    )(q, kn, kp, v, cos_t, sin_t, lse, do)


def shift(x, bit):
    return lax.ppermute(x, 'tp', [(d, d ^ bit) for d in range(8)])


PAIR, XBIT, YBIT = 1, 2, 4


def hop_order():
    me = lax.axis_index('tp')
    flip = lambda v, bit: v + bit - 2 * bit * ((v // bit) % 2)
    own = [me, flip(me, XBIT), flip(me, YBIT), flip(flip(me, XBIT), YBIT)]
    return own + [flip(d, PAIR) for d in own]


def to_hop_order(x, axis):
    n = x.shape[axis] // 8
    return jnp.concatenate([lax.dynamic_slice_in_dim(x, d * n, n, axis) for d in hop_order()], axis=axis)


class Exchange:
    def __init__(self, widths, pieces):
        self.widths, self.pieces = widths, pieces
        self.order = range(len(pieces))

    def rs_scratch(self, rows):
        n = len(self.pieces)
        out = []
        for w in self.widths:
            out += [VM((4, rows, w), BF16), VM((2, rows, w), BF16), VM((2, rows, w), BF16), VM((rows, w), BF16), VM((rows, w), BF16)]
        dma = pltpu.SemaphoreType.DMA
        return out + [dma((4, n)), dma((4, n)), dma((2, n)), dma((2, n)), dma((n,)), dma((n,))]

    def ag_scratch(self):
        n = len(self.pieces)
        dma = pltpu.SemaphoreType.DMA
        return [dma((2, n)), dma((2, n)), dma((n,)), dma((n,)), dma((4, n)), dma((4, n))]

    def place(self, rows):
        me = lax.axis_index('tp')
        core, x, y = me % 2, (me // 2) % 2, me // 4
        dev = lambda yy, xx, cc: (yy * 2 + xx) * 2 + cc
        self.me, self.rows = me, rows
        self.pn, self.xn, self.yn = dev(y, x, 1 - core), dev(y, 1 - x, core), dev(1 - y, x, core)
        chips = [(y, x), (y, 1 - x), (1 - y, x), (1 - y, 1 - x)]
        at = lambda d: pl.ds(pl.multiple_of(d * rows, rows), rows)
        self.mine = [at(dev(*ch, core)) for ch in chips]
        self.theirs = [at(dev(*ch, 1 - core)) for ch in chips]
        self.chip = [pl.ds(pl.multiple_of(dev(*ch, 0) * rows, 2 * rows), 2 * rows) for ch in chips]

    def enter(self):
        sem = pltpu.get_barrier_semaphore()
        near = (self.pn, self.xn, self.yn)
        for d in near:
            pl.semaphore_signal(sem, inc=1, device_id={'tp': d}, device_id_type=pl.DeviceIdType.MESH)
        pl.semaphore_wait(sem, len(near))

    def copy(self, src, dst, ssem, rsem, dev):
        return pltpu.make_async_remote_copy(src_ref=src, dst_ref=dst, send_sem=ssem, recv_sem=rsem, device_id={'tp': dev}, device_id_type=pl.DeviceIdType.MESH)

    def saver(self, src, dst, sem):
        return [pltpu.make_async_copy(src.at[rows, :], dst.at[rows, :], sem.at[j]) for j, rows in enumerate(self.chip)]

    def rs_begin(self, parts, scratch):
        na = len(self.widths)
        self.parts = parts
        self.bufs = [scratch[5 * a:5 * a + 5] for a in range(na)]
        ds, dr, s1, r1, s2, r2 = scratch[5 * na:5 * na + 6]
        self.pair, self.hop1, self.hop2 = {}, {}, {}
        for i, (h, a, c0, cn) in enumerate(self.pieces):
            cols = pl.ds(c0, cn)
            dbuf, sb1, rb1, sb2, rb2 = self.bufs[a]
            for j in range(4):
                self.pair[j, i] = self.copy(parts[a].at[self.theirs[j], cols], dbuf.at[j, :, cols], ds.at[j, i], dr.at[j, i], self.pn)
            to1, to2 = (self.xn, self.yn) if h == 0 else (self.yn, self.xn)
            for k in range(2):
                self.hop1[k, i] = self.copy(sb1.at[k, :, cols], rb1.at[k, :, cols], s1.at[k, i], r1.at[k, i], to1)
            self.hop2[i] = self.copy(sb2.at[:, cols], rb2.at[:, cols], s2.at[i], r2.at[i], to2)

    def ready(self, j):
        for i in self.order:
            self.pair[j, i].start()

    def chip_sum(self, j, i):
        h, a, c0, cn = self.pieces[i]
        self.pair[j, i].wait_recv()
        return self.parts[a][self.mine[j], c0:c0 + cn].astype(F32) + self.bufs[a][0][j, :, c0:c0 + cn].astype(F32)

    def push(self, j):
        for i in self.order:
            h, a, c0, cn = self.pieces[i]
            if j == 3 or j == 1 + h:
                k = 1 if j == 3 else 0
                self.bufs[a][1][k, :, c0:c0 + cn] = self.chip_sum(j, i).astype(BF16)
                self.hop1[k, i].start()

    def relay(self, halves=(0, 1)):
        for i in self.order:
            h, a, c0, cn = self.pieces[i]
            if h not in halves:
                continue
            own = self.chip_sum(2 - h, i)
            self.hop1[1, i].wait_recv()
            self.bufs[a][3][:, c0:c0 + cn] = (own + self.bufs[a][2][1, :, c0:c0 + cn].astype(F32)).astype(BF16)
            self.hop2[i].start()

    def land(self, accs):
        for i in self.order:
            h, a, c0, cn = self.pieces[i]
            own = self.chip_sum(0, i)
            self.hop1[0, i].wait_recv()
            own = own + self.bufs[a][2][0, :, c0:c0 + cn].astype(F32)
            self.hop2[i].wait_recv()
            accs[a][:, c0:c0 + cn] = own + self.bufs[a][4][:, c0:c0 + cn].astype(F32)

    def drain(self):
        for cp in list(self.pair.values()) + list(self.hop1.values()) + list(self.hop2.values()):
            cp.wait_send()

    def reduce_scatter(self, accs, produce):
        late = None
        for j in (3, 1, 2, 0):
            produce(j)
            self.ready(j)
            if late:
                self.push(late)
            late = j
        self.relay()
        self.land(accs)

    def all_gather(self, fulls, scratch, arrive, blocks=(1, 2, 3), known=False):
        os_, xr, fs, fr, ps, pr = scratch
        half0 = [i for i in self.order if self.pieces[i][0] == 0]
        half1 = [i for i in self.order if self.pieces[i][0] == 1]

        def to(i, j, ssem, rsem, dev, rows=None):
            h, a, c0, cn = self.pieces[i]
            ref = fulls[a].at[(rows or self.mine)[j], pl.ds(c0, cn)]
            return self.copy(ref, ref, ssem, rsem, dev)

        near = (self.xn, self.yn)
        own = [[to(i, 0, os_.at[k, i], xr.at[k, i], dev) for i in self.order] for k, dev in enumerate(near)]
        from_n = [[to(i, 1 + k, os_.at[k, i], xr.at[k, i], dev) for i in self.order] for k, dev in enumerate(near)]
        fwd = [to(i, 2 - self.pieces[i][0], fs.at[i], fr.at[i], near[self.pieces[i][0]]) for i in self.order]
        diag = [to(i, 3, fs.at[i], fr.at[i], self.xn) for i in self.order]
        give = [[to(i, j, ps.at[j, i], pr.at[j, i], self.pn) for i in self.order] for j in range(4)]
        take = [[to(i, j, ps.at[j, i], pr.at[j, i], self.pn, self.theirs) for i in self.order] for j in range(4)]
        pairs = list(zip(half0, half1))
        sent = fwd + [cp for g in give for cp in g]

        def start(copies):
            for cp in copies:
                cp.start()

        def landed(copies):
            for cp in copies:
                cp.wait_recv()

        if not known:
            sent += own[0] + own[1]
            for i0, i1 in pairs:
                start((own[0][i1], own[1][i0]))
            for i0, i1 in pairs:
                start((own[0][i0], own[1][i1]))
        start(give[0])
        if known:
            start(fwd + give[1] + give[2])
        landed(take[0])
        arrive(0)
        if not known:
            for i0, i1 in pairs:
                from_n[1][i0].wait_recv()
                start((fwd[i0], give[2][i0]))
                from_n[0][i1].wait_recv()
                start((fwd[i1], give[1][i1]))
            for i0, i1 in pairs:
                from_n[1][i1].wait_recv()
                give[2][i1].start()
                from_n[0][i0].wait_recv()
                give[1][i0].start()
        for j in blocks:
            if j == 3:
                for i in self.order:
                    diag[i].wait_recv()
                    give[3][i].start()
            landed(take[j])
            arrive(j)
        for cp in sent:
            cp.wait_send()


def halves(width, n):
    step = width // (2 * n)
    return [(h, 0, (h * n + k) * step, step) for k in range(n) for h in range(2)]


MAIN = halves(2560, 2)
LAST = MAIN + [(0, 1, 0, 256), (1, 1, 256, 128)]
NRS, NAG = 11, 6
COLS = 512


def norm_rows(x, gain):
    return x * lax.rsqrt(mean_last(x * x) + EPSILON) * gain


def norm_rows_vjp(x, gain, dy):
    r = lax.rsqrt(mean_last(x * x) + EPSILON)
    gd = dy * gain
    dot = mean_last(gd * x)
    return r * gd - x * (r * r * r * dot), sum_rows(dy * x * r)


def exchange_call(body, name, cid, ins, out_shape, scratch, far=0, out=0, limit=50):
    vmem, hbm = pl.BlockSpec(memory_space=VM), pl.BlockSpec(memory_space=pltpu.HBM)
    return pl.pallas_call(
        body, out_shape=out_shape, in_specs=[vmem] * (len(ins) - far) + [hbm] * far, out_specs=[vmem] * (len(out_shape) - out) + [hbm] * out, scratch_shapes=scratch,
        compiler_params=pltpu.CompilerParams(vmem_limit_bytes=limit << 20, collective_id=cid, has_side_effects=True), name=name)(*ins)


def shape(dims, dtype):
    return jax.ShapeDtypeStruct(dims, dtype)


def idle(j):
    pass


def embed_body(part, gain, wq, wdkv, e_ref, q_ref, lat_ref, u_out, full, usem, acc, *scratch):
    ex = Exchange([part.shape[1]], MAIN)
    ex.place(acc.shape[0])
    ex.enter()
    ex.rs_begin([part], scratch)
    ex.reduce_scatter([acc], idle)
    e = acc[...].astype(BF16)
    e_ref[...] = e
    full[ex.mine[0], :] = norm_rows(e.astype(F32), gain[...]).astype(BF16)

    def arrive(j):
        u = full[ex.chip[j], :]
        q_ref[:, ex.chip[j]] = nt(wq[...], u).astype(BF16)
        lat_ref[ex.chip[j], :] = nt(u, wdkv[...])
        save[j].start()

    save = ex.saver(full, u_out, usem)
    ex.all_gather([full], scratch[NRS:], arrive)
    ex.drain()
    for cp in save:
        cp.wait()


def attn_body(lat, g_kv, wuk, wuv, q_ref, cos_ref, sin_ref, dy_ref, dyx_ref, dyy_ref, c_ref, kn_ref, kp_ref, v_ref, o_ref, lse_ref, dy_out, dyf, dsem, *scratch):
    ex = Exchange([dyf.shape[1]], MAIN)
    ex.place(dy_ref.shape[0])
    ex.enter()
    for rows, ref in zip(ex.mine, (dy_ref, dyx_ref, dyy_ref)):
        dyf[rows, :] = ref[...]
    lora, half, heads = c_ref.shape[1], cos_ref.shape[0], lse_ref.shape[0]
    per = lambda ref, h: ref.at[pl.ds(h * (ref.shape[0] // heads), ref.shape[0] // heads), :]

    save = ex.saver(dyf, dy_out, dsem)

    def arrive(j):
        save[j].start()
        if j:
            return
        c = norm_rows(lat[:, :lora], g_kv[...]).astype(BF16)
        c_ref[...] = c
        pe = lat[:, lora:].T
        lo, hi, cos_t, sin_t = pe[:half], pe[half:], cos_ref[...], sin_ref[...]
        kp_ref[...] = jnp.concatenate([lo * cos_t - hi * sin_t, hi * cos_t + lo * sin_t], axis=0).astype(BF16)
        kn_ref[...] = nt(wuk[...], c).astype(BF16)
        v_ref[...] = nt(wuv[...], c).astype(BF16)
        for h in range(heads):
            attn_fwd_body(per(q_ref, h), per(kn_ref, h), kp_ref, per(v_ref, h), cos_ref, sin_ref, per(o_ref, h), lse_ref.at[pl.ds(h, 1)])

    ex.all_gather([dyf], scratch, arrive, known=True)
    for cp in save:
        cp.wait()


def middle_body(o_ref, wo, e_ref, gain, dyl_ref, dy_hbm, wg_hbm, wu_hbm, wd_hbm,
                h_ref, y_ref, dres_ref, dgain_ref, do_ref, z_out, hid_out, dgate_out, dup_out, dfull_out,
                wall, dyb, act, part, ypart, z, acc, wsem, dsem, asem, zsem, fsem, *scratch):
    ex, ey = Exchange([part.shape[1]], MAIN), Exchange([part.shape[1]], MAIN)
    for e in (ex, ey):
        e.place(acc.shape[0])
    ex.enter()
    ffn = wd_hbm.shape[0]
    wg, wu, wd = (wall.at[pl.ds(k * ffn, ffn), :] for k in range(3))
    dfull = wall.at[pl.ds(0, part.shape[0]), :]
    loads = [pltpu.make_async_copy(a, b, wsem.at[k]) for k, (a, b) in enumerate(((wg_hbm, wg), (wu_hbm, wu), (wd_hbm, wd)))]
    turns = (0, 1, 3, 2)
    dy_in = [pltpu.make_async_copy(dy_hbm.at[ex.chip[j], :], dyb.at[k % 2], dsem.at[k % 2]) for k, j in enumerate(turns)]
    for cp in loads + dy_in[:2]:
        cp.start()
    rs = 2 * NRS
    ex.rs_begin([part], scratch)
    ey.rs_begin([ypart], scratch[NRS:])
    width = part.shape[1]

    def attn_part(j):
        part[ex.chip[j], :] = tn(o_ref[:, ex.chip[j]], wo[...]).astype(BF16)

    ex.reduce_scatter([acc], attn_part)
    h = (e_ref[...].astype(F32) + acc[...].astype(BF16).astype(F32)).astype(BF16)
    h_ref[...] = h
    z[ex.mine[0], :] = norm_rows(h.astype(F32), gain[...]).astype(BF16)
    save_z, save_d = ex.saver(z, z_out, zsem), ex.saver(dfull, dfull_out, fsem)
    save_a = [[pltpu.make_async_copy(act.at[t % 2, k], dst.at[ex.chip[j], :], asem.at[t % 2, k]) for k, dst in enumerate((hid_out, dgate_out, dup_out))]
              for t, j in enumerate(turns)]

    def mlp(j, t):
        rows = ex.chip[j]
        gate, up = nt(z[rows, :], wg[...]), nt(z[rows, :], wu[...])
        sig = jax.nn.sigmoid(gate)
        hid = (gate * sig * up).astype(BF16)
        dh = nt(dyb[t % 2], wd[...])
        dup = (dh * gate * sig).astype(BF16)
        dgate = (dh * up * sig * (1.0 + gate * (1.0 - sig))).astype(BF16)
        if t > 1:
            for cp in save_a[t - 2]:
                cp.wait()
        for k, value in enumerate((hid, dgate, dup)):
            act[t % 2, k] = value
        for c in range(0, width, COLS):
            cols = slice(c, c + COLS)
            part[rows, cols] = (nn(dgate, wg[:, cols]) + nn(dup, wu[:, cols])).astype(BF16)
            ypart[rows, cols] = nn(hid, wd[:, cols]).astype(BF16)
        for cp in save_a[t]:
            cp.start()

    def arrive_z(j):
        if j == 0:
            ex.drain()
            for cp in loads:
                cp.wait()
        save_z[j].start()
        for e in (ex, ey):
            if j == 3:
                e.push(1)
            if j == 2:
                e.push(3)
        k = turns.index(j)
        dy_in[k].wait()
        mlp(j, k)
        if k < 2:
            dy_in[k + 2].start()
        for e in (ex, ey):
            e.ready(j)

    ex.all_gather([z], scratch[rs:rs + NAG], arrive_z, blocks=turns[1:])
    for e in (ex, ey):
        e.relay((1,))
        e.push(2)
        e.relay((0,))
    ex.land([acc])
    dx, dgain_ref[...] = norm_rows_vjp(h_ref[...].astype(F32), gain[...], acc[...])
    dres = dyl_ref[...].astype(F32) + dx
    dres_ref[...] = dres
    dfull[ex.mine[0], :] = dres.astype(BF16)

    def arrive_d(j):
        do_ref[:, ex.chip[j]] = nt(wo[...], dfull[ex.chip[j], :]).astype(BF16)
        save_d[j].start()
        if j == 2:
            ey.land([acc])
            y_ref[...] = (h_ref[...].astype(F32) + acc[...].astype(BF16).astype(F32)).astype(BF16)

    ex.all_gather([dfull], scratch[rs + NAG:], arrive_d)
    ex.drain()
    ey.drain()
    for cp in save_z + save_d + save_a[2] + save_a[3]:
        cp.wait()


def attn_back_body(dq_ref, lat, wq, wdkv, e_ref, dres_ref, gain, de_ref, dg_ref, part, acc, acc_lat, *scratch):
    ex = Exchange([part.shape[1], lat.shape[1]], LAST)
    ex.place(acc.shape[0])
    ex.enter()
    ex.rs_begin([part, lat], scratch)
    lw = wdkv.shape[0]

    def produce(j):
        rows = ex.chip[j]
        part[rows, :] = (tn(dq_ref[:, rows], wq[...]) + nn(lat[rows, :lw], wdkv[...])).astype(BF16)

    ex.reduce_scatter([acc, acc_lat], produce)
    dx, dg_ref[...] = norm_rows_vjp(e_ref[...].astype(F32), gain[...], acc[...])
    de_ref[:, :dx.shape[1]] = (dres_ref[...] + dx).astype(BF16)
    de_ref[:, dx.shape[1]:] = acc_lat[...].astype(BF16)
    ex.drain()


def layer_pass(rows, d_out, w_q, w_dkv, g_kv, w_uk, w_uv, w_o, g_attn, g_mlp, w_gate, w_up, w_down, vocab, key, blocks, count):
    w_q, heads = w_q
    seq, width = rows.shape
    local = d_out.shape[0]
    lora = g_kv.shape[0]
    latw = w_dkv.shape[0]
    one = Exchange([width], MAIN)
    main = [VM((local, width), F32)] + one.rs_scratch(local) + one.ag_scratch()
    partb = [VM((seq, width), BF16)]
    dma = pltpu.SemaphoreType.DMA
    saved = partb + [dma((4,))]
    loc, fullb = shape((local, width), BF16), shape((seq, width), BF16)
    ga, gm = g_attn[None, :], g_mlp[None, :]
    rows, dy_near = lax.optimization_barrier((rows, [shift(d_out, XBIT), shift(d_out, YBIT)]))
    embedded, query, latent, x_attn = exchange_call(
        embed_body, 'embed_exchange', 1, [rows, ga, w_q, w_dkv], [loc, shape((w_q.shape[0], seq), BF16), shape((seq, latw), F32), fullb], saved + main, out=1)
    cos_t, sin_t = (t.T for t in rope_tables(seq, latw - lora))
    nq, nk, nv = w_q.shape[0], w_uk.shape[0], w_uv.shape[0]
    c_kv, k_nope, k_pe_t, value, attn_out, lse, dy_full = exchange_call(
        attn_body, 'attend_fwd', 2, [latent, g_kv[None, :], w_uk, w_uv, query, cos_t, sin_t, d_out, *dy_near],
        [shape((seq, lora), BF16), shape((nk, seq), BF16), shape((latw - lora, seq), BF16), shape((nv, seq), BF16), shape((nv, seq), BF16),
         shape((heads, 1, seq), F32), fullb], saved + one.ag_scratch(), out=1, limit=ALL)
    kv_pull = jax.vjp(kv_prep, latent, g_kv)[1]
    ffn = w_gate.shape[0]
    act = shape((seq, ffn), BF16)
    residual, layer_out, d_residual, dg_mlp, d_attn_out, x_mlp, hidden, d_gate, d_up, d_attn_full = exchange_call(
        middle_body, 'middle', 3, [attn_out, w_o, embedded, gm, d_out, dy_full, w_gate, w_up, w_down],
        [loc, loc, shape((local, width), F32), shape((1, width), F32), shape((w_o.shape[0], seq), BF16), fullb, act, act, act, fullb],
        [VM((3 * ffn, width), BF16), VM((2, seq // 4, width), BF16), VM((2, 3, seq // 4, ffn), BF16)] + partb * 3
        + [VM((local, width), F32), dma((3,)), dma((2,)), dma((2, 3)), dma((4,)), dma((4,))]
        + one.rs_scratch(local) * 2 + one.ag_scratch() * 2, far=4, out=5, limit=ALL)
    d_query, d_knope, d_value, d_kpe, table0 = attend_bwd(query, k_nope, k_pe_t, value, cos_t, sin_t, lse, d_attn_out, heads, (vocab, width))
    d_ckv = (tn(d_knope, w_uk) + tn(d_value, w_uv)).astype(BF16)
    d_latent, dg_kv = kv_pull((d_ckv, d_kpe.T.astype(BF16)))
    lat_part = jnp.pad(d_latent.astype(BF16), ((0, 0), (0, -latw % 128)))
    padw = lat_part.shape[1]
    two = Exchange([width, padw], LAST)
    de, dg_attn = exchange_call(
        attn_back_body, 'back_exchange', 4, [d_query, lat_part, w_q, w_dkv, embedded, d_residual, ga],
        [shape((local, width + padw), BF16), shape((1, width), F32)],
        partb + [VM((local, width), F32), VM((local, padw), F32)] + two.rs_scratch(local))
    later = lax.optimization_barrier
    dg = jnp.concatenate([dg_attn[0], dg_mlp[0], dg_kv])
    hidden, d_gate, d_up, d_query, de, dg = later((hidden, d_gate, d_up, d_query, de, dg))
    near = [shift(de, XBIT), shift(de, YBIT), shift(de, XBIT + YBIT)]
    pair = shift(de, PAIR)
    dg = dg + shift(dg, PAIR)
    dw_down, dw_gate, dw_up, dw_q = tn(hidden, dy_full), tn(d_gate, x_mlp), tn(d_up, x_mlp), nn(d_query, x_attn)
    dw_down, dw_gate, dw_up, dw_q, near, pair, dg, attn_out = later((dw_down, dw_gate, dw_up, dw_q, near, pair, dg, attn_out))
    far = [shift(b, PAIR) for b in near]
    dg = dg + shift(dg, XBIT)
    dw_o = nn(attn_out, d_attn_full)
    dw_o, far, dg, d_knope, d_value = later((dw_o, far, dg, d_knope, d_value))
    dg = dg + shift(dg, YBIT)
    dw_uk, dw_uv = nn(d_knope, c_kv), nn(d_value, c_kv)
    d_table, lat_full = table_grad(to_hop_order(key, 0), blocks, count, [de, *near, pair, *far], table0)
    dw_dkv = tn(lat_full[:, :latw], x_attn)
    dg_attn, dg_mlp, dg_kv = dg[:width], dg[width:2 * width], dg[2 * width:]
    return layer_out, d_table, (dw_q, dw_dkv, dg_kv, dw_uk, dw_uv, dw_o, dg_attn, dg_mlp, dw_gate, dw_up, dw_down)


def rows_of(w):
    return jnp.transpose(w, (1, 2, 0)).reshape(-1, w.shape[0])


def unrows(g, heads):
    return jnp.transpose(g.reshape(heads, -1, g.shape[1]), (2, 0, 1))


def solution(mesh):
    def device_step(tokens, embed_table, w_q, w_dkv, g_kv, w_uk, w_uv, w_o, g_attn, g_mlp, w_gate, w_up, w_down, d_out):
        vocab_local, model_dim = embed_table.shape
        heads = w_q.shape[1]
        key, blocks, count = block_index(tokens, vocab_local)
        rows = gather_rows(key, blocks, count, embed_table)
        layer_out, d_table, grads = layer_pass(
            rows, d_out[0], (rows_of(w_q), heads), w_dkv.T, g_kv, rows_of(w_uk), rows_of(w_uv), w_o.reshape(-1, model_dim),
            g_attn, g_mlp, w_gate.T, w_up.T, w_down, vocab_local, key, blocks, count)
        dw_q, dw_dkv, dg_kv, dw_uk, dw_uv, dw_o, dg_attn, dg_mlp, dw_gate, dw_up, dw_down = grads
        return (layer_out[None], d_table, unrows(dw_q, heads), dw_dkv.T, dg_kv, unrows(dw_uk, heads), unrows(dw_uv, heads),
                dw_o.reshape(w_o.shape), dg_attn, dg_mlp, dw_gate.T, dw_up.T, dw_down)

    row_spec = P('dp', 'tp', None)
    head_spec = P(None, 'tp', None)
    in_specs = (P('dp', None), P('tp', None), head_spec, P(None, None), P(None), head_spec, head_spec, P('tp', None, None), P(None), P(None), P(None, 'tp'), P(None, 'tp'), P('tp', None), row_spec)
    out_specs = (row_spec, P(('dp', 'tp'), None), P('dp', 'tp', None), P('dp', None), P('dp'), P('dp', 'tp', None), P('dp', 'tp', None), P(('dp', 'tp'), None, None), P('dp'), P('dp'), P('dp', 'tp'), P('dp', 'tp'), P(('dp', 'tp'), None))
    return jax.shard_map(device_step, mesh=mesh, in_specs=in_specs, out_specs=out_specs, check_vma=False)
```

```python
import functools

import jax
import jax.numpy as jnp
from jax import lax
from jax.experimental import pallas as pl
from jax.experimental.pallas import tpu as pltpu
from jax.sharding import PartitionSpec as P

EPSILON = 1e-6
ROPE_BASE = 10000.0
F32, BF16 = jnp.float32, jnp.bfloat16
LOG2E = 1.4426950408889634
VM = pltpu.VMEM
ZR = 248
GB = 64
GR = GB * 8
LIMIT = 40 << 20
ALL = 63
QB = 256


def mm(lhs, rhs, lc, rc):
    return lax.dot_general(lhs, rhs, (((lc,), (rc,)), ((), ())), preferred_element_type=F32)


def nn(a, b):
    return mm(a, b, 1, 0)


def nt(a, b):
    return mm(a, b, 1, 1)


def tn(a, b):
    return mm(a, b, 0, 0)


mean_last = functools.partial(jnp.mean, axis=-1, keepdims=True)
sum_rows = functools.partial(jnp.sum, axis=0, keepdims=True)


def rope_tables(seq_len, rope_dim):
    inv_freq = ROPE_BASE ** (-jnp.arange(0, rope_dim, 2, dtype=F32) / rope_dim)
    angles = jnp.arange(seq_len, dtype=F32)[:, None] * inv_freq[None, :]
    return jnp.cos(angles), jnp.sin(angles)


def apply_rope(x_in, cos_t, sin_t):
    half_dim = x_in.shape[-1] // 2
    x_lo, x_hi = x_in[..., :half_dim], x_in[..., half_dim:]
    return jnp.concatenate([x_lo * cos_t - x_hi * sin_t, x_hi * cos_t + x_lo * sin_t], axis=-1)


def rms_norm(x_in, gain):
    inv_rms = lax.rsqrt(mean_last(x_in * x_in) + EPSILON)
    return (x_in * inv_rms * gain).astype(BF16)


def kv_prep(latent, g_kv):
    lora = g_kv.shape[0]
    cos_t, sin_t = rope_tables(latent.shape[0], latent.shape[-1] - lora)
    k_pe = apply_rope(latent[:, lora:], cos_t, sin_t).astype(BF16)
    return rms_norm(latent[:, :lora], g_kv), k_pe


def block_index(tokens, vocab_local):
    ids = tokens.reshape(-1) - lax.axis_index('tp') * vocab_local
    n = ids.shape[0]
    owned = (ids >= 0) & (ids < vocab_local)
    blk = jnp.where(owned, ids >> 3, -1)
    pos = jnp.arange(n, dtype=jnp.int32)
    eq = (blk[:, None] == blk[None, :])
    first = jnp.min(jnp.where(eq, pos[None, :], n), axis=1)
    isf = owned & (first == pos)
    slot = jnp.sum((isf[None, :] & (pos[None, :] < first[:, None])).astype(jnp.int32), axis=1)
    key = jnp.where(owned, slot * 8 + (ids & 7), -1)
    blocks = jnp.sum(jnp.where(isf[None, :] & (slot[None, :] == pos[:, None]), blk[None, :], 0), axis=1)
    count = jnp.sum(isf.astype(jnp.int32)).reshape(1)
    return key, blocks, count


def gather_body(count_ref, blocks_ref, key_ref, tail_ref, table_ref, out_ref, stage, sem):
    rows, width = out_ref.shape
    full = table_ref.shape[0] // 8
    stage[...] = jnp.zeros_like(stage)
    out_ref[...] = jnp.zeros_like(out_ref)
    count = count_ref[0]

    def fetch(b, i):
        return pltpu.make_async_copy(table_ref.at[pl.ds(pl.multiple_of(b * 8, 8), 8), :], stage.at[i], sem)

    def chunk(ci, carry):
        base = ci * GB
        n = jnp.minimum(GB, count - base)

        def start(i, c):
            b = blocks_ref[base + i]

            @pl.when(b < full)
            def _():
                fetch(b, i).start()

            @pl.when(b >= full)
            def _():
                stage[i] = tail_ref[...]
            return c

        def wait(i, c):
            b = blocks_ref[base + i]

            @pl.when(b < full)
            def _():
                fetch(b, i).wait()
            return c

        lax.fori_loop(0, n, start, 0)
        lax.fori_loop(0, n, wait, 0)
        cols = lax.broadcasted_iota(jnp.int32, (rows, GR), 1) + base * 8
        hot = jnp.where(cols == key_ref[...], 1.0, 0.0).astype(BF16)
        for c in range(0, width, COLS):
            got = nn(hot, stage[:, :, c:c + COLS].reshape(GR, COLS))
            out_ref[:, c:c + COLS] += got.astype(BF16)
        return carry

    lax.fori_loop(0, (count + GB - 1) // GB, chunk, 0)


def gather_rows(key, blocks, count, table):
    rows, (vocab, width) = key.shape[0], table.shape
    full = vocab // 8 * 8
    tail = jnp.pad(table[full:], ((0, 8 - (vocab - full)), (0, 0)))
    smem = pl.BlockSpec(memory_space=pltpu.SMEM)
    return pl.pallas_call(
        gather_body, out_shape=jax.ShapeDtypeStruct((rows, width), BF16),
        in_specs=[smem, smem, pl.BlockSpec(memory_space=VM), pl.BlockSpec(memory_space=VM), pl.BlockSpec(memory_space=pl.ANY)],
        out_specs=pl.BlockSpec(memory_space=VM),
        scratch_shapes=[VM((GB, 8, width), BF16), pltpu.SemaphoreType.DMA],
        compiler_params=pltpu.CompilerParams(vmem_limit_bytes=LIMIT), name='gather_rows',
    )(count, blocks, key[:, None], tail, table)


def table_grad_body(count_ref, blocks_ref, key_ref, zeros_ref, *refs):
    pieces, (out_ref, tail_ref, lat_ref, de_ref, stage, sem) = refs[:-6], refs[-6:]
    rows, width = de_ref.shape
    local = rows // len(pieces)
    for k, (piece, d) in enumerate(zip(pieces, hop_order())):
        de_ref[k * local:(k + 1) * local, :] = piece[:, :width]
        lat_ref[pl.ds(pl.multiple_of(d * local, local), local), :] = piece[:, width:]
    full = out_ref.shape[0] // 8
    tail_ref[...] = jnp.zeros_like(tail_ref)
    count = count_ref[0]

    def put(b, i):
        return pltpu.make_async_copy(stage.at[i], out_ref.at[pl.ds(pl.multiple_of(b * 8, 8), 8), :], sem)

    def sums(ci):
        ids = lax.broadcasted_iota(jnp.int32, (GR, rows), 0) + ci * GR
        hot = jnp.where(ids == key_ref[...], 1.0, 0.0).astype(BF16)
        for c in range(0, width, COLS):
            got = nn(hot, de_ref[:, c:c + COLS])
            stage[:, :, c:c + COLS] = got.astype(BF16).reshape(GB, 8, COLS)

    def move(ci, go):
        base = ci * GB

        def one(i, c):
            b = blocks_ref[base + i]

            @pl.when(b < full)
            def _():
                go(put(b, i))
            @pl.when(b >= full)
            def _():
                tail_ref[...] = stage[i]
            return c

        lax.fori_loop(0, jnp.minimum(GB, count - base), one, 0)

    def chunk(ci, carry):
        sums(ci)
        move(ci, lambda cp: cp.start())
        move(ci, lambda cp: cp.wait())
        return carry

    lax.fori_loop(0, (count + GB - 1) // GB, chunk, 0)


def table_grad(key, blocks, count, pieces, table):
    (vocab, width), rows = table.shape, key.shape[0]
    latw = pieces[0].shape[1] - width
    smem, vmem, anym = (pl.BlockSpec(memory_space=m) for m in (pltpu.SMEM, VM, pl.ANY))
    full = vocab // 8 * 8
    out, tail, lat = pl.pallas_call(
        table_grad_body, out_shape=[shape((vocab, width), BF16), shape((8, width), BF16), shape((rows, latw), BF16)],
        in_specs=[smem, smem, vmem, anym] + [vmem] * len(pieces), input_output_aliases={3: 0},
        out_specs=[anym, vmem, vmem],
        scratch_shapes=[VM((rows, width), BF16), VM((GB, 8, width), BF16), pltpu.SemaphoreType.DMA],
        compiler_params=pltpu.CompilerParams(vmem_limit_bytes=LIMIT), name='table_grad',
    )(count, blocks, key[None, :], table, *pieces)
    return lax.dynamic_update_slice(out, tail[:vocab - full], (full, 0)), lat


def heads_of(q_ref, kn_ref, kp_ref, cos_ref, sin_ref, nope, half):
    q_pe = q_ref[nope:, :].astype(F32)
    lo, hi, cos_t, sin_t = q_pe[:half], q_pe[half:], cos_ref[...], sin_ref[...]
    q_all = jnp.concatenate([q_ref[:nope, :], (lo * cos_t - hi * sin_t).astype(BF16), (hi * cos_t + lo * sin_t).astype(BF16)], axis=0)
    return q_all, jnp.concatenate([kn_ref[...], kp_ref[...]], axis=0)


def scores_of(k_all, q_all, ki, qi, scale):
    s = tn(k_all[:, ki * QB:(ki + 1) * QB], q_all[:, qi * QB:(qi + 1) * QB]) * scale
    if ki == qi:
        keys = lax.broadcasted_iota(jnp.int32, (QB, QB), 0)
        s = jnp.where(keys <= lax.broadcasted_iota(jnp.int32, (QB, QB), 1), s, -1e30)
    return s


def attn_fwd_body(q_ref, kn_ref, kp_ref, v_ref, cos_ref, sin_ref, o_ref, lse_ref):
    nope, half = kn_ref.shape[0], cos_ref.shape[0]
    scale = q_ref.shape[0] ** -0.5 * LOG2E
    q_all, k_all = heads_of(q_ref, kn_ref, kp_ref, cos_ref, sin_ref, nope, half)
    for qi in range(q_ref.shape[1] // QB):
        lanes = slice(qi * QB, (qi + 1) * QB)
        s = [scores_of(k_all, q_all, ki, qi, scale) for ki in range(qi + 1)]
        top = functools.reduce(jnp.maximum, [jnp.max(x, axis=0, keepdims=True) for x in s])
        p = [jnp.exp2(x - top) for x in s]
        total = sum(sum_rows(x) for x in p)
        inv = 1.0 / total
        o = sum(nn(v_ref[:, ki * QB:(ki + 1) * QB], (x * inv).astype(BF16)) for ki, x in enumerate(p))
        o_ref[:, lanes] = o.astype(BF16)
        lse_ref[0, :, lanes] = top + jnp.log2(total)


def attn_bwd_body(heads, q_ref, kn_ref, kp_ref, v_ref, cos_ref, sin_ref, lse_ref, do_ref, dq_ref, dkn_ref, dv_ref, dkp_ref, table_ref, dk_acc, dv_acc, zero, zsem):
    full = table_ref.shape[0] // 8 * 8
    fills = [pltpu.make_async_copy(zero.at[pl.ds(0, n), :], table_ref.at[pl.ds(r, n), :], zsem.at[k])
             for k, (r, n) in enumerate((r, min(ZR, full - r)) for r in range(0, full, ZR))]

    head = pl.program_id(0)
    share = -(-len(fills) // heads)

    @pl.when(head == 0)
    def _():
        zero[...] = jnp.zeros_like(zero)
    for h in range(heads):
        @pl.when(head == h)
        def _():
            for cp in fills[h * share:(h + 1) * share]:
                cp.start()

    nope, half = kn_ref.shape[0], cos_ref.shape[0]
    raw = q_ref.shape[0] ** -0.5
    q_all, k_all = heads_of(q_ref, kn_ref, kp_ref, cos_ref, sin_ref, nope, half)
    dk_acc[...] = jnp.zeros_like(dk_acc)
    dv_acc[...] = jnp.zeros_like(dv_acc)
    for qi in range(q_ref.shape[1] // QB):
        lanes = slice(qi * QB, (qi + 1) * QB)
        q_b, do_b, lse = q_all[:, lanes], do_ref[:, lanes], lse_ref[0, :, lanes]
        p = [jnp.exp2(scores_of(k_all, q_all, ki, qi, raw * LOG2E) - lse) for ki in range(qi + 1)]
        dp = [tn(v_ref[:, ki * QB:(ki + 1) * QB], do_b) for ki in range(qi + 1)]
        delta = sum(sum_rows(a * b) for a, b in zip(p, dp))
        dq = None
        for ki in range(qi + 1):
            keys = slice(ki * QB, (ki + 1) * QB)
            ds = (p[ki] * (dp[ki] - delta) * raw).astype(BF16)
            part = nn(k_all[:, keys], ds)
            dq = part if dq is None else dq + part
            dk_acc[:, keys] += nt(q_b, ds)
            dv_acc[:, keys] += nt(do_b, p[ki].astype(BF16))
        cos_t, sin_t = cos_ref[:, lanes], sin_ref[:, lanes]
        lo, hi = dq[nope:nope + half], dq[nope + half:]
        dq_ref[:nope, lanes] = dq[:nope].astype(BF16)
        dq_ref[nope:nope + half, lanes] = (lo * cos_t + hi * sin_t).astype(BF16)
        dq_ref[nope + half:, lanes] = (hi * cos_t - lo * sin_t).astype(BF16)
    dkn_ref[...] = dk_acc[:nope, :].astype(BF16)
    dv_ref[...] = dv_acc[...].astype(BF16)

    @pl.when(head == 0)
    def _():
        dkp_ref[...] = jnp.zeros_like(dkp_ref)
    dkp_ref[...] += dk_acc[nope:, :]

    @pl.when(head == heads - 1)
    def _():
        for cp in fills:
            cp.wait()


def attn_specs(heads, qd, nope, rope, vd, seq):
    per = lambda r: pl.BlockSpec((r, seq), lambda h: (h, 0))
    one = lambda r: pl.BlockSpec((r, seq), lambda h: (0, 0))
    return [per(qd), per(nope), one(rope), per(vd), one(rope // 2), one(rope // 2)], per, one, pl.BlockSpec((1, 1, seq), lambda h: (h, 0, 0))


def attend_bwd(q, kn, kp, v, cos_t, sin_t, lse, do, heads, table):
    seq, qd, nope, vd, rope = q.shape[1], q.shape[0] // heads, kn.shape[0] // heads, v.shape[0] // heads, kp.shape[0]
    ins, per, one, lse_spec = attn_specs(heads, qd, nope, rope, vd, seq)
    return pl.pallas_call(
        functools.partial(attn_bwd_body, heads), grid=(heads,), in_specs=ins + [lse_spec, per(vd)], out_specs=[per(qd), per(nope), per(vd), one(rope), pl.BlockSpec(memory_space=pl.ANY)],
        out_shape=[jax.ShapeDtypeStruct(q.shape, BF16), jax.ShapeDtypeStruct(kn.shape, BF16), jax.ShapeDtypeStruct(v.shape, BF16), jax.ShapeDtypeStruct(kp.shape, F32), jax.ShapeDtypeStruct(table, BF16)],
        scratch_shapes=[VM((qd, seq), F32), VM((vd, seq), F32), VM((ZR, table[1]), BF16), pltpu.SemaphoreType.DMA((-(-table[0] // ZR),))],
        compiler_params=pltpu.CompilerParams(vmem_limit_bytes=ALL << 20), name='attend_bwd',
    )(q, kn, kp, v, cos_t, sin_t, lse, do)


def shift(x, bit):
    return lax.ppermute(x, 'tp', [(d, d ^ bit) for d in range(8)])


PAIR, XBIT, YBIT = 1, 2, 4


def hop_order():
    me = lax.axis_index('tp')
    flip = lambda v, bit: v + bit - 2 * bit * ((v // bit) % 2)
    own = [me, flip(me, XBIT), flip(me, YBIT), flip(flip(me, XBIT), YBIT)]
    return own + [flip(d, PAIR) for d in own]


def to_hop_order(x, axis):
    n = x.shape[axis] // 8
    return jnp.concatenate([lax.dynamic_slice_in_dim(x, d * n, n, axis) for d in hop_order()], axis=axis)


class Exchange:
    def __init__(self, widths, pieces):
        self.widths, self.pieces = widths, pieces
        self.order = range(len(pieces))

    def rs_scratch(self, rows):
        n = len(self.pieces)
        out = []
        for w in self.widths:
            out += [VM((4, rows, w), BF16), VM((2, rows, w), BF16), VM((2, rows, w), BF16), VM((rows, w), BF16), VM((rows, w), BF16)]
        dma = pltpu.SemaphoreType.DMA
        return out + [dma((4, n)), dma((4, n)), dma((2, n)), dma((2, n)), dma((n,)), dma((n,))]

    def ag_scratch(self):
        n = len(self.pieces)
        dma = pltpu.SemaphoreType.DMA
        return [dma((2, n)), dma((2, n)), dma((n,)), dma((n,)), dma((4, n)), dma((4, n))]

    def place(self, rows):
        me = lax.axis_index('tp')
        core, x, y = me % 2, (me // 2) % 2, me // 4
        dev = lambda yy, xx, cc: (yy * 2 + xx) * 2 + cc
        self.me, self.rows = me, rows
        self.pn, self.xn, self.yn = dev(y, x, 1 - core), dev(y, 1 - x, core), dev(1 - y, x, core)
        chips = [(y, x), (y, 1 - x), (1 - y, x), (1 - y, 1 - x)]
        at = lambda d: pl.ds(pl.multiple_of(d * rows, rows), rows)
        self.mine = [at(dev(*ch, core)) for ch in chips]
        self.theirs = [at(dev(*ch, 1 - core)) for ch in chips]
        self.chip = [pl.ds(pl.multiple_of(dev(*ch, 0) * rows, 2 * rows), 2 * rows) for ch in chips]

    def enter(self):
        sem = pltpu.get_barrier_semaphore()
        near = (self.pn, self.xn, self.yn)
        for d in near:
            pl.semaphore_signal(sem, inc=1, device_id={'tp': d}, device_id_type=pl.DeviceIdType.MESH)
        pl.semaphore_wait(sem, len(near))

    def copy(self, src, dst, ssem, rsem, dev):
        return pltpu.make_async_remote_copy(src_ref=src, dst_ref=dst, send_sem=ssem, recv_sem=rsem, device_id={'tp': dev}, device_id_type=pl.DeviceIdType.MESH)

    def saver(self, src, dst, sem):
        return [pltpu.make_async_copy(src.at[rows, :], dst.at[rows, :], sem.at[j]) for j, rows in enumerate(self.chip)]

    def rs_begin(self, parts, scratch):
        na = len(self.widths)
        self.parts = parts
        self.bufs = [scratch[5 * a:5 * a + 5] for a in range(na)]
        ds, dr, s1, r1, s2, r2 = scratch[5 * na:5 * na + 6]
        self.pair, self.hop1, self.hop2 = {}, {}, {}
        for i, (h, a, c0, cn) in enumerate(self.pieces):
            cols = pl.ds(c0, cn)
            dbuf, sb1, rb1, sb2, rb2 = self.bufs[a]
            for j in range(4):
                self.pair[j, i] = self.copy(parts[a].at[self.theirs[j], cols], dbuf.at[j, :, cols], ds.at[j, i], dr.at[j, i], self.pn)
            to1, to2 = (self.xn, self.yn) if h == 0 else (self.yn, self.xn)
            for k in range(2):
                self.hop1[k, i] = self.copy(sb1.at[k, :, cols], rb1.at[k, :, cols], s1.at[k, i], r1.at[k, i], to1)
            self.hop2[i] = self.copy(sb2.at[:, cols], rb2.at[:, cols], s2.at[i], r2.at[i], to2)

    def ready(self, j):
        for i in self.order:
            self.pair[j, i].start()

    def chip_sum(self, j, i):
        h, a, c0, cn = self.pieces[i]
        self.pair[j, i].wait_recv()
        return self.parts[a][self.mine[j], c0:c0 + cn].astype(F32) + self.bufs[a][0][j, :, c0:c0 + cn].astype(F32)

    def push(self, j):
        for i in self.order:
            h, a, c0, cn = self.pieces[i]
            if j == 3 or j == 1 + h:
                k = 1 if j == 3 else 0
                self.bufs[a][1][k, :, c0:c0 + cn] = self.chip_sum(j, i).astype(BF16)
                self.hop1[k, i].start()

    def relay(self, halves=(0, 1)):
        for i in self.order:
            h, a, c0, cn = self.pieces[i]
            if h not in halves:
                continue
            own = self.chip_sum(2 - h, i)
            self.hop1[1, i].wait_recv()
            self.bufs[a][3][:, c0:c0 + cn] = (own + self.bufs[a][2][1, :, c0:c0 + cn].astype(F32)).astype(BF16)
            self.hop2[i].start()

    def land(self, accs):
        for i in self.order:
            h, a, c0, cn = self.pieces[i]
            own = self.chip_sum(0, i)
            self.hop1[0, i].wait_recv()
            own = own + self.bufs[a][2][0, :, c0:c0 + cn].astype(F32)
            self.hop2[i].wait_recv()
            accs[a][:, c0:c0 + cn] = own + self.bufs[a][4][:, c0:c0 + cn].astype(F32)

    def drain(self):
        for cp in list(self.pair.values()) + list(self.hop1.values()) + list(self.hop2.values()):
            cp.wait_send()

    def reduce_scatter(self, accs, produce):
        late = None
        for j in (3, 1, 2, 0):
            produce(j)
            self.ready(j)
            if late:
                self.push(late)
            late = j
        self.relay()
        self.land(accs)

    def all_gather(self, fulls, scratch, arrive, blocks=(1, 2, 3), known=False):
        os_, xr, fs, fr, ps, pr = scratch
        half0 = [i for i in self.order if self.pieces[i][0] == 0]
        half1 = [i for i in self.order if self.pieces[i][0] == 1]

        def to(i, j, ssem, rsem, dev, rows=None):
            h, a, c0, cn = self.pieces[i]
            ref = fulls[a].at[(rows or self.mine)[j], pl.ds(c0, cn)]
            return self.copy(ref, ref, ssem, rsem, dev)

        near = (self.xn, self.yn)
        own = [[to(i, 0, os_.at[k, i], xr.at[k, i], dev) for i in self.order] for k, dev in enumerate(near)]
        from_n = [[to(i, 1 + k, os_.at[k, i], xr.at[k, i], dev) for i in self.order] for k, dev in enumerate(near)]
        fwd = [to(i, 2 - self.pieces[i][0], fs.at[i], fr.at[i], near[self.pieces[i][0]]) for i in self.order]
        diag = [to(i, 3, fs.at[i], fr.at[i], self.xn) for i in self.order]
        give = [[to(i, j, ps.at[j, i], pr.at[j, i], self.pn) for i in self.order] for j in range(4)]
        take = [[to(i, j, ps.at[j, i], pr.at[j, i], self.pn, self.theirs) for i in self.order] for j in range(4)]
        pairs = list(zip(half0, half1))
        sent = fwd + [cp for g in give for cp in g]

        def start(copies):
            for cp in copies:
                cp.start()

        def landed(copies):
            for cp in copies:
                cp.wait_recv()

        if not known:
            sent += own[0] + own[1]
            for i0, i1 in pairs:
                start((own[0][i1], own[1][i0]))
            for i0, i1 in pairs:
                start((own[0][i0], own[1][i1]))
        start(give[0])
        if known:
            start(fwd + give[1] + give[2])
        landed(take[0])
        arrive(0)
        if not known:
            for i0, i1 in pairs:
                from_n[1][i0].wait_recv()
                start((fwd[i0], give[2][i0]))
                from_n[0][i1].wait_recv()
                start((fwd[i1], give[1][i1]))
            for i0, i1 in pairs:
                from_n[1][i1].wait_recv()
                give[2][i1].start()
                from_n[0][i0].wait_recv()
                give[1][i0].start()
        for j in blocks:
            if j == 3:
                for i in self.order:
                    diag[i].wait_recv()
                    give[3][i].start()
            landed(take[j])
            arrive(j)
        for cp in sent:
            cp.wait_send()


def halves(width, n):
    step = width // (2 * n)
    return [(h, 0, (h * n + k) * step, step) for k in range(n) for h in range(2)]


MAIN = halves(2560, 2)
LAST = MAIN + [(0, 1, 0, 256), (1, 1, 256, 128)]
NRS, NAG = 11, 6
COLS = 512


def norm_rows(x, gain):
    return x * lax.rsqrt(mean_last(x * x) + EPSILON) * gain


def norm_rows_vjp(x, gain, dy):
    r = lax.rsqrt(mean_last(x * x) + EPSILON)
    gd = dy * gain
    dot = mean_last(gd * x)
    return r * gd - x * (r * r * r * dot), sum_rows(dy * x * r)


def exchange_call(body, name, cid, ins, out_shape, scratch, far=0, out=0, limit=50):
    vmem, hbm = pl.BlockSpec(memory_space=VM), pl.BlockSpec(memory_space=pltpu.HBM)
    return pl.pallas_call(
        body, out_shape=out_shape, in_specs=[vmem] * (len(ins) - far) + [hbm] * far, out_specs=[vmem] * (len(out_shape) - out) + [hbm] * out, scratch_shapes=scratch,
        compiler_params=pltpu.CompilerParams(vmem_limit_bytes=limit << 20, collective_id=cid, has_side_effects=True), name=name)(*ins)


def shape(dims, dtype):
    return jax.ShapeDtypeStruct(dims, dtype)


def idle(j):
    pass


def embed_body(part, gain, wq, wdkv, e_ref, q_ref, lat_ref, u_out, full, usem, acc, *scratch):
    ex = Exchange([part.shape[1]], MAIN)
    ex.place(acc.shape[0])
    ex.enter()
    ex.rs_begin([part], scratch)
    ex.reduce_scatter([acc], idle)
    e = acc[...].astype(BF16)
    e_ref[...] = e
    full[ex.mine[0], :] = norm_rows(e.astype(F32), gain[...]).astype(BF16)

    def arrive(j):
        u = full[ex.chip[j], :]
        q_ref[:, ex.chip[j]] = nt(wq[...], u).astype(BF16)
        lat_ref[ex.chip[j], :] = nt(u, wdkv[...])
        save[j].start()

    save = ex.saver(full, u_out, usem)
    ex.all_gather([full], scratch[NRS:], arrive)
    ex.drain()
    for cp in save:
        cp.wait()


def attn_body(lat, g_kv, wuk, wuv, q_ref, cos_ref, sin_ref, dy_ref, dyx_ref, dyy_ref, c_ref, kn_ref, kp_ref, v_ref, o_ref, lse_ref, dy_out, dyf, dsem, *scratch):
    ex = Exchange([dyf.shape[1]], MAIN)
    ex.place(dy_ref.shape[0])
    ex.enter()
    for rows, ref in zip(ex.mine, (dy_ref, dyx_ref, dyy_ref)):
        dyf[rows, :] = ref[...]
    lora, half, heads = c_ref.shape[1], cos_ref.shape[0], lse_ref.shape[0]
    per = lambda ref, h: ref.at[pl.ds(h * (ref.shape[0] // heads), ref.shape[0] // heads), :]

    save = ex.saver(dyf, dy_out, dsem)

    def arrive(j):
        save[j].start()
        if j:
            return
        c = norm_rows(lat[:, :lora], g_kv[...]).astype(BF16)
        c_ref[...] = c
        pe = lat[:, lora:].T
        lo, hi, cos_t, sin_t = pe[:half], pe[half:], cos_ref[...], sin_ref[...]
        kp_ref[...] = jnp.concatenate([lo * cos_t - hi * sin_t, hi * cos_t + lo * sin_t], axis=0).astype(BF16)
        kn_ref[...] = nt(wuk[...], c).astype(BF16)
        v_ref[...] = nt(wuv[...], c).astype(BF16)
        for h in range(heads):
            attn_fwd_body(per(q_ref, h), per(kn_ref, h), kp_ref, per(v_ref, h), cos_ref, sin_ref, per(o_ref, h), lse_ref.at[pl.ds(h, 1)])

    ex.all_gather([dyf], scratch, arrive, known=True)
    for cp in save:
        cp.wait()


def middle_body(o_ref, wo, e_ref, gain, dyl_ref, dy_hbm, wg_hbm, wu_hbm, wd_hbm,
                h_ref, y_ref, dres_ref, dgain_ref, do_ref, z_out, hid_out, dgate_out, dup_out, dfull_out,
                wall, dyb, act, part, ypart, z, acc, wsem, dsem, asem, zsem, fsem, *scratch):
    ex, ey = Exchange([part.shape[1]], MAIN), Exchange([part.shape[1]], MAIN)
    for e in (ex, ey):
        e.place(acc.shape[0])
    ex.enter()
    ffn = wd_hbm.shape[0]
    wg, wu, wd = (wall.at[pl.ds(k * ffn, ffn), :] for k in range(3))
    dfull = wall.at[pl.ds(0, part.shape[0]), :]
    loads = [pltpu.make_async_copy(a, b, wsem.at[k]) for k, (a, b) in enumerate(((wg_hbm, wg), (wu_hbm, wu), (wd_hbm, wd)))]
    turns = (0, 1, 3, 2)
    dy_in = [pltpu.make_async_copy(dy_hbm.at[ex.chip[j], :], dyb.at[k % 2], dsem.at[k % 2]) for k, j in enumerate(turns)]
    for cp in loads + dy_in[:2]:
        cp.start()
    rs = 2 * NRS
    ex.rs_begin([part], scratch)
    ey.rs_begin([ypart], scratch[NRS:])
    width = part.shape[1]

    def attn_part(j):
        part[ex.chip[j], :] = tn(o_ref[:, ex.chip[j]], wo[...]).astype(BF16)

    ex.reduce_scatter([acc], attn_part)
    h = (e_ref[...].astype(F32) + acc[...].astype(BF16).astype(F32)).astype(BF16)
    h_ref[...] = h
    z[ex.mine[0], :] = norm_rows(h.astype(F32), gain[...]).astype(BF16)
    save_z, save_d = ex.saver(z, z_out, zsem), ex.saver(dfull, dfull_out, fsem)
    save_a = [[pltpu.make_async_copy(act.at[t % 2, k], dst.at[ex.chip[j], :], asem.at[t % 2, k]) for k, dst in enumerate((hid_out, dgate_out, dup_out))]
              for t, j in enumerate(turns)]

    def mlp(j, t):
        rows = ex.chip[j]
        gate, up = nt(z[rows, :], wg[...]), nt(z[rows, :], wu[...])
        sig = jax.nn.sigmoid(gate)
        hid = (gate * sig * up).astype(BF16)
        dh = nt(dyb[t % 2], wd[...])
        dup = (dh * gate * sig).astype(BF16)
        dgate = (dh * up * sig * (1.0 + gate * (1.0 - sig))).astype(BF16)
        if t > 1:
            for cp in save_a[t - 2]:
                cp.wait()
        for k, value in enumerate((hid, dgate, dup)):
            act[t % 2, k] = value
        for c in range(0, width, COLS):
            cols = slice(c, c + COLS)
            part[rows, cols] = (nn(dgate, wg[:, cols]) + nn(dup, wu[:, cols])).astype(BF16)
            ypart[rows, cols] = nn(hid, wd[:, cols]).astype(BF16)
        for cp in save_a[t]:
            cp.start()

    def arrive_z(j):
        if j == 0:
            ex.drain()
            for cp in loads:
                cp.wait()
        save_z[j].start()
        for e in (ex, ey):
            if j == 3:
                e.push(1)
            if j == 2:
                e.push(3)
        k = turns.index(j)
        dy_in[k].wait()
        mlp(j, k)
        if k < 2:
            dy_in[k + 2].start()
        for e in (ex, ey):
            e.ready(j)

    ex.all_gather([z], scratch[rs:rs + NAG], arrive_z, blocks=turns[1:])
    for e in (ex, ey):
        e.relay((1,))
        e.push(2)
        e.relay((0,))
    ex.land([acc])
    dx, dgain_ref[...] = norm_rows_vjp(h_ref[...].astype(F32), gain[...], acc[...])
    dres = dyl_ref[...].astype(F32) + dx
    dres_ref[...] = dres
    dfull[ex.mine[0], :] = dres.astype(BF16)

    def arrive_d(j):
        do_ref[:, ex.chip[j]] = nt(wo[...], dfull[ex.chip[j], :]).astype(BF16)
        save_d[j].start()
        if j == 2:
            ey.land([acc])
            y_ref[...] = (h_ref[...].astype(F32) + acc[...].astype(BF16).astype(F32)).astype(BF16)

    ex.all_gather([dfull], scratch[rs + NAG:], arrive_d)
    ex.drain()
    ey.drain()
    for cp in save_z + save_d + save_a[2] + save_a[3]:
        cp.wait()


def attn_back_body(dq_ref, lat, wq, wdkv, e_ref, dres_ref, gain, de_ref, dg_ref, part, acc, acc_lat, *scratch):
    ex = Exchange([part.shape[1], lat.shape[1]], LAST)
    ex.place(acc.shape[0])
    ex.enter()
    ex.rs_begin([part, lat], scratch)
    lw = wdkv.shape[0]

    def produce(j):
        rows = ex.chip[j]
        part[rows, :] = (tn(dq_ref[:, rows], wq[...]) + nn(lat[rows, :lw], wdkv[...])).astype(BF16)

    ex.reduce_scatter([acc, acc_lat], produce)
    dx, dg_ref[...] = norm_rows_vjp(e_ref[...].astype(F32), gain[...], acc[...])
    de_ref[:, :dx.shape[1]] = (dres_ref[...] + dx).astype(BF16)
    de_ref[:, dx.shape[1]:] = acc_lat[...].astype(BF16)
    ex.drain()


def layer_pass(rows, d_out, w_q, w_dkv, g_kv, w_uk, w_uv, w_o, g_attn, g_mlp, w_gate, w_up, w_down, vocab, key, blocks, count):
    w_q, heads = w_q
    seq, width = rows.shape
    local = d_out.shape[0]
    lora = g_kv.shape[0]
    latw = w_dkv.shape[0]
    one = Exchange([width], MAIN)
    main = [VM((local, width), F32)] + one.rs_scratch(local) + one.ag_scratch()
    partb = [VM((seq, width), BF16)]
    dma = pltpu.SemaphoreType.DMA
    saved = partb + [dma((4,))]
    loc, fullb = shape((local, width), BF16), shape((seq, width), BF16)
    ga, gm = g_attn[None, :], g_mlp[None, :]
    rows, dy_near = lax.optimization_barrier((rows, [shift(d_out, XBIT), shift(d_out, YBIT)]))
    embedded, query, latent, x_attn = exchange_call(
        embed_body, 'embed_exchange', 1, [rows, ga, w_q, w_dkv], [loc, shape((w_q.shape[0], seq), BF16), shape((seq, latw), F32), fullb], saved + main, out=1, limit=36)
    cos_t, sin_t = (t.T for t in rope_tables(seq, latw - lora))
    nq, nk, nv = w_q.shape[0], w_uk.shape[0], w_uv.shape[0]
    c_kv, k_nope, k_pe_t, value, attn_out, lse, dy_full = exchange_call(
        attn_body, 'attend_fwd', 2, [latent, g_kv[None, :], w_uk, w_uv, query, cos_t, sin_t, d_out, *dy_near],
        [shape((seq, lora), BF16), shape((nk, seq), BF16), shape((latw - lora, seq), BF16), shape((nv, seq), BF16), shape((nv, seq), BF16),
         shape((heads, 1, seq), F32), fullb], saved + one.ag_scratch(), out=1, limit=ALL)
    kv_pull = jax.vjp(kv_prep, latent, g_kv)[1]
    ffn = w_gate.shape[0]
    act = shape((seq, ffn), BF16)
    residual, layer_out, d_residual, dg_mlp, d_attn_out, x_mlp, hidden, d_gate, d_up, d_attn_full = exchange_call(
        middle_body, 'middle', 3, [attn_out, w_o, embedded, gm, d_out, dy_full, w_gate, w_up, w_down],
        [loc, loc, shape((local, width), F32), shape((1, width), F32), shape((w_o.shape[0], seq), BF16), fullb, act, act, act, fullb],
        [VM((3 * ffn, width), BF16), VM((2, seq // 4, width), BF16), VM((2, 3, seq // 4, ffn), BF16)] + partb * 3
        + [VM((local, width), F32), dma((3,)), dma((2,)), dma((2, 3)), dma((4,)), dma((4,))]
        + one.rs_scratch(local) * 2 + one.ag_scratch() * 2, far=4, out=5, limit=ALL)
    d_query, d_knope, d_value, d_kpe, table0 = attend_bwd(query, k_nope, k_pe_t, value, cos_t, sin_t, lse, d_attn_out, heads, (vocab, width))
    d_ckv = (tn(d_knope, w_uk) + tn(d_value, w_uv)).astype(BF16)
    d_latent, dg_kv = kv_pull((d_ckv, d_kpe.T.astype(BF16)))
    lat_part = jnp.pad(d_latent.astype(BF16), ((0, 0), (0, -latw % 128)))
    padw = lat_part.shape[1]
    two = Exchange([width, padw], LAST)
    de, dg_attn = exchange_call(
        attn_back_body, 'back_exchange', 4, [d_query, lat_part, w_q, w_dkv, embedded, d_residual, ga],
        [shape((local, width + padw), BF16), shape((1, width), F32)],
        partb + [VM((local, width), F32), VM((local, padw), F32)] + two.rs_scratch(local))
    later = lax.optimization_barrier
    dg = jnp.concatenate([dg_attn[0], dg_mlp[0], dg_kv])
    hidden, d_gate, d_up, d_query, attn_out, de, dg = later((hidden, d_gate, d_up, d_query, attn_out, de, dg))
    near = [shift(de, XBIT), shift(de, YBIT), shift(de, XBIT + YBIT)]
    pair = shift(de, PAIR)
    dg = dg + shift(dg, PAIR)
    dw_down, dw_gate, dw_up, dw_q, dw_o = tn(hidden, dy_full), tn(d_gate, x_mlp), tn(d_up, x_mlp), nn(d_query, x_attn), nn(attn_out, d_attn_full)
    dw_down, dw_gate, dw_up, dw_q, dw_o, near, pair, dg, d_knope, d_value = later((dw_down, dw_gate, dw_up, dw_q, dw_o, near, pair, dg, d_knope, d_value))
    far = [shift(b, PAIR) for b in near]
    dg = dg + shift(dg, XBIT)
    dw_uk, dw_uv = nn(d_knope, c_kv), nn(d_value, c_kv)
    dw_uk, dw_uv, far, dg = later((dw_uk, dw_uv, far, dg))
    dg = dg + shift(dg, YBIT)
    d_table, lat_full = table_grad(to_hop_order(key, 0), blocks, count, [de, *near, pair, *far], table0)
    dw_dkv = tn(lat_full[:, :latw], x_attn)
    dg_attn, dg_mlp, dg_kv = dg[:width], dg[width:2 * width], dg[2 * width:]
    return layer_out, d_table, (dw_q, dw_dkv, dg_kv, dw_uk, dw_uv, dw_o, dg_attn, dg_mlp, dw_gate, dw_up, dw_down)


def rows_of(w):
    return jnp.transpose(w, (1, 2, 0)).reshape(-1, w.shape[0])


def unrows(g, heads):
    return jnp.transpose(g.reshape(heads, -1, g.shape[1]), (2, 0, 1))


def solution(mesh):
    def device_step(tokens, embed_table, w_q, w_dkv, g_kv, w_uk, w_uv, w_o, g_attn, g_mlp, w_gate, w_up, w_down, d_out):
        vocab_local, model_dim = embed_table.shape
        heads = w_q.shape[1]
        key, blocks, count = block_index(tokens, vocab_local)
        rows = gather_rows(key, blocks, count, embed_table)
        layer_out, d_table, grads = layer_pass(
            rows, d_out[0], (rows_of(w_q), heads), w_dkv.T, g_kv, rows_of(w_uk), rows_of(w_uv), w_o.reshape(-1, model_dim),
            g_attn, g_mlp, w_gate.T, w_up.T, w_down, vocab_local, key, blocks, count)
        dw_q, dw_dkv, dg_kv, dw_uk, dw_uv, dw_o, dg_attn, dg_mlp, dw_gate, dw_up, dw_down = grads
        return (layer_out[None], d_table, unrows(dw_q, heads), dw_dkv.T, dg_kv, unrows(dw_uk, heads), unrows(dw_uv, heads),
                dw_o.reshape(w_o.shape), dg_attn, dg_mlp, dw_gate.T, dw_up.T, dw_down)

    row_spec = P('dp', 'tp', None)
    head_spec = P(None, 'tp', None)
    in_specs = (P('dp', None), P('tp', None), head_spec, P(None, None), P(None), head_spec, head_spec, P('tp', None, None), P(None), P(None), P(None, 'tp'), P(None, 'tp'), P('tp', None), row_spec)
    out_specs = (row_spec, P(('dp', 'tp'), None), P('dp', 'tp', None), P('dp', None), P('dp'), P('dp', 'tp', None), P('dp', 'tp', None), P(('dp', 'tp'), None, None), P('dp'), P('dp'), P('dp', 'tp'), P('dp', 'tp'), P(('dp', 'tp'), None))
    return jax.shard_map(device_step, mesh=mesh, in_specs=in_specs, out_specs=out_specs, check_vma=False)
```

```python
import functools

import jax
import jax.numpy as jnp
from jax import lax
from jax.experimental import pallas as pl
from jax.experimental.pallas import tpu as pltpu
from jax.sharding import PartitionSpec as P

EPSILON = 1e-6
ROPE_BASE = 10000.0
F32, BF16 = jnp.float32, jnp.bfloat16
LOG2E = 1.4426950408889634
VM = pltpu.VMEM
ZR = 248
GB = 64
GR = GB * 8
LIMIT = 40 << 20
ALL = 63
QB = 256


def mm(lhs, rhs, lc, rc):
    return lax.dot_general(lhs, rhs, (((lc,), (rc,)), ((), ())), preferred_element_type=F32)


def nn(a, b):
    return mm(a, b, 1, 0)


def nt(a, b):
    return mm(a, b, 1, 1)


def tn(a, b):
    return mm(a, b, 0, 0)


mean_last = functools.partial(jnp.mean, axis=-1, keepdims=True)
sum_rows = functools.partial(jnp.sum, axis=0, keepdims=True)


def rope_tables(seq_len, rope_dim):
    inv_freq = ROPE_BASE ** (-jnp.arange(0, rope_dim, 2, dtype=F32) / rope_dim)
    angles = jnp.arange(seq_len, dtype=F32)[:, None] * inv_freq[None, :]
    return jnp.cos(angles), jnp.sin(angles)


def apply_rope(x_in, cos_t, sin_t):
    half_dim = x_in.shape[-1] // 2
    x_lo, x_hi = x_in[..., :half_dim], x_in[..., half_dim:]
    return jnp.concatenate([x_lo * cos_t - x_hi * sin_t, x_hi * cos_t + x_lo * sin_t], axis=-1)


def rms_norm(x_in, gain):
    inv_rms = lax.rsqrt(mean_last(x_in * x_in) + EPSILON)
    return (x_in * inv_rms * gain).astype(BF16)


def kv_prep(latent, g_kv):
    lora = g_kv.shape[0]
    cos_t, sin_t = rope_tables(latent.shape[0], latent.shape[-1] - lora)
    k_pe = apply_rope(latent[:, lora:], cos_t, sin_t).astype(BF16)
    return rms_norm(latent[:, :lora], g_kv), k_pe


def block_index(tokens, vocab_local):
    ids = tokens.reshape(-1) - lax.axis_index('tp') * vocab_local
    n = ids.shape[0]
    owned = (ids >= 0) & (ids < vocab_local)
    blk = jnp.where(owned, ids >> 3, -1)
    pos = jnp.arange(n, dtype=jnp.int32)
    eq = (blk[:, None] == blk[None, :])
    first = jnp.min(jnp.where(eq, pos[None, :], n), axis=1)
    isf = owned & (first == pos)
    slot = jnp.sum((isf[None, :] & (pos[None, :] < first[:, None])).astype(jnp.int32), axis=1)
    key = jnp.where(owned, slot * 8 + (ids & 7), -1)
    blocks = jnp.sum(jnp.where(isf[None, :] & (slot[None, :] == pos[:, None]), blk[None, :], 0), axis=1)
    count = jnp.sum(isf.astype(jnp.int32)).reshape(1)
    return key, blocks, count


def gather_body(count_ref, blocks_ref, key_ref, tail_ref, table_ref, out_ref, stage, sem):
    rows, width = out_ref.shape
    full = table_ref.shape[0] // 8
    stage[...] = jnp.zeros_like(stage)
    out_ref[...] = jnp.zeros_like(out_ref)
    count = count_ref[0]

    def fetch(b, i):
        return pltpu.make_async_copy(table_ref.at[pl.ds(pl.multiple_of(b * 8, 8), 8), :], stage.at[i], sem)

    def chunk(ci, carry):
        base = ci * GB
        n = jnp.minimum(GB, count - base)

        def start(i, c):
            b = blocks_ref[base + i]

            @pl.when(b < full)
            def _():
                fetch(b, i).start()

            @pl.when(b >= full)
            def _():
                stage[i] = tail_ref[...]
            return c

        def wait(i, c):
            b = blocks_ref[base + i]

            @pl.when(b < full)
            def _():
                fetch(b, i).wait()
            return c

        lax.fori_loop(0, n, start, 0)
        lax.fori_loop(0, n, wait, 0)
        cols = lax.broadcasted_iota(jnp.int32, (rows, GR), 1) + base * 8
        hot = jnp.where(cols == key_ref[...], 1.0, 0.0).astype(BF16)
        for c in range(0, width, COLS):
            got = nn(hot, stage[:, :, c:c + COLS].reshape(GR, COLS))
            out_ref[:, c:c + COLS] += got.astype(BF16)
        return carry

    lax.fori_loop(0, (count + GB - 1) // GB, chunk, 0)


def gather_rows(key, blocks, count, table):
    rows, (vocab, width) = key.shape[0], table.shape
    full = vocab // 8 * 8
    tail = jnp.pad(table[full:], ((0, 8 - (vocab - full)), (0, 0)))
    smem = pl.BlockSpec(memory_space=pltpu.SMEM)
    return pl.pallas_call(
        gather_body, out_shape=jax.ShapeDtypeStruct((rows, width), BF16),
        in_specs=[smem, smem, pl.BlockSpec(memory_space=VM), pl.BlockSpec(memory_space=VM), pl.BlockSpec(memory_space=pl.ANY)],
        out_specs=pl.BlockSpec(memory_space=VM),
        scratch_shapes=[VM((GB, 8, width), BF16), pltpu.SemaphoreType.DMA],
        compiler_params=pltpu.CompilerParams(vmem_limit_bytes=LIMIT), name='gather_rows',
    )(count, blocks, key[:, None], tail, table)


def table_grad_body(count_ref, blocks_ref, key_ref, zeros_ref, *refs):
    pieces, (out_ref, tail_ref, lat_ref, de_ref, stage, sem) = refs[:-6], refs[-6:]
    rows, width = de_ref.shape
    local = rows // len(pieces)
    for k, (piece, d) in enumerate(zip(pieces, hop_order())):
        de_ref[k * local:(k + 1) * local, :] = piece[:, :width]
        lat_ref[pl.ds(pl.multiple_of(d * local, local), local), :] = piece[:, width:]
    full = out_ref.shape[0] // 8
    tail_ref[...] = jnp.zeros_like(tail_ref)
    count = count_ref[0]

    def put(b, i):
        return pltpu.make_async_copy(stage.at[i], out_ref.at[pl.ds(pl.multiple_of(b * 8, 8), 8), :], sem)

    def sums(ci):
        ids = lax.broadcasted_iota(jnp.int32, (GR, rows), 0) + ci * GR
        hot = jnp.where(ids == key_ref[...], 1.0, 0.0).astype(BF16)
        for c in range(0, width, COLS):
            got = nn(hot, de_ref[:, c:c + COLS])
            stage[:, :, c:c + COLS] = got.astype(BF16).reshape(GB, 8, COLS)

    def move(ci, go):
        base = ci * GB

        def one(i, c):
            b = blocks_ref[base + i]

            @pl.when(b < full)
            def _():
                go(put(b, i))
            @pl.when(b >= full)
            def _():
                tail_ref[...] = stage[i]
            return c

        lax.fori_loop(0, jnp.minimum(GB, count - base), one, 0)

    def chunk(ci, carry):
        sums(ci)
        move(ci, lambda cp: cp.start())
        move(ci, lambda cp: cp.wait())
        return carry

    lax.fori_loop(0, (count + GB - 1) // GB, chunk, 0)


def table_grad(key, blocks, count, pieces, table):
    (vocab, width), rows = table.shape, key.shape[0]
    latw = pieces[0].shape[1] - width
    smem, vmem, anym = (pl.BlockSpec(memory_space=m) for m in (pltpu.SMEM, VM, pl.ANY))
    full = vocab // 8 * 8
    out, tail, lat = pl.pallas_call(
        table_grad_body, out_shape=[shape((vocab, width), BF16), shape((8, width), BF16), shape((rows, latw), BF16)],
        in_specs=[smem, smem, vmem, anym] + [vmem] * len(pieces), input_output_aliases={3: 0},
        out_specs=[anym, vmem, vmem],
        scratch_shapes=[VM((rows, width), BF16), VM((GB, 8, width), BF16), pltpu.SemaphoreType.DMA],
        compiler_params=pltpu.CompilerParams(vmem_limit_bytes=LIMIT), name='table_grad',
    )(count, blocks, key[None, :], table, *pieces)
    return lax.dynamic_update_slice(out, tail[:vocab - full], (full, 0)), lat


def heads_of(q_ref, kn_ref, kp_ref, cos_ref, sin_ref, nope, half):
    q_pe = q_ref[nope:, :].astype(F32)
    lo, hi, cos_t, sin_t = q_pe[:half], q_pe[half:], cos_ref[...], sin_ref[...]
    q_all = jnp.concatenate([q_ref[:nope, :], (lo * cos_t - hi * sin_t).astype(BF16), (hi * cos_t + lo * sin_t).astype(BF16)], axis=0)
    return q_all, jnp.concatenate([kn_ref[...], kp_ref[...]], axis=0)


def scores_of(k_all, q_all, ki, qi, scale):
    s = tn(k_all[:, ki * QB:(ki + 1) * QB], q_all[:, qi * QB:(qi + 1) * QB]) * scale
    if ki == qi:
        keys = lax.broadcasted_iota(jnp.int32, (QB, QB), 0)
        s = jnp.where(keys <= lax.broadcasted_iota(jnp.int32, (QB, QB), 1), s, -1e30)
    return s


def attn_fwd_body(q_ref, kn_ref, kp_ref, v_ref, cos_ref, sin_ref, o_ref, lse_ref):
    nope, half = kn_ref.shape[0], cos_ref.shape[0]
    scale = q_ref.shape[0] ** -0.5 * LOG2E
    q_all, k_all = heads_of(q_ref, kn_ref, kp_ref, cos_ref, sin_ref, nope, half)
    for qi in range(q_ref.shape[1] // QB):
        lanes = slice(qi * QB, (qi + 1) * QB)
        s = [scores_of(k_all, q_all, ki, qi, scale) for ki in range(qi + 1)]
        top = functools.reduce(jnp.maximum, [jnp.max(x, axis=0, keepdims=True) for x in s])
        p = [jnp.exp2(x - top) for x in s]
        total = sum(sum_rows(x) for x in p)
        inv = 1.0 / total
        o = sum(nn(v_ref[:, ki * QB:(ki + 1) * QB], (x * inv).astype(BF16)) for ki, x in enumerate(p))
        o_ref[:, lanes] = o.astype(BF16)
        lse_ref[0, :, lanes] = top + jnp.log2(total)


def attn_bwd_body(heads, q_ref, kn_ref, kp_ref, v_ref, cos_ref, sin_ref, lse_ref, do_ref, dq_ref, dkn_ref, dv_ref, dkp_ref, table_ref, dk_acc, dv_acc, zero, zsem):
    full = table_ref.shape[0] // 8 * 8
    fills = [pltpu.make_async_copy(zero.at[pl.ds(0, n), :], table_ref.at[pl.ds(r, n), :], zsem.at[k])
             for k, (r, n) in enumerate((r, min(ZR, full - r)) for r in range(0, full, ZR))]

    head = pl.program_id(0)
    share = -(-len(fills) // heads)

    @pl.when(head == 0)
    def _():
        zero[...] = jnp.zeros_like(zero)
    for h in range(heads):
        @pl.when(head == h)
        def _():
            for cp in fills[h * share:(h + 1) * share]:
                cp.start()

    nope, half = kn_ref.shape[0], cos_ref.shape[0]
    raw = q_ref.shape[0] ** -0.5
    q_all, k_all = heads_of(q_ref, kn_ref, kp_ref, cos_ref, sin_ref, nope, half)
    dk_acc[...] = jnp.zeros_like(dk_acc)
    dv_acc[...] = jnp.zeros_like(dv_acc)
    for qi in range(q_ref.shape[1] // QB):
        lanes = slice(qi * QB, (qi + 1) * QB)
        q_b, do_b, lse = q_all[:, lanes], do_ref[:, lanes], lse_ref[0, :, lanes]
        p = [jnp.exp2(scores_of(k_all, q_all, ki, qi, raw * LOG2E) - lse) for ki in range(qi + 1)]
        dp = [tn(v_ref[:, ki * QB:(ki + 1) * QB], do_b) for ki in range(qi + 1)]
        delta = sum(sum_rows(a * b) for a, b in zip(p, dp))
        dq = None
        for ki in range(qi + 1):
            keys = slice(ki * QB, (ki + 1) * QB)
            ds = (p[ki] * (dp[ki] - delta) * raw).astype(BF16)
            part = nn(k_all[:, keys], ds)
            dq = part if dq is None else dq + part
            dk_acc[:, keys] += nt(q_b, ds)
            dv_acc[:, keys] += nt(do_b, p[ki].astype(BF16))
        cos_t, sin_t = cos_ref[:, lanes], sin_ref[:, lanes]
        lo, hi = dq[nope:nope + half], dq[nope + half:]
        dq_ref[:nope, lanes] = dq[:nope].astype(BF16)
        dq_ref[nope:nope + half, lanes] = (lo * cos_t + hi * sin_t).astype(BF16)
        dq_ref[nope + half:, lanes] = (hi * cos_t - lo * sin_t).astype(BF16)
    dkn_ref[...] = dk_acc[:nope, :].astype(BF16)
    dv_ref[...] = dv_acc[...].astype(BF16)

    @pl.when(head == 0)
    def _():
        dkp_ref[...] = jnp.zeros_like(dkp_ref)
    dkp_ref[...] += dk_acc[nope:, :]

    @pl.when(head == heads - 1)
    def _():
        for cp in fills:
            cp.wait()


def attn_specs(heads, qd, nope, rope, vd, seq):
    per = lambda r: pl.BlockSpec((r, seq), lambda h: (h, 0))
    one = lambda r: pl.BlockSpec((r, seq), lambda h: (0, 0))
    return [per(qd), per(nope), one(rope), per(vd), one(rope // 2), one(rope // 2)], per, one, pl.BlockSpec((1, 1, seq), lambda h: (h, 0, 0))


def attend_bwd(q, kn, kp, v, cos_t, sin_t, lse, do, heads, table):
    seq, qd, nope, vd, rope = q.shape[1], q.shape[0] // heads, kn.shape[0] // heads, v.shape[0] // heads, kp.shape[0]
    ins, per, one, lse_spec = attn_specs(heads, qd, nope, rope, vd, seq)
    return pl.pallas_call(
        functools.partial(attn_bwd_body, heads), grid=(heads,), in_specs=ins + [lse_spec, per(vd)], out_specs=[per(qd), per(nope), per(vd), one(rope), pl.BlockSpec(memory_space=pl.ANY)],
        out_shape=[jax.ShapeDtypeStruct(q.shape, BF16), jax.ShapeDtypeStruct(kn.shape, BF16), jax.ShapeDtypeStruct(v.shape, BF16), jax.ShapeDtypeStruct(kp.shape, F32), jax.ShapeDtypeStruct(table, BF16)],
        scratch_shapes=[VM((qd, seq), F32), VM((vd, seq), F32), VM((ZR, table[1]), BF16), pltpu.SemaphoreType.DMA((-(-table[0] // ZR),))],
        compiler_params=pltpu.CompilerParams(vmem_limit_bytes=ALL << 20), name='attend_bwd',
    )(q, kn, kp, v, cos_t, sin_t, lse, do)


def shift(x, bit):
    return lax.ppermute(x, 'tp', [(d, d ^ bit) for d in range(8)])


PAIR, XBIT, YBIT = 1, 2, 4


def hop_order():
    me = lax.axis_index('tp')
    flip = lambda v, bit: v + bit - 2 * bit * ((v // bit) % 2)
    own = [me, flip(me, XBIT), flip(me, YBIT), flip(flip(me, XBIT), YBIT)]
    return own + [flip(d, PAIR) for d in own]


def to_hop_order(x, axis):
    n = x.shape[axis] // 8
    return jnp.concatenate([lax.dynamic_slice_in_dim(x, d * n, n, axis) for d in hop_order()], axis=axis)


class Exchange:
    def __init__(self, widths, pieces):
        self.widths, self.pieces = widths, pieces
        self.order = range(len(pieces))

    def rs_scratch(self, rows):
        n = len(self.pieces)
        out = []
        for w in self.widths:
            out += [VM((4, rows, w), BF16), VM((2, rows, w), BF16), VM((2, rows, w), BF16), VM((rows, w), BF16), VM((rows, w), BF16)]
        dma = pltpu.SemaphoreType.DMA
        return out + [dma((4, n)), dma((4, n)), dma((2, n)), dma((2, n)), dma((n,)), dma((n,))]

    def ag_scratch(self):
        n = len(self.pieces)
        dma = pltpu.SemaphoreType.DMA
        return [dma((2, n)), dma((2, n)), dma((n,)), dma((n,)), dma((4, n)), dma((4, n))]

    def place(self, rows):
        me = lax.axis_index('tp')
        core, x, y = me % 2, (me // 2) % 2, me // 4
        dev = lambda yy, xx, cc: (yy * 2 + xx) * 2 + cc
        self.me, self.rows = me, rows
        self.pn, self.xn, self.yn = dev(y, x, 1 - core), dev(y, 1 - x, core), dev(1 - y, x, core)
        chips = [(y, x), (y, 1 - x), (1 - y, x), (1 - y, 1 - x)]
        at = lambda d: pl.ds(pl.multiple_of(d * rows, rows), rows)
        self.mine = [at(dev(*ch, core)) for ch in chips]
        self.theirs = [at(dev(*ch, 1 - core)) for ch in chips]
        self.chip = [pl.ds(pl.multiple_of(dev(*ch, 0) * rows, 2 * rows), 2 * rows) for ch in chips]

    def enter(self):
        sem = pltpu.get_barrier_semaphore()
        near = (self.pn, self.xn, self.yn)
        for d in near:
            pl.semaphore_signal(sem, inc=1, device_id={'tp': d}, device_id_type=pl.DeviceIdType.MESH)
        pl.semaphore_wait(sem, len(near))

    def copy(self, src, dst, ssem, rsem, dev):
        return pltpu.make_async_remote_copy(src_ref=src, dst_ref=dst, send_sem=ssem, recv_sem=rsem, device_id={'tp': dev}, device_id_type=pl.DeviceIdType.MESH)

    def saver(self, src, dst, sem):
        return [pltpu.make_async_copy(src.at[rows, :], dst.at[rows, :], sem.at[j]) for j, rows in enumerate(self.chip)]

    def rs_begin(self, parts, scratch):
        na = len(self.widths)
        self.parts = parts
        self.bufs = [scratch[5 * a:5 * a + 5] for a in range(na)]
        ds, dr, s1, r1, s2, r2 = scratch[5 * na:5 * na + 6]
        self.pair, self.hop1, self.hop2 = {}, {}, {}
        for i, (h, a, c0, cn) in enumerate(self.pieces):
            cols = pl.ds(c0, cn)
            dbuf, sb1, rb1, sb2, rb2 = self.bufs[a]
            for j in range(4):
                self.pair[j, i] = self.copy(parts[a].at[self.theirs[j], cols], dbuf.at[j, :, cols], ds.at[j, i], dr.at[j, i], self.pn)
            to1, to2 = (self.xn, self.yn) if h == 0 else (self.yn, self.xn)
            for k in range(2):
                self.hop1[k, i] = self.copy(sb1.at[k, :, cols], rb1.at[k, :, cols], s1.at[k, i], r1.at[k, i], to1)
            self.hop2[i] = self.copy(sb2.at[:, cols], rb2.at[:, cols], s2.at[i], r2.at[i], to2)

    def ready(self, j):
        for i in self.order:
            self.pair[j, i].start()

    def chip_sum(self, j, i):
        h, a, c0, cn = self.pieces[i]
        self.pair[j, i].wait_recv()
        return self.parts[a][self.mine[j], c0:c0 + cn].astype(F32) + self.bufs[a][0][j, :, c0:c0 + cn].astype(F32)

    def push(self, j):
        for i in self.order:
            h, a, c0, cn = self.pieces[i]
            if j == 3 or j == 1 + h:
                k = 1 if j == 3 else 0
                self.bufs[a][1][k, :, c0:c0 + cn] = self.chip_sum(j, i).astype(BF16)
                self.hop1[k, i].start()

    def relay(self, halves=(0, 1)):
        for i in self.order:
            h, a, c0, cn = self.pieces[i]
            if h not in halves:
                continue
            own = self.chip_sum(2 - h, i)
            self.hop1[1, i].wait_recv()
            self.bufs[a][3][:, c0:c0 + cn] = (own + self.bufs[a][2][1, :, c0:c0 + cn].astype(F32)).astype(BF16)
            self.hop2[i].start()

    def land(self, accs):
        for i in self.order:
            h, a, c0, cn = self.pieces[i]
            own = self.chip_sum(0, i)
            self.hop1[0, i].wait_recv()
            own = own + self.bufs[a][2][0, :, c0:c0 + cn].astype(F32)
            self.hop2[i].wait_recv()
            accs[a][:, c0:c0 + cn] = own + self.bufs[a][4][:, c0:c0 + cn].astype(F32)

    def drain(self):
        for cp in list(self.pair.values()) + list(self.hop1.values()) + list(self.hop2.values()):
            cp.wait_send()

    def reduce_scatter(self, accs, produce):
        late = None
        for j in (3, 1, 2, 0):
            produce(j)
            self.ready(j)
            if late:
                self.push(late)
            late = j
        self.relay()
        self.land(accs)

    def all_gather(self, fulls, scratch, arrive, blocks=(1, 2, 3), known=False):
        os_, xr, fs, fr, ps, pr = scratch
        half0 = [i for i in self.order if self.pieces[i][0] == 0]
        half1 = [i for i in self.order if self.pieces[i][0] == 1]

        def to(i, j, ssem, rsem, dev, rows=None):
            h, a, c0, cn = self.pieces[i]
            ref = fulls[a].at[(rows or self.mine)[j], pl.ds(c0, cn)]
            return self.copy(ref, ref, ssem, rsem, dev)

        near = (self.xn, self.yn)
        own = [[to(i, 0, os_.at[k, i], xr.at[k, i], dev) for i in self.order] for k, dev in enumerate(near)]
        from_n = [[to(i, 1 + k, os_.at[k, i], xr.at[k, i], dev) for i in self.order] for k, dev in enumerate(near)]
        fwd = [to(i, 2 - self.pieces[i][0], fs.at[i], fr.at[i], near[self.pieces[i][0]]) for i in self.order]
        diag = [to(i, 3, fs.at[i], fr.at[i], self.xn) for i in self.order]
        give = [[to(i, j, ps.at[j, i], pr.at[j, i], self.pn) for i in self.order] for j in range(4)]
        take = [[to(i, j, ps.at[j, i], pr.at[j, i], self.pn, self.theirs) for i in self.order] for j in range(4)]
        pairs = list(zip(half0, half1))
        sent = fwd + [cp for g in give for cp in g]

        def start(copies):
            for cp in copies:
                cp.start()

        def landed(copies):
            for cp in copies:
                cp.wait_recv()

        if not known:
            sent += own[0] + own[1]
            for i0, i1 in pairs:
                start((own[0][i1], own[1][i0]))
            for i0, i1 in pairs:
                start((own[0][i0], own[1][i1]))
        start(give[0])
        if known:
            start(fwd + give[1] + give[2])
        landed(take[0])
        arrive(0)
        if not known:
            for i0, i1 in pairs:
                from_n[1][i0].wait_recv()
                start((fwd[i0], give[2][i0]))
                from_n[0][i1].wait_recv()
                start((fwd[i1], give[1][i1]))
            for i0, i1 in pairs:
                from_n[1][i1].wait_recv()
                give[2][i1].start()
                from_n[0][i0].wait_recv()
                give[1][i0].start()
        for j in blocks:
            if j == 3:
                for i in self.order:
                    diag[i].wait_recv()
                    give[3][i].start()
            landed(take[j])
            arrive(j)
        for cp in sent:
            cp.wait_send()


def halves(width, n):
    step = width // (2 * n)
    return [(h, 0, (h * n + k) * step, step) for k in range(n) for h in range(2)]


MAIN = halves(2560, 2)
LAST = MAIN + [(0, 1, 0, 256), (1, 1, 256, 128)]
NRS, NAG = 11, 6
COLS = 512


def norm_rows(x, gain):
    return x * lax.rsqrt(mean_last(x * x) + EPSILON) * gain


def norm_rows_vjp(x, gain, dy):
    r = lax.rsqrt(mean_last(x * x) + EPSILON)
    gd = dy * gain
    dot = mean_last(gd * x)
    return r * gd - x * (r * r * r * dot), sum_rows(dy * x * r)


def exchange_call(body, name, cid, ins, out_shape, scratch, far=0, out=0, limit=50):
    vmem, hbm = pl.BlockSpec(memory_space=VM), pl.BlockSpec(memory_space=pltpu.HBM)
    return pl.pallas_call(
        body, out_shape=out_shape, in_specs=[vmem] * (len(ins) - far) + [hbm] * far, out_specs=[vmem] * (len(out_shape) - out) + [hbm] * out, scratch_shapes=scratch,
        compiler_params=pltpu.CompilerParams(vmem_limit_bytes=limit << 20, collective_id=cid, has_side_effects=True), name=name)(*ins)


def shape(dims, dtype):
    return jax.ShapeDtypeStruct(dims, dtype)


def idle(j):
    pass


def embed_body(part, gain, wq, wdkv, e_ref, q_ref, lat_ref, u_out, full, usem, acc, *scratch):
    ex = Exchange([part.shape[1]], MAIN)
    ex.place(acc.shape[0])
    ex.enter()
    ex.rs_begin([part], scratch)
    ex.reduce_scatter([acc], idle)
    e = acc[...].astype(BF16)
    e_ref[...] = e
    full[ex.mine[0], :] = norm_rows(e.astype(F32), gain[...]).astype(BF16)

    def arrive(j):
        u = full[ex.chip[j], :]
        q_ref[:, ex.chip[j]] = nt(wq[...], u).astype(BF16)
        lat_ref[ex.chip[j], :] = nt(u, wdkv[...])
        save[j].start()

    save = ex.saver(full, u_out, usem)
    ex.all_gather([full], scratch[NRS:], arrive)
    ex.drain()
    for cp in save:
        cp.wait()


def attn_body(lat, g_kv, wuk, wuv, q_ref, cos_ref, sin_ref, dy_ref, dyx_ref, dyy_ref, c_ref, kn_ref, kp_ref, v_ref, o_ref, lse_ref, dy_out, dyf, dsem, *scratch):
    ex = Exchange([dyf.shape[1]], MAIN)
    ex.place(dy_ref.shape[0])
    ex.enter()
    for rows, ref in zip(ex.mine, (dy_ref, dyx_ref, dyy_ref)):
        dyf[rows, :] = ref[...]
    lora, half, heads = c_ref.shape[1], cos_ref.shape[0], lse_ref.shape[0]
    per = lambda ref, h: ref.at[pl.ds(h * (ref.shape[0] // heads), ref.shape[0] // heads), :]

    save = ex.saver(dyf, dy_out, dsem)

    def arrive(j):
        save[j].start()
        if j:
            return
        c = norm_rows(lat[:, :lora], g_kv[...]).astype(BF16)
        c_ref[...] = c
        pe = lat[:, lora:].T
        lo, hi, cos_t, sin_t = pe[:half], pe[half:], cos_ref[...], sin_ref[...]
        kp_ref[...] = jnp.concatenate([lo * cos_t - hi * sin_t, hi * cos_t + lo * sin_t], axis=0).astype(BF16)
        kn_ref[...] = nt(wuk[...], c).astype(BF16)
        v_ref[...] = nt(wuv[...], c).astype(BF16)
        for h in range(heads):
            attn_fwd_body(per(q_ref, h), per(kn_ref, h), kp_ref, per(v_ref, h), cos_ref, sin_ref, per(o_ref, h), lse_ref.at[pl.ds(h, 1)])

    ex.all_gather([dyf], scratch, arrive, known=True)
    for cp in save:
        cp.wait()


def middle_body(o_ref, wo, e_ref, gain, dyl_ref, dy_hbm, wg_hbm, wu_hbm, wd_hbm,
                h_ref, y_ref, dres_ref, dgain_ref, do_ref, z_out, hid_out, dgate_out, dup_out, dfull_out,
                wall, dyb, act, part, ypart, z, acc, wsem, dsem, asem, zsem, fsem, *scratch):
    ex, ey = Exchange([part.shape[1]], MAIN), Exchange([part.shape[1]], MAIN)
    for e in (ex, ey):
        e.place(acc.shape[0])
    ex.enter()
    ffn = wd_hbm.shape[0]
    wg, wu, wd = (wall.at[pl.ds(k * ffn, ffn), :] for k in range(3))
    dfull = wall.at[pl.ds(0, part.shape[0]), :]
    loads = [pltpu.make_async_copy(a, b, wsem.at[k]) for k, (a, b) in enumerate(((wg_hbm, wg), (wu_hbm, wu), (wd_hbm, wd)))]
    turns = (0, 1, 3, 2)
    dy_in = [pltpu.make_async_copy(dy_hbm.at[ex.chip[j], :], dyb.at[k % 2], dsem.at[k % 2]) for k, j in enumerate(turns)]
    for cp in loads + dy_in[:2]:
        cp.start()
    rs = 2 * NRS
    ex.rs_begin([part], scratch)
    ey.rs_begin([ypart], scratch[NRS:])
    width = part.shape[1]

    def attn_part(j):
        part[ex.chip[j], :] = tn(o_ref[:, ex.chip[j]], wo[...]).astype(BF16)

    ex.reduce_scatter([acc], attn_part)
    h = (e_ref[...].astype(F32) + acc[...].astype(BF16).astype(F32)).astype(BF16)
    h_ref[...] = h
    z[ex.mine[0], :] = norm_rows(h.astype(F32), gain[...]).astype(BF16)
    save_z, save_d = ex.saver(z, z_out, zsem), ex.saver(dfull, dfull_out, fsem)
    save_a = [[pltpu.make_async_copy(act.at[t % 2, k], dst.at[ex.chip[j], :], asem.at[t % 2, k]) for k, dst in enumerate((hid_out, dgate_out, dup_out))]
              for t, j in enumerate(turns)]

    def mlp(j, t):
        rows = ex.chip[j]
        gate, up = nt(z[rows, :], wg[...]), nt(z[rows, :], wu[...])
        sig = jax.nn.sigmoid(gate)
        hid = (gate * sig * up).astype(BF16)
        dh = nt(dyb[t % 2], wd[...])
        dup = (dh * gate * sig).astype(BF16)
        dgate = (dh * up * sig * (1.0 + gate * (1.0 - sig))).astype(BF16)
        if t > 1:
            for cp in save_a[t - 2]:
                cp.wait()
        for k, value in enumerate((hid, dgate, dup)):
            act[t % 2, k] = value
        for c in range(0, width, COLS):
            cols = slice(c, c + COLS)
            part[rows, cols] = (nn(dgate, wg[:, cols]) + nn(dup, wu[:, cols])).astype(BF16)
            ypart[rows, cols] = nn(hid, wd[:, cols]).astype(BF16)
        for cp in save_a[t]:
            cp.start()

    def arrive_z(j):
        if j == 0:
            ex.drain()
            for cp in loads:
                cp.wait()
        save_z[j].start()
        for e in (ex, ey):
            if j == 3:
                e.push(1)
            if j == 2:
                e.push(3)
        k = turns.index(j)
        dy_in[k].wait()
        mlp(j, k)
        if k < 2:
            dy_in[k + 2].start()
        for e in (ex, ey):
            e.ready(j)

    ex.all_gather([z], scratch[rs:rs + NAG], arrive_z, blocks=turns[1:])
    for e in (ex, ey):
        e.relay((1,))
        e.push(2)
        e.relay((0,))
    ex.land([acc])
    dx, dgain_ref[...] = norm_rows_vjp(h_ref[...].astype(F32), gain[...], acc[...])
    dres = dyl_ref[...].astype(F32) + dx
    dres_ref[...] = dres
    dfull[ex.mine[0], :] = dres.astype(BF16)

    def arrive_d(j):
        do_ref[:, ex.chip[j]] = nt(wo[...], dfull[ex.chip[j], :]).astype(BF16)
        save_d[j].start()
        if j == 2:
            ey.land([acc])
            y_ref[...] = (h_ref[...].astype(F32) + acc[...].astype(BF16).astype(F32)).astype(BF16)

    ex.all_gather([dfull], scratch[rs + NAG:], arrive_d)
    ex.drain()
    ey.drain()
    for cp in save_z + save_d + save_a[2] + save_a[3]:
        cp.wait()


def attn_back_body(dq_ref, lat, wq, wdkv, e_ref, dres_ref, gain, de_ref, dg_ref, part, acc, acc_lat, *scratch):
    ex = Exchange([part.shape[1], lat.shape[1]], LAST)
    ex.place(acc.shape[0])
    ex.enter()
    ex.rs_begin([part, lat], scratch)
    lw = wdkv.shape[0]

    def produce(j):
        rows = ex.chip[j]
        part[rows, :] = (tn(dq_ref[:, rows], wq[...]) + nn(lat[rows, :lw], wdkv[...])).astype(BF16)

    ex.reduce_scatter([acc, acc_lat], produce)
    dx, dg_ref[...] = norm_rows_vjp(e_ref[...].astype(F32), gain[...], acc[...])
    de_ref[:, :dx.shape[1]] = (dres_ref[...] + dx).astype(BF16)
    de_ref[:, dx.shape[1]:] = acc_lat[...].astype(BF16)
    ex.drain()


def layer_pass(rows, d_out, w_q, w_dkv, g_kv, w_uk, w_uv, w_o, g_attn, g_mlp, w_gate, w_up, w_down, vocab, key, blocks, count):
    w_q, heads = w_q
    seq, width = rows.shape
    local = d_out.shape[0]
    lora = g_kv.shape[0]
    latw = w_dkv.shape[0]
    one = Exchange([width], MAIN)
    main = [VM((local, width), F32)] + one.rs_scratch(local) + one.ag_scratch()
    partb = [VM((seq, width), BF16)]
    dma = pltpu.SemaphoreType.DMA
    saved = partb + [dma((4,))]
    loc, fullb = shape((local, width), BF16), shape((seq, width), BF16)
    ga, gm = g_attn[None, :], g_mlp[None, :]
    rows, dy_near = lax.optimization_barrier((rows, [shift(d_out, XBIT), shift(d_out, YBIT)]))
    embedded, query, latent, x_attn = exchange_call(
        embed_body, 'embed_exchange', 1, [rows, ga, w_q, w_dkv], [loc, shape((w_q.shape[0], seq), BF16), shape((seq, latw), F32), fullb], saved + main, out=1, limit=36)
    cos_t, sin_t = (t.T for t in rope_tables(seq, latw - lora))
    nq, nk, nv = w_q.shape[0], w_uk.shape[0], w_uv.shape[0]
    c_kv, k_nope, k_pe_t, value, attn_out, lse, dy_full = exchange_call(
        attn_body, 'attend_fwd', 2, [latent, g_kv[None, :], w_uk, w_uv, query, cos_t, sin_t, d_out, *dy_near],
        [shape((seq, lora), BF16), shape((nk, seq), BF16), shape((latw - lora, seq), BF16), shape((nv, seq), BF16), shape((nv, seq), BF16),
         shape((heads, 1, seq), F32), fullb], saved + one.ag_scratch(), out=1, limit=ALL)
    kv_pull = jax.vjp(kv_prep, latent, g_kv)[1]
    ffn = w_gate.shape[0]
    act = shape((seq, ffn), BF16)
    residual, layer_out, d_residual, dg_mlp, d_attn_out, x_mlp, hidden, d_gate, d_up, d_attn_full = exchange_call(
        middle_body, 'middle', 3, [attn_out, w_o, embedded, gm, d_out, dy_full, w_gate, w_up, w_down],
        [loc, loc, shape((local, width), F32), shape((1, width), F32), shape((w_o.shape[0], seq), BF16), fullb, act, act, act, fullb],
        [VM((3 * ffn, width), BF16), VM((2, seq // 4, width), BF16), VM((2, 3, seq // 4, ffn), BF16)] + partb * 3
        + [VM((local, width), F32), dma((3,)), dma((2,)), dma((2, 3)), dma((4,)), dma((4,))]
        + one.rs_scratch(local) * 2 + one.ag_scratch() * 2, far=4, out=5, limit=ALL)
    d_query, d_knope, d_value, d_kpe, table0 = attend_bwd(query, k_nope, k_pe_t, value, cos_t, sin_t, lse, d_attn_out, heads, (vocab, width))
    d_ckv = (tn(d_knope, w_uk) + tn(d_value, w_uv)).astype(BF16)
    d_latent, dg_kv = kv_pull((d_ckv, d_kpe.T.astype(BF16)))
    lat_part = jnp.pad(d_latent.astype(BF16), ((0, 0), (0, -latw % 128)))
    padw = lat_part.shape[1]
    two = Exchange([width, padw], LAST)
    de, dg_attn = exchange_call(
        attn_back_body, 'back_exchange', 4, [d_query, lat_part, w_q, w_dkv, embedded, d_residual, ga],
        [shape((local, width + padw), BF16), shape((1, width), F32)],
        partb + [VM((local, width), F32), VM((local, padw), F32)] + two.rs_scratch(local))
    later = lax.optimization_barrier
    dg = jnp.concatenate([dg_attn[0], dg_mlp[0], dg_kv])
    hidden, d_gate, d_up, d_query, attn_out, de, dg = later((hidden, d_gate, d_up, d_query, attn_out, de, dg))
    near = [shift(de, XBIT), shift(de, YBIT), shift(de, XBIT + YBIT)]
    pair = shift(de, PAIR)
    dg = dg + shift(dg, PAIR)
    dw_q, dw_o = nn(d_query, x_attn), nn(attn_out, d_attn_full)
    dw_q, dw_o, hidden, d_gate, d_up = later((dw_q, dw_o, hidden, d_gate, d_up))
    dw_down, dw_gate, dw_up = tn(hidden, dy_full), tn(d_gate, x_mlp), tn(d_up, x_mlp)
    dw_down, dw_gate, dw_up, dw_q, dw_o, near, pair, dg, d_knope, d_value = later((dw_down, dw_gate, dw_up, dw_q, dw_o, near, pair, dg, d_knope, d_value))
    far = [shift(b, PAIR) for b in near]
    dg = dg + shift(dg, XBIT)
    dw_uk, dw_uv = nn(d_knope, c_kv), nn(d_value, c_kv)
    dw_uk, dw_uv, far, dg = later((dw_uk, dw_uv, far, dg))
    dg = dg + shift(dg, YBIT)
    d_table, lat_full = table_grad(to_hop_order(key, 0), blocks, count, [de, *near, pair, *far], table0)
    dw_dkv = tn(lat_full[:, :latw], x_attn)
    dg_attn, dg_mlp, dg_kv = dg[:width], dg[width:2 * width], dg[2 * width:]
    return layer_out, d_table, (dw_q, dw_dkv, dg_kv, dw_uk, dw_uv, dw_o, dg_attn, dg_mlp, dw_gate, dw_up, dw_down)


def rows_of(w):
    return jnp.transpose(w, (1, 2, 0)).reshape(-1, w.shape[0])


def unrows(g, heads):
    return jnp.transpose(g.reshape(heads, -1, g.shape[1]), (2, 0, 1))


def solution(mesh):
    def device_step(tokens, embed_table, w_q, w_dkv, g_kv, w_uk, w_uv, w_o, g_attn, g_mlp, w_gate, w_up, w_down, d_out):
        vocab_local, model_dim = embed_table.shape
        heads = w_q.shape[1]
        key, blocks, count = block_index(tokens, vocab_local)
        rows = gather_rows(key, blocks, count, embed_table)
        layer_out, d_table, grads = layer_pass(
            rows, d_out[0], (rows_of(w_q), heads), w_dkv.T, g_kv, rows_of(w_uk), rows_of(w_uv), w_o.reshape(-1, model_dim),
            g_attn, g_mlp, w_gate.T, w_up.T, w_down, vocab_local, key, blocks, count)
        dw_q, dw_dkv, dg_kv, dw_uk, dw_uv, dw_o, dg_attn, dg_mlp, dw_gate, dw_up, dw_down = grads
        return (layer_out[None], d_table, unrows(dw_q, heads), dw_dkv.T, dg_kv, unrows(dw_uk, heads), unrows(dw_uv, heads),
                dw_o.reshape(w_o.shape), dg_attn, dg_mlp, dw_gate.T, dw_up.T, dw_down)

    row_spec = P('dp', 'tp', None)
    head_spec = P(None, 'tp', None)
    in_specs = (P('dp', None), P('tp', None), head_spec, P(None, None), P(None), head_spec, head_spec, P('tp', None, None), P(None), P(None), P(None, 'tp'), P(None, 'tp'), P('tp', None), row_spec)
    out_specs = (row_spec, P(('dp', 'tp'), None), P('dp', 'tp', None), P('dp', None), P('dp'), P('dp', 'tp', None), P('dp', 'tp', None), P(('dp', 'tp'), None, None), P('dp'), P('dp'), P('dp', 'tp'), P('dp', 'tp'), P(('dp', 'tp'), None))
    return jax.shard_map(device_step, mesh=mesh, in_specs=in_specs, out_specs=out_specs, check_vma=False)
```
